32 devices in a mesh: rows: 4 (over y, core), cols: 8 (over z, x).
Axes of the slice: x: 2, y: 2, z: 4, core: 2. Of those that a mesh axis runs over, the one named last changes fastest.
Arguments:
- single: bfloat16 [512, 1024], P('rows'), may hold values from -6 to 6
- pair: bfloat16 [512, 512, 128], P('rows', 'cols'), may hold values from -6 to 6
- residue_mask: int32 [512], replicated, may hold values from 0 to 1, as said below
- w_bias: bfloat16 [128, 32], replicated, may hold values from -40 to 40
- w_project: bfloat16 [4, 1024, 1024], P(None, None, 'cols'), may hold values from -0.1875 to 0.1875
- w_out: bfloat16 [1024, 1024], replicated, may hold values from -0.1875 to 0.1875
- w_factors: bfloat16 [1024, 128], replicated, may hold values from -0.1875 to 0.1875
- w_pairout: bfloat16 [128, 128], replicated, may hold values from -0.5 to 0.5
- w_up: bfloat16 [128, 512], replicated, may hold values from -0.5 to 0.5
- w_down: bfloat16 [512, 128], replicated, may hold values from -0.25 to 0.25
Outputs:
- single_out: bfloat16 [512, 1024], P('rows')
- pair_out: bfloat16 [512, 512, 128], P('rows', 'cols')
The draws below stay inside these ranges and needn't reach their ends.
Inputs may be any that keep to these rules, and one draw needn't show every extreme that they name: residue_mask is 1 on a leading run of at least 256 positions and 0 after it.
All inputs are finite; a program needn't handle non-finite values.
Results may differ from the reference program's by a relative error of at most 0.01.
The reference program's roundings to bfloat16 on the way count: a program that leaves them out, or rounds other values in their place, can miss the bound.
Values may be sent and summed in bfloat16 or wider, within the bound.
A program may use at most 64 MiB of HBM per device.

```python
import math
import jax
import jax.numpy as jnp
from jax import lax

SINGLE = 1024
HEADS = 32
HEAD_DIM = 32
PAIR = 128
PAIR_HID = 512
OPD = 64
RESIDUES = 512


def draw_residue_mask(key, part):
    length_now = jax.random.randint(jax.random.fold_in(key, 11), (), RESIDUES // 2, RESIDUES + 1)
    return (jnp.arange(RESIDUES, dtype=jnp.int32) < length_now).astype(jnp.int32)


def draw_w_bias(key, part):
    drawn = jax.random.normal(jax.random.fold_in(key, 23), (PAIR, HEADS), jnp.float32) / jnp.sqrt(jnp.float32(PAIR))
    return jnp.clip(drawn, -40.0, 40.0).astype(jnp.bfloat16)


def block_levels(key, shape, split, smallest, high):
    gain, own = 1.0, jax.random.fold_in(key, 6)
    for position, blocks in split:
        steps = jnp.exp(jax.random.uniform(jax.random.fold_in(own, position), (blocks,), jnp.float32, smallest / len(split), high / len(split)))
        gain = gain * jnp.repeat(steps, shape[position] // blocks).reshape([-1 if axis == position else 1 for axis in range(len(shape))])
    return gain


def scatter_about(stream_key, dims, deviation, limit, split=(), kind=jnp.bfloat16):
    entries = deviation * jax.random.normal(stream_key, dims, jnp.float32)
    if split:
        entries = entries * block_levels(stream_key, dims, split, -0.22, 0.18)
    return jnp.clip(entries, -limit, limit).astype(kind)


def setup_inputs(seed: int = 0) -> dict:
    streams_of = jax.random.split(jax.random.key(seed), 11)
    return {
        "single": scatter_about(streams_of[0], (RESIDUES, SINGLE), 1.0, 6.0, ((0, 4),)),
        "pair": scatter_about(streams_of[1], (RESIDUES, RESIDUES, PAIR), 1.0, 6.0, ((0, 4), (1, 8))),
        "residue_mask": draw_residue_mask(jax.random.fold_in(streams_of[10], 71), 0),
        "w_bias": draw_w_bias(jax.random.fold_in(streams_of[10], 71), 0),
        "w_project": scatter_about(streams_of[4], (4, SINGLE, SINGLE), SINGLE ** -0.5, 0.1875, ((2, 8),)),
        "w_out": scatter_about(streams_of[5], (SINGLE, SINGLE), SINGLE ** -0.5, 0.1875),
        "w_factors": scatter_about(streams_of[6], (SINGLE, 2 * OPD), SINGLE ** -0.5, 0.1875),
        "w_pairout": scatter_about(streams_of[7], (2 * OPD, PAIR), (2 * OPD) ** -0.5, 0.5),
        "w_up": scatter_about(streams_of[8], (PAIR, PAIR_HID), PAIR ** -0.5, 0.5),
        "w_down": scatter_about(streams_of[9], (PAIR_HID, PAIR), PAIR_HID ** -0.5, 0.25),
    }


epsilon = 1e-05

def normalize(values):
    values = values.astype(jnp.float32)
    centred = values - lax.optimization_barrier(jnp.mean(values, -1, keepdims=True))
    return centred * lax.rsqrt(lax.optimization_barrier(jnp.mean(centred * centred, -1, keepdims=True)) + epsilon)

def reference(single, pair, residue_mask, w_bias, w_project, w_out, w_factors, w_pairout, w_up, w_down):
    block_rows = math.gcd(RESIDUES, 32)
    count_blocks = RESIDUES // block_rows
    pair_blocks = pair.reshape(count_blocks, block_rows, RESIDUES, PAIR)

    def bias_block(pair_block):
        normed_pair = normalize(pair_block).astype(jnp.bfloat16)
        return jnp.einsum('rcp,ph->hrc', normed_pair.astype(jnp.float32), w_bias.astype(jnp.float32)).astype(jnp.bfloat16)
    bias_parts = lax.map(bias_block, pair_blocks)
    bias_all = jnp.transpose(bias_parts, (1, 0, 2, 3)).reshape(HEADS, RESIDUES, RESIDUES)
    normed_single = normalize(single).astype(jnp.bfloat16)
    projected = jnp.einsum('rs,fsc->frc', normed_single.astype(jnp.float32), w_project.astype(jnp.float32))
    query_rows = projected[0].astype(jnp.bfloat16).reshape(RESIDUES, HEADS, HEAD_DIM).transpose(1, 0, 2)
    key_rows = projected[1].astype(jnp.bfloat16).reshape(RESIDUES, HEADS, HEAD_DIM).transpose(1, 0, 2)
    value_rows = projected[2].astype(jnp.bfloat16).reshape(RESIDUES, HEADS, HEAD_DIM).transpose(1, 0, 2)
    gate_values = jax.nn.sigmoid(projected[3])
    key_valid = (residue_mask > 0)[None, :]
    score_scale = 1.0 / math.sqrt(HEAD_DIM)

    def attend_head(operands):
        query_head, key_head, value_head, bias_head = operands
        scores = jnp.dot(query_head, key_head.T, preferred_element_type=jnp.float32) * score_scale + bias_head.astype(jnp.float32)
        scores = jnp.where(key_valid, scores, -jnp.inf)
        weights = jax.nn.softmax(scores, axis=-1).astype(jnp.bfloat16)
        return jnp.dot(weights, value_head, preferred_element_type=jnp.float32)
    attended = lax.map(attend_head, (query_rows, key_rows, value_rows, bias_all))
    attended = attended.transpose(1, 0, 2).reshape(RESIDUES, SINGLE)
    mixed = (attended * gate_values).astype(jnp.bfloat16)
    single_out = (single.astype(jnp.float32) + jnp.dot(mixed, w_out, preferred_element_type=jnp.float32)).astype(jnp.bfloat16)
    normed_out = normalize(single_out).astype(jnp.bfloat16)
    factors = jnp.dot(normed_out, w_factors, preferred_element_type=jnp.float32).astype(jnp.bfloat16)
    left_factor = factors[:, :OPD]
    right_factor = factors[:, OPD:]

    def update_block(operands):
        pair_block, left_block = operands
        left_wide = left_block.astype(jnp.float32)[:, None, :]
        right_wide = right_factor.astype(jnp.float32)[None, :, :]
        paired = jnp.concatenate([left_wide * right_wide, left_wide - right_wide], -1).astype(jnp.bfloat16)
        pair_mid = (pair_block.astype(jnp.float32) + jnp.einsum('rcq,qp->rcp', paired.astype(jnp.float32), w_pairout.astype(jnp.float32))).astype(jnp.bfloat16)
        normed_mid = normalize(pair_mid).astype(jnp.bfloat16)
        hidden = jax.nn.relu(jnp.einsum('rcp,pk->rck', normed_mid.astype(jnp.float32), w_up.astype(jnp.float32))).astype(jnp.bfloat16)
        return (pair_mid.astype(jnp.float32) + jnp.einsum('rck,kp->rcp', hidden.astype(jnp.float32), w_down.astype(jnp.float32))).astype(jnp.bfloat16)
    updated = lax.map(update_block, (pair_blocks, left_factor.reshape(count_blocks, block_rows, OPD)))
    return (single_out, updated.reshape(RESIDUES, RESIDUES, PAIR))
```

```python
import functools
import math

import jax
import jax.numpy as jnp
from jax import lax
from jax.experimental import pallas as pl
from jax.experimental.pallas import tpu as pltpu
from jax.sharding import PartitionSpec as P

epsilon = 1e-05


def enter(axes):
    barrier = pltpu.get_barrier_semaphore()
    total = 0
    for axis, size in axes:
        me = lax.axis_index(axis)
        for step in range(1, size):
            pl.semaphore_signal(
                barrier,
                inc=1,
                device_id={axis: lax.rem(me + step, size)},
                device_id_type=pl.DeviceIdType.MESH,
            )
        total += size - 1
    pl.semaphore_wait(barrier, total)


def spread(axis, size, source, landing, send_sems, recv_sems):
    me = lax.axis_index(axis)
    copies = []
    for step in range(1, size):
        copy = pltpu.make_async_remote_copy(
            src_ref=source,
            dst_ref=landing.at[me],
            send_sem=send_sems.at[step - 1],
            recv_sem=recv_sems.at[step - 1],
            device_id={axis: lax.rem(me + step, size)},
            device_id_type=pl.DeviceIdType.MESH,
        )
        copy.start()
        copies.append(copy)
    return copies


def gather_kernel(axis, size, source, gathered, send_sems, recv_sems, own_sem):
    enter([(axis, size)])
    copies = spread(axis, size, source, gathered, send_sems, recv_sems)
    own = pltpu.make_async_copy(source, gathered.at[lax.axis_index(axis)], own_sem)
    own.start()
    own.wait()
    for copy in copies:
        copy.wait()


def gather(values, axis, size, collective_id):
    return pl.pallas_call(
        functools.partial(gather_kernel, axis, size),
        out_shape=jax.ShapeDtypeStruct((size, *values.shape), values.dtype),
        in_specs=[pl.BlockSpec(memory_space=pltpu.VMEM)],
        out_specs=pl.BlockSpec(memory_space=pltpu.VMEM),
        scratch_shapes=[
            pltpu.SemaphoreType.DMA((size - 1,)),
            pltpu.SemaphoreType.DMA((size - 1,)),
            pltpu.SemaphoreType.DMA,
        ],
        compiler_params=pltpu.CompilerParams(collective_id=collective_id, has_side_effects=True),
        name="gather_" + axis,
    )(values)


def single_kernel(
    row_size, col_size, tile_cols,
    mixed, single, w_out, w_factors, single_out, left_out, right_out,
    gathered, factor_right, send_sems, recv_sems, row_send, row_recv, own_sem,
):
    enter([("cols", col_size), ("rows", row_size)])
    tile_rows, width = mixed.shape
    me_col = lax.axis_index("cols")
    me_row = lax.axis_index("rows")
    copies = spread("cols", col_size, mixed, gathered, send_sems, recv_sems)
    own = pltpu.make_async_copy(mixed, gathered.at[me_col], own_sem)
    own.start()
    own.wait()
    for copy in copies:
        copy.wait()
    whole = jnp.concatenate([gathered[part] for part in range(col_size)], axis=1)
    total = jnp.dot(whole, w_out[...], preferred_element_type=jnp.float32)
    updated = (single[...].astype(jnp.float32) + total).astype(jnp.bfloat16)
    single_out[...] = updated
    normed = layer_norm(updated).astype(jnp.bfloat16)
    factors = jnp.dot(normed, w_factors[...], preferred_element_type=jnp.float32)
    factors = factors.astype(jnp.bfloat16).astype(jnp.float32)
    half = factors.shape[1] // 2
    swapped = jnp.concatenate([factors[:, half:], factors[:, :half]], axis=1)
    lower = lax.broadcasted_iota(jnp.int32, factors.shape, 1) < half
    left_out[...] = jnp.where(lower, factors, swapped)
    factor_right[...] = jnp.where(lower, swapped, factors).astype(jnp.bfloat16)
    first = me_col * tile_cols
    owner = first // tile_rows
    offset = pl.multiple_of(first - owner * tile_rows, tile_cols)
    piece = factor_right.at[pl.ds(offset, tile_cols)]

    @pl.when(me_row == owner)
    def _():
        local = pltpu.make_async_copy(piece, right_out, own_sem)
        local.start()
        sends = []
        for step in range(1, row_size):
            send = pltpu.make_async_remote_copy(
                src_ref=piece,
                dst_ref=right_out,
                send_sem=row_send.at[step - 1],
                recv_sem=row_recv,
                device_id={"rows": lax.rem(me_row + step, row_size)},
                device_id_type=pl.DeviceIdType.MESH,
            )
            send.start()
            sends.append(send)
        local.wait()
        for send in sends:
            send.wait_send()

    @pl.when(me_row != owner)
    def _():
        pltpu.make_async_remote_copy(
            src_ref=piece,
            dst_ref=right_out,
            send_sem=row_send.at[0],
            recv_sem=row_recv,
            device_id={"rows": lax.rem(me_row + 1, row_size)},
            device_id_type=pl.DeviceIdType.MESH,
        ).wait_recv()


def update_single(mixed, single, w_out, w_factors, row_size, col_size, tile_cols):
    tile_rows, width = single.shape
    wide = w_factors.shape[1]
    return pl.pallas_call(
        functools.partial(single_kernel, row_size, col_size, tile_cols),
        out_shape=(
            jax.ShapeDtypeStruct((tile_rows, width), jnp.bfloat16),
            jax.ShapeDtypeStruct((tile_rows, wide), jnp.float32),
            jax.ShapeDtypeStruct((tile_cols, wide), jnp.bfloat16),
        ),
        in_specs=[pl.BlockSpec(memory_space=pltpu.VMEM)] * 4,
        out_specs=[pl.BlockSpec(memory_space=pltpu.VMEM)] * 3,
        scratch_shapes=[
            pltpu.VMEM((col_size, *mixed.shape), jnp.bfloat16),
            pltpu.VMEM((tile_rows, wide), jnp.bfloat16),
            pltpu.SemaphoreType.DMA((col_size - 1,)),
            pltpu.SemaphoreType.DMA((col_size - 1,)),
            pltpu.SemaphoreType.DMA((row_size - 1,)),
            pltpu.SemaphoreType.DMA,
            pltpu.SemaphoreType.DMA,
        ],
        compiler_params=pltpu.CompilerParams(collective_id=2, has_side_effects=True),
        name="update_single",
    )(mixed, single, w_out, w_factors)


def matmul_norm(values):
    wide = values.shape[1]
    share = jnp.full((2 * wide, wide), 1.0 / wide, jnp.bfloat16)
    mean = jnp.dot(values, share[:wide], preferred_element_type=jnp.float32)
    centred = values.astype(jnp.float32) - mean
    square = centred * centred
    high = square.astype(jnp.bfloat16)
    low = (square - high.astype(jnp.float32)).astype(jnp.bfloat16)
    spread_out = jnp.dot(
        jnp.concatenate([high, low], 1), share, preferred_element_type=jnp.float32
    )
    return (centred * lax.rsqrt(spread_out + epsilon)).astype(jnp.bfloat16)


def norm_kernel(values, normed):
    normed[...] = matmul_norm(values[...])


def norm_rows(values, block):
    spec = pl.BlockSpec((block, values.shape[1]), lambda step: (step, 0))
    return pl.pallas_call(
        norm_kernel,
        out_shape=jax.ShapeDtypeStruct(values.shape, jnp.bfloat16),
        grid=(values.shape[0] // block,),
        in_specs=[spec],
        out_specs=spec,
        name="norm_pair",
    )(values)


def pair_kernel(pair, left, right, w_pairout, w_up, w_down, updated):
    block_rows, tile_cols, wide = pair.shape
    left_wide = left[...][:, None, :]
    right_wide = right[...].astype(jnp.float32)[None, :, :]
    lower = lax.broadcasted_iota(jnp.int32, pair.shape, 2) < wide // 2
    paired = jnp.where(lower, left_wide * right_wide, left_wide - right_wide)
    paired = paired.astype(jnp.bfloat16).reshape(block_rows * tile_cols, wide)
    flat = pair[...].reshape(block_rows * tile_cols, wide).astype(jnp.float32)
    mid = flat + jnp.dot(paired, w_pairout[...], preferred_element_type=jnp.float32)
    mid = mid.astype(jnp.bfloat16)
    normed = matmul_norm(mid)
    hidden = jnp.dot(normed, w_up[...], preferred_element_type=jnp.float32)
    hidden = jnp.maximum(hidden, 0.0).astype(jnp.bfloat16)
    out = mid.astype(jnp.float32) + jnp.dot(
        hidden, w_down[...], preferred_element_type=jnp.float32
    )
    updated[...] = out.astype(jnp.bfloat16).reshape(pair.shape)


def update_pair(pair, left, right, w_pairout, w_up, w_down):
    tile_rows, tile_cols, wide = pair.shape
    block = math.gcd(tile_rows, max(8, 1024 // tile_cols))
    tile = pl.BlockSpec((block, tile_cols, wide), lambda step: (step, 0, 0))

    def whole(array):
        return pl.BlockSpec(array.shape, lambda step: (0, 0))

    return pl.pallas_call(
        pair_kernel,
        out_shape=jax.ShapeDtypeStruct(pair.shape, jnp.bfloat16),
        grid=(tile_rows // block,),
        in_specs=[
            tile,
            pl.BlockSpec((block, wide), lambda step: (step, 0)),
            whole(right),
            whole(w_pairout),
            whole(w_up),
            whole(w_down),
        ],
        out_specs=tile,
        name="update_pair",
    )(pair, left, right, w_pairout, w_up, w_down)


def layer_norm(values):
    values = values.astype(jnp.float32)
    centred = values - jnp.mean(values, -1, keepdims=True)
    return centred * lax.rsqrt(jnp.mean(centred * centred, -1, keepdims=True) + epsilon)


def per_device(
    row_size, col_size,
    single, pair, residue_mask, w_bias, w_project, w_out, w_factors, w_pairout, w_up, w_down
):
    tile_rows = pair.shape[0]
    tile_cols = pair.shape[1]
    normed_pair = norm_rows(
        pair.reshape(tile_rows * tile_cols, pair.shape[2]), math.gcd(tile_rows * tile_cols, 1024)
    ).reshape(pair.shape)
    bias_local = jnp.einsum(
        "rcp,ph->hrc", normed_pair, w_bias, preferred_element_type=jnp.float32
    ).astype(jnp.bfloat16)
    normed_single = layer_norm(single).astype(jnp.bfloat16)
    projected = jnp.einsum(
        "rs,fsc->frc", normed_single, w_project, preferred_element_type=jnp.float32
    )
    query_rows = projected[0].astype(jnp.bfloat16)
    key_local = projected[1].astype(jnp.bfloat16)
    value_local = projected[2].astype(jnp.bfloat16)
    gate_values = jax.nn.sigmoid(projected[3])
    bias_heads = lax.all_to_all(bias_local, "cols", split_axis=0, concat_axis=2, tiled=True)
    both = gather(jnp.concatenate([key_local, value_local], 1), "rows", row_size, 1)
    both = both.reshape(row_size * tile_rows, both.shape[2])
    key_rows, value_rows = both[:, : key_local.shape[1]], both[:, key_local.shape[1] :]
    heads_here = bias_heads.shape[0]
    head_width = query_rows.shape[1] // heads_here
    residues = key_rows.shape[0]
    query_split = query_rows.reshape(tile_rows, heads_here, head_width)
    key_split = key_rows.reshape(residues, heads_here, head_width)
    value_split = value_rows.reshape(residues, heads_here, head_width)
    score_scale = 1.0 / math.sqrt(head_width)
    scores = jnp.einsum(
        "rhd,lhd->hrl", query_split, key_split, preferred_element_type=jnp.float32
    ) * score_scale + bias_heads.astype(jnp.float32)
    key_valid = (residue_mask > 0)[None, None, :]
    scores = jnp.where(key_valid, scores, -jnp.inf)
    weights = jax.nn.softmax(scores, axis=-1).astype(jnp.bfloat16)
    attended = jnp.einsum("hrl,lhd->rhd", weights, value_split, preferred_element_type=jnp.float32)
    attended = attended.reshape(tile_rows, heads_here * head_width)
    mixed = (attended * gate_values).astype(jnp.bfloat16)
    single_out, left, right = update_single(
        mixed, single, w_out, w_factors, row_size, col_size, tile_cols
    )
    return (single_out, update_pair(pair, left, right, w_pairout, w_up, w_down))


LANES = 128
excluded = -1e30


def lane_iota(shape):
    return lax.broadcasted_iota(jnp.int32, shape, len(shape) - 1)


def block_constants(wide, copies):
    size = wide * copies
    row = lax.broadcasted_iota(jnp.int32, (size, size), 0)
    col = lax.broadcasted_iota(jnp.int32, (size, size), 1)
    same = row // wide == col // wide
    share = jnp.where(same, 1.0 / wide, 0.0)
    centre = jnp.where(row == col, 1.0, 0.0) - share
    return centre.astype(jnp.bfloat16), share.astype(jnp.bfloat16)


def norm_centred(values, centre, share):
    centred = jnp.dot(values, centre, preferred_element_type=jnp.float32)
    square = centred * centred
    high = square.astype(jnp.bfloat16)
    low = (square - high.astype(jnp.float32)).astype(jnp.bfloat16)
    spread_out = jnp.dot(high, share, preferred_element_type=jnp.float32)
    spread_out = spread_out + jnp.dot(low, share, preferred_element_type=jnp.float32)
    return (centred * lax.rsqrt(spread_out + epsilon)).astype(jnp.bfloat16)


def attend_kernel(
    row_size, col_size, heads, tile_cols, stride,
    single, pair, mask, w_bias, w_project, w_out, w_factors,
    single_out, left_out, right_out,
    single_v, pair_v, mask_v, bias_w, project_v, out_v, factors_v, own_single,
    kv_send, kv_recv, q_recv, gate_send, gate_recv, bias_v, o_send, o_recv,
    st_send, st_recv, left_send, right_send, left_recv, right_recv, so_send, consts, spread_v,
    load_sems, pair_sems, col_send, col_recv, fan_send, fan_recv,
):
    me_row = lax.axis_index("rows")
    me_col = lax.axis_index("cols")
    total = row_size * col_size
    barrier = pltpu.get_barrier_semaphore()
    me = me_row * col_size + me_col
    for step in range(1, total):
        to = lax.rem(me + step, total)
        pl.semaphore_signal(
            barrier,
            inc=1,
            device_id={"rows": to // col_size, "cols": lax.rem(to, col_size)},
            device_id_type=pl.DeviceIdType.MESH,
        )
    halves, depth, _, wide = pair.shape
    tile_rows, width = single.shape
    group = w_project.shape[2]
    rows_each = depth // col_size
    heads_here = heads // col_size
    head_width = group // heads_here
    chunk = depth // pair_sems.shape[0]
    loads = [
        pltpu.make_async_copy(source, target, load_sems.at[index])
        for index, (source, target) in enumerate(
            [(single, single_v)]
            + [(w_project.at[part], project_v.at[part]) for part in (1, 2, 0, 3)]
            + [(w_bias, bias_w), (mask, mask_v)]
            + [
                (single.at[pl.ds(half * depth + me_col * rows_each, rows_each)], own_single.at[half])
                for half in range(halves)
            ]
            + [(w_out, out_v), (w_factors, factors_v)]
        )
    ]
    for copy in loads[:7]:
        copy.start()

    def pair_load(step):
        part = pl.ds(step * chunk, chunk)
        return pltpu.make_async_copy(pair.at[:, part], pair_v.at[:, part], pair_sems.at[step])

    for step in range(depth // chunk):
        pair_load(step).start()
    for copy in loads[7:]:
        copy.start()

    centre, share = block_constants(wide, halves)
    consts[0] = centre
    consts[1] = share

    def to_cols(kind, source_of, target):
        copies = []
        for step in range(1, col_size):
            to = lax.rem(me_col + step, col_size)
            copy = pltpu.make_async_remote_copy(
                src_ref=source_of(to),
                dst_ref=target,
                send_sem=col_send.at[kind, step - 1],
                recv_sem=col_recv.at[kind, step - 1],
                device_id={"cols": to},
                device_id_type=pl.DeviceIdType.MESH,
            )
            copy.start()
            copies.append(copy)
        return copies

    owner = me_col // halves
    mine = owner == me_row
    half_mine = lax.rem(me_col, halves)

    def fan_copies(kind, source_of, target):
        copies = []
        for step in range(row_size):
            for half in range(halves):
                to = halves * me_row + half
                copy = pltpu.make_async_remote_copy(
                    src_ref=source_of(half),
                    dst_ref=target.at[me_col],
                    send_sem=fan_send.at[kind, step * halves + half],
                    recv_sem=fan_recv.at[kind, me_col],
                    device_id={"rows": lax.rem(me_row + step, row_size), "cols": to},
                    device_id_type=pl.DeviceIdType.MESH,
                )
                copies.append((copy, step, to))
        return copies

    def on_fan(copies, act):
        for copy, step, to in copies:
            if step:
                act(copy)
            else:
                pl.when(to != me_col)(functools.partial(act, copy))

    def fan_wait(kind, source_of, target):
        for part in range(col_size):
            copy = pltpu.make_async_remote_copy(
                src_ref=source_of(0),
                dst_ref=target.at[part],
                send_sem=fan_send.at[kind, 0],
                recv_sem=fan_recv.at[kind, part],
                device_id={"rows": lax.rem(me_row + 1, row_size)},
                device_id_type=pl.DeviceIdType.MESH,
            )
            pl.when(jnp.logical_not(jnp.logical_and(mine, part == me_col)))(copy.wait_recv)

    loads[0].wait()
    normed = layer_norm(single_v[...]).astype(jnp.bfloat16)
    loads[1].wait()
    loads[2].wait()
    key_value = jnp.dot(
        normed,
        jnp.concatenate([project_v[1], project_v[2]], axis=1),
        preferred_element_type=jnp.float32,
    ).astype(jnp.bfloat16)
    for half in range(halves):
        for kind in range(2):
            kv_send[half, kind] = key_value[
                half * tile_cols : (half + 1) * tile_cols, kind * group : (kind + 1) * group
            ]
    pl.semaphore_wait(barrier, total - 1)
    kv_copies = fan_copies(0, lambda half: kv_send.at[half], kv_recv)
    on_fan(kv_copies, lambda copy: copy.start())

    @pl.when(mine)
    def _():
        kv_recv[me_col] = kv_send[half_mine]

    loads[3].wait()
    loads[4].wait()
    query_gate = jnp.dot(
        normed,
        jnp.concatenate([project_v[0], project_v[3]], axis=1),
        preferred_element_type=jnp.float32,
    )
    q_recv[me_col] = query_gate[:, :group].astype(jnp.bfloat16)
    q_copies = to_cols(0, lambda to: q_recv.at[me_col], q_recv.at[me_col])
    gate_send[...] = jax.nn.sigmoid(query_gate[:, group:]).reshape(halves, depth, group)

    def own_rows(to):
        return pl.ds(pl.multiple_of(to * rows_each, rows_each), rows_each)

    gate_copies = to_cols(1, lambda to: gate_send.at[:, own_rows(to)], gate_recv.at[me_col])
    gate_recv[me_col] = gate_send[:, own_rows(me_col)]

    loads[5].wait()
    loads[6].wait()

    def bias_step(step, _):
        pair_load(step).wait()
        parts = [
            pair_v[half, pl.ds(step * chunk, chunk)].reshape(chunk * tile_cols, wide)
            for half in range(halves)
        ]
        normed_pair = norm_centred(jnp.concatenate(parts, axis=1), consts[0], consts[1])
        parts = [
            normed_pair[:, half * wide : (half + 1) * wide].reshape(chunk, 1, tile_cols, wide)
            for half in range(halves)
        ]
        normed_pair = jnp.concatenate(parts, axis=1).reshape(chunk * halves * tile_cols, wide)
        bias = lax.dot_general(
            bias_w[...], normed_pair, (((1,), (1,)), ((), ())), preferred_element_type=jnp.float32
        )
        bias = bias.astype(jnp.bfloat16).astype(jnp.float32)
        for part in range(chunk):
            bias_v[pl.ds(step * chunk + part, heads, stride=stride), :] = bias[
                :, part * LANES : (part + 1) * LANES
            ]
        return 0

    lax.fori_loop(0, depth // chunk, bias_step, 0)

    lane_row = lane_iota((2 * halves * heads, width))
    place = lax.broadcasted_iota(jnp.int32, (2 * halves * heads, width), 0)
    for half in range(halves):
        picked = jnp.where(place == half * heads + lane_row // head_width, 1.0, 0.0)
        spread_v[half, :LANES] = picked.astype(jnp.bfloat16)
        spread_v[half, LANES:] = picked.astype(jnp.bfloat16)

    fan_wait(0, lambda half: kv_send.at[half], kv_recv)
    for copy in q_copies:
        copy.wait_recv()

    length = jnp.sum(jnp.sum(mask_v[...], axis=1, keepdims=True), axis=0, keepdims=True)
    lane = lane_iota((depth, LANES))
    low = lane < tile_cols
    valid = me_col * tile_cols + lax.rem(lane, tile_cols) < length
    head_of = lane_iota((tile_cols, group)) // head_width
    head_masks = [
        jnp.where(head_of == head, 1.0, 0.0).astype(jnp.bfloat16) for head in range(heads_here)
    ]
    zeros = jnp.zeros((tile_cols, group), jnp.bfloat16)
    scale = 1.0 / math.sqrt(head_width)
    st_send[...] = jnp.zeros_like(st_send)
    block_place = lax.broadcasted_iota(jnp.int32, (heads_here * LANES, LANES), 0) // tile_cols
    block_target = (
        halves * heads + lax.rem(block_place, halves) * heads + block_place // halves
    )
    block_lane = lane_iota((heads_here * LANES, LANES))

    def attend_step(part, _):
        query = q_recv[part]
        query = jnp.concatenate([query[:depth], query[depth:]], axis=1)
        key, value = kv_recv[part, 0], kv_recv[part, 1]
        weights, value_rows = [], []
        stats = st_send[...]
        for first in range(0, heads_here, 2):
            key_rows = []
            for head in (first, first + 1):
                masked = key * head_masks[head]
                key_rows.append(jnp.concatenate([masked, zeros], axis=1))
                key_rows.append(jnp.concatenate([zeros, masked], axis=1))
            raw = lax.dot_general(
                query,
                jnp.concatenate(key_rows, axis=0),
                (((1,), (1,)), ((), ())),
                preferred_element_type=jnp.float32,
            )
            for head in (first, first + 1):
                index = part * heads_here + head
                bias = bias_v[pl.ds(pl.multiple_of(index * stride, 8), depth), :]
                scores = raw[:, (head - first) * LANES : (head - first + 1) * LANES] * scale + bias
                scores = jnp.where(valid, scores, excluded)
                top0 = jnp.max(jnp.where(low, scores, excluded), axis=1, keepdims=True)
                top1 = jnp.max(jnp.where(low, excluded, scores), axis=1, keepdims=True)
                weights.append(
                    jnp.exp(scores - jnp.where(low, top0, top1)).astype(jnp.bfloat16)
                )
                stats = jnp.where(lane == index, top0, stats)
                stats = jnp.where(lane == heads + index, top1, stats)
        for head in range(heads_here):
            masked = value * head_masks[head]
            value_rows.append(jnp.concatenate([masked, zeros], axis=1))
            value_rows.append(jnp.concatenate([zeros, masked], axis=1))
        weights = jnp.concatenate(weights, axis=1)
        mixed = jnp.dot(
            weights, jnp.concatenate(value_rows, axis=0), preferred_element_type=jnp.float32
        )
        ones = jnp.where(block_lane == block_target + part * heads_here, 1.0, 0.0)
        sums = jnp.dot(weights, ones.astype(jnp.bfloat16), preferred_element_type=jnp.float32)
        st_send[...] = stats + sums
        pieces = [
            mixed[:, half * group : (half + 1) * group].reshape(col_size, rows_each, group)
            for half in range(halves)
        ]
        o_send[:, :, pl.ds(pl.multiple_of(part * group, group), group)] = jnp.concatenate(
            pieces, axis=1
        ).astype(jnp.bfloat16)
        return 0

    lax.fori_loop(0, col_size, attend_step, 0)

    st_copies = to_cols(2, lambda to: st_send.at[own_rows(to)], st_recv.at[me_col])
    o_copies = to_cols(3, lambda to: o_send.at[to], o_recv.at[me_col])
    st_recv[me_col] = st_send[own_rows(me_col)]
    o_recv[me_col] = o_send[me_col]
    for copy in gate_copies + st_copies:
        copy.wait_recv()
    stats = st_recv[...]
    lane = lane_iota(stats.shape)
    top = jnp.max(stats, axis=0, keepdims=True)
    factor = jnp.exp(stats - top)
    sums = jnp.sum(factor * pltpu.roll(stats, halves * heads, axis=2), axis=0, keepdims=True)
    factor = jnp.where(lane < halves * heads, factor / sums, 0.0)
    factor = factor.reshape(col_size * rows_each, LANES)
    high = factor.astype(jnp.bfloat16)
    rest = (factor - high.astype(jnp.float32)).astype(jnp.bfloat16)
    factor = jnp.concatenate([high, rest], axis=1)
    scales = [
        jnp.dot(factor, spread_v[half], preferred_element_type=jnp.float32) for half in range(halves)
    ]
    gate = jnp.concatenate(
        [gate_recv[part].reshape(halves * rows_each, group) for part in range(col_size)], axis=1
    )
    for copy in o_copies:
        copy.wait_recv()
    attended = jnp.zeros((halves * rows_each, width), jnp.float32)
    for part in range(col_size):
        rows = slice(part * rows_each, (part + 1) * rows_each)
        part_scale = jnp.concatenate([scales[half][rows] for half in range(halves)], axis=0)
        attended = attended + part_scale * o_recv[part].astype(jnp.float32)
    mixed = (attended * gate).astype(jnp.bfloat16)
    for copy in loads[7:]:
        copy.wait()
    added = jnp.dot(mixed, out_v[...], preferred_element_type=jnp.float32)
    own = own_single[...].astype(jnp.float32).reshape(halves * rows_each, width)
    updated = (own + added).astype(jnp.bfloat16)
    so_send[...] = updated.astype(jnp.float32).reshape(halves, rows_each, width).astype(jnp.bfloat16)
    factors = jnp.dot(
        layer_norm(updated).astype(jnp.bfloat16),
        factors_v[...],
        preferred_element_type=jnp.float32,
    )
    factors = factors.astype(jnp.bfloat16).astype(jnp.float32)
    first, second = factors[:rows_each], factors[rows_each:]
    shift = factors.shape[1] // 2
    low = lane_iota(first.shape) < shift
    left = jnp.where(low, first, pltpu.roll(second, shift, axis=1))
    right = jnp.where(low, pltpu.roll(first, shift, axis=1), second)
    left_send[...] = left
    right_send[...] = right
    right_copies = fan_copies(1, lambda half: right_send, right_recv)
    on_fan(right_copies, lambda copy: copy.start())
    left_copies = to_cols(4, lambda to: left_send, left_recv.at[me_col])
    so_copies = to_cols(5, lambda to: so_send, single_out.at[:, me_col])
    own_copy = pltpu.make_async_copy(so_send, single_out.at[:, me_col], load_sems.at[0])
    own_copy.start()
    left_recv[me_col] = left

    @pl.when(mine)
    def _():
        right_recv[me_col] = right_send[...]

    fan_wait(1, lambda half: right_send, right_recv)
    for copy in left_copies:
        copy.wait_recv()
    left = left_recv[...].reshape(depth, LANES)
    turned = pltpu.roll(left, shift, axis=1)
    low = lane_iota(left.shape) < shift
    left_out[:depth] = jnp.where(low, left, turned)
    left_out[depth:] = jnp.where(low, turned, left)
    right = right_recv[...].reshape(tile_cols, LANES)
    turned = pltpu.roll(right, shift, axis=1)
    right_out[...] = jnp.where(lane_iota(right.shape) // shift == half_mine, right, turned)

    for copies in (q_copies, gate_copies, st_copies, o_copies, left_copies, so_copies):
        for copy in copies:
            copy.wait_send()
    on_fan(kv_copies, lambda copy: copy.wait_send())
    on_fan(right_copies, lambda copy: copy.wait_send())
    for copy in so_copies:
        copy.wait_recv()
    own_copy.wait()


def attend(single, pair, mask, w_bias, w_project, w_out, w_factors, row_size, col_size):
    tile_rows, tile_cols, wide = pair.shape
    width = single.shape[1]
    heads = w_bias.shape[1]
    halves = tile_rows // tile_cols
    depth = tile_rows // halves
    rows_each = depth // col_size
    group = w_project.shape[2]
    steps = 8
    stride = depth + 8
    any_spec = pl.BlockSpec(memory_space=pl.ANY)
    vmem_spec = pl.BlockSpec(memory_space=pltpu.VMEM)
    bf16, f32 = jnp.bfloat16, jnp.float32
    single_out, left, right = pl.pallas_call(
        functools.partial(attend_kernel, row_size, col_size, heads, tile_cols, stride),
        out_shape=(
            jax.ShapeDtypeStruct((halves, col_size, rows_each, width), bf16),
            jax.ShapeDtypeStruct((tile_rows, wide), f32),
            jax.ShapeDtypeStruct((tile_cols, wide), f32),
        ),
        in_specs=[any_spec] * 7,
        out_specs=[any_spec, vmem_spec, vmem_spec],
        scratch_shapes=[
            pltpu.VMEM((tile_rows, width), bf16),
            pltpu.VMEM((halves, depth, tile_cols, wide), bf16),
            pltpu.VMEM((mask.shape[0] // LANES, LANES), jnp.int32),
            pltpu.VMEM((heads, wide), bf16),
            pltpu.VMEM(w_project.shape, bf16),
            pltpu.VMEM(w_out.shape, bf16),
            pltpu.VMEM(w_factors.shape, bf16),
            pltpu.VMEM((halves, rows_each, width), bf16),
            pltpu.VMEM((halves, 2, tile_cols, group), bf16),
            pltpu.VMEM((col_size, 2, tile_cols, group), bf16),
            pltpu.VMEM((col_size, tile_rows, group), bf16),
            pltpu.VMEM((halves, depth, group), f32),
            pltpu.VMEM((col_size, halves, rows_each, group), f32),
            pltpu.VMEM((heads * stride, LANES), f32),
            pltpu.VMEM((col_size, halves * rows_each, width), bf16),
            pltpu.VMEM((col_size, halves * rows_each, width), bf16),
            pltpu.VMEM((depth, LANES), f32),
            pltpu.VMEM((col_size, rows_each, LANES), f32),
            pltpu.VMEM((rows_each, LANES), f32),
            pltpu.VMEM((rows_each, LANES), f32),
            pltpu.VMEM((col_size, rows_each, LANES), f32),
            pltpu.VMEM((col_size, rows_each, LANES), f32),
            pltpu.VMEM((halves, rows_each, width), bf16),
            pltpu.VMEM((2, halves * wide, halves * wide), bf16),
            pltpu.VMEM((halves, 2 * LANES, width), bf16),
            pltpu.SemaphoreType.DMA((9 + halves,)),
            pltpu.SemaphoreType.DMA((steps,)),
            pltpu.SemaphoreType.DMA((6, col_size - 1)),
            pltpu.SemaphoreType.DMA((6, col_size - 1)),
            pltpu.SemaphoreType.DMA((2, row_size * halves)),
            pltpu.SemaphoreType.DMA((2, col_size)),
        ],
        compiler_params=pltpu.CompilerParams(collective_id=3, has_side_effects=True),
        name="attend",
    )(
        single,
        pair.reshape(halves, depth, tile_cols, wide),
        mask.reshape(mask.shape[0] // LANES, LANES),
        w_bias.T,
        w_project,
        w_out,
        w_factors,
    )
    return single_out.reshape(tile_rows, width), left, right


def fits(row_size, col_size, single, pair, mask, w_bias, w_project, w_factors):
    tile_rows, tile_cols, wide = pair.shape
    heads = w_bias.shape[1]
    return (
        tile_rows == 2 * tile_cols
        and 2 * tile_cols == LANES
        and wide == LANES
        and w_factors.shape[1] == LANES
        and w_project.shape[2] == LANES
        and 4 * heads == LANES
        and heads % (2 * col_size) == 0
        and tile_cols % (8 * col_size) == 0
        and col_size == 2 * row_size
        and mask.shape[0] % LANES == 0
    )


def per_device_keys(
    row_size, col_size,
    single, pair, residue_mask, w_bias, w_project, w_out, w_factors, w_pairout, w_up, w_down
):
    single_out, left, right = attend(
        single, pair, residue_mask, w_bias, w_project, w_out, w_factors, row_size, col_size
    )
    return (single_out, update_pair(pair, left, right, w_pairout, w_up, w_down))


def dispatch(row_size, col_size, *arrays):
    single, pair, residue_mask, w_bias, w_project, w_out, w_factors = arrays[:7]
    if fits(row_size, col_size, single, pair, residue_mask, w_bias, w_project, w_factors):
        return per_device_keys(row_size, col_size, *arrays)
    return per_device(row_size, col_size, *arrays)


def solution(mesh):
    return jax.shard_map(
        functools.partial(dispatch, mesh.shape["rows"], mesh.shape["cols"]),
        mesh=mesh,
        in_specs=(
            P("rows", None),
            P("rows", "cols", None),
            P(),
            P(),
            P(None, None, "cols"),
            P(),
            P(),
            P(),
            P(),
            P(),
        ),
        out_specs=(P("rows", None), P("rows", "cols", None)),
        check_vma=False,
    )
```

```python
import functools
import math

import jax
import jax.numpy as jnp
from jax import lax
from jax.experimental import pallas as pl
from jax.experimental.pallas import tpu as pltpu
from jax.sharding import PartitionSpec as P

epsilon = 1e-05


def enter(axes):
    barrier = pltpu.get_barrier_semaphore()
    total = 0
    for axis, size in axes:
        me = lax.axis_index(axis)
        for step in range(1, size):
            pl.semaphore_signal(
                barrier,
                inc=1,
                device_id={axis: lax.rem(me + step, size)},
                device_id_type=pl.DeviceIdType.MESH,
            )
        total += size - 1
    pl.semaphore_wait(barrier, total)


def spread(axis, size, source, landing, send_sems, recv_sems):
    me = lax.axis_index(axis)
    copies = []
    for step in range(1, size):
        copy = pltpu.make_async_remote_copy(
            src_ref=source,
            dst_ref=landing.at[me],
            send_sem=send_sems.at[step - 1],
            recv_sem=recv_sems.at[step - 1],
            device_id={axis: lax.rem(me + step, size)},
            device_id_type=pl.DeviceIdType.MESH,
        )
        copy.start()
        copies.append(copy)
    return copies


def gather_kernel(axis, size, source, gathered, send_sems, recv_sems, own_sem):
    enter([(axis, size)])
    copies = spread(axis, size, source, gathered, send_sems, recv_sems)
    own = pltpu.make_async_copy(source, gathered.at[lax.axis_index(axis)], own_sem)
    own.start()
    own.wait()
    for copy in copies:
        copy.wait()


def gather(values, axis, size, collective_id):
    return pl.pallas_call(
        functools.partial(gather_kernel, axis, size),
        out_shape=jax.ShapeDtypeStruct((size, *values.shape), values.dtype),
        in_specs=[pl.BlockSpec(memory_space=pltpu.VMEM)],
        out_specs=pl.BlockSpec(memory_space=pltpu.VMEM),
        scratch_shapes=[
            pltpu.SemaphoreType.DMA((size - 1,)),
            pltpu.SemaphoreType.DMA((size - 1,)),
            pltpu.SemaphoreType.DMA,
        ],
        compiler_params=pltpu.CompilerParams(collective_id=collective_id, has_side_effects=True),
        name="gather_" + axis,
    )(values)


def single_kernel(
    row_size, col_size, tile_cols,
    mixed, single, w_out, w_factors, single_out, left_out, right_out,
    gathered, factor_right, send_sems, recv_sems, row_send, row_recv, own_sem,
):
    enter([("cols", col_size), ("rows", row_size)])
    tile_rows, width = mixed.shape
    me_col = lax.axis_index("cols")
    me_row = lax.axis_index("rows")
    copies = spread("cols", col_size, mixed, gathered, send_sems, recv_sems)
    own = pltpu.make_async_copy(mixed, gathered.at[me_col], own_sem)
    own.start()
    own.wait()
    for copy in copies:
        copy.wait()
    whole = jnp.concatenate([gathered[part] for part in range(col_size)], axis=1)
    total = jnp.dot(whole, w_out[...], preferred_element_type=jnp.float32)
    updated = (single[...].astype(jnp.float32) + total).astype(jnp.bfloat16)
    single_out[...] = updated
    normed = layer_norm(updated).astype(jnp.bfloat16)
    factors = jnp.dot(normed, w_factors[...], preferred_element_type=jnp.float32)
    factors = factors.astype(jnp.bfloat16).astype(jnp.float32)
    half = factors.shape[1] // 2
    swapped = jnp.concatenate([factors[:, half:], factors[:, :half]], axis=1)
    lower = lax.broadcasted_iota(jnp.int32, factors.shape, 1) < half
    left_out[...] = jnp.where(lower, factors, swapped)
    factor_right[...] = jnp.where(lower, swapped, factors).astype(jnp.bfloat16)
    first = me_col * tile_cols
    owner = first // tile_rows
    offset = pl.multiple_of(first - owner * tile_rows, tile_cols)
    piece = factor_right.at[pl.ds(offset, tile_cols)]

    @pl.when(me_row == owner)
    def _():
        local = pltpu.make_async_copy(piece, right_out, own_sem)
        local.start()
        sends = []
        for step in range(1, row_size):
            send = pltpu.make_async_remote_copy(
                src_ref=piece,
                dst_ref=right_out,
                send_sem=row_send.at[step - 1],
                recv_sem=row_recv,
                device_id={"rows": lax.rem(me_row + step, row_size)},
                device_id_type=pl.DeviceIdType.MESH,
            )
            send.start()
            sends.append(send)
        local.wait()
        for send in sends:
            send.wait_send()

    @pl.when(me_row != owner)
    def _():
        pltpu.make_async_remote_copy(
            src_ref=piece,
            dst_ref=right_out,
            send_sem=row_send.at[0],
            recv_sem=row_recv,
            device_id={"rows": lax.rem(me_row + 1, row_size)},
            device_id_type=pl.DeviceIdType.MESH,
        ).wait_recv()


def update_single(mixed, single, w_out, w_factors, row_size, col_size, tile_cols):
    tile_rows, width = single.shape
    wide = w_factors.shape[1]
    return pl.pallas_call(
        functools.partial(single_kernel, row_size, col_size, tile_cols),
        out_shape=(
            jax.ShapeDtypeStruct((tile_rows, width), jnp.bfloat16),
            jax.ShapeDtypeStruct((tile_rows, wide), jnp.float32),
            jax.ShapeDtypeStruct((tile_cols, wide), jnp.bfloat16),
        ),
        in_specs=[pl.BlockSpec(memory_space=pltpu.VMEM)] * 4,
        out_specs=[pl.BlockSpec(memory_space=pltpu.VMEM)] * 3,
        scratch_shapes=[
            pltpu.VMEM((col_size, *mixed.shape), jnp.bfloat16),
            pltpu.VMEM((tile_rows, wide), jnp.bfloat16),
            pltpu.SemaphoreType.DMA((col_size - 1,)),
            pltpu.SemaphoreType.DMA((col_size - 1,)),
            pltpu.SemaphoreType.DMA((row_size - 1,)),
            pltpu.SemaphoreType.DMA,
            pltpu.SemaphoreType.DMA,
        ],
        compiler_params=pltpu.CompilerParams(collective_id=2, has_side_effects=True),
        name="update_single",
    )(mixed, single, w_out, w_factors)


def matmul_norm(values):
    wide = values.shape[1]
    share = jnp.full((2 * wide, wide), 1.0 / wide, jnp.bfloat16)
    mean = jnp.dot(values, share[:wide], preferred_element_type=jnp.float32)
    centred = values.astype(jnp.float32) - mean
    square = centred * centred
    high = square.astype(jnp.bfloat16)
    low = (square - high.astype(jnp.float32)).astype(jnp.bfloat16)
    spread_out = jnp.dot(
        jnp.concatenate([high, low], 1), share, preferred_element_type=jnp.float32
    )
    return (centred * lax.rsqrt(spread_out + epsilon)).astype(jnp.bfloat16)


def norm_kernel(values, normed):
    normed[...] = matmul_norm(values[...])


def norm_rows(values, block):
    spec = pl.BlockSpec((block, values.shape[1]), lambda step: (step, 0))
    return pl.pallas_call(
        norm_kernel,
        out_shape=jax.ShapeDtypeStruct(values.shape, jnp.bfloat16),
        grid=(values.shape[0] // block,),
        in_specs=[spec],
        out_specs=spec,
        name="norm_pair",
    )(values)


def pair_kernel(pair, left, right, w_pairout, w_up, w_down, updated):
    block_rows, tile_cols, wide = pair.shape
    left_wide = left[...][:, None, :]
    right_wide = right[...].astype(jnp.float32)[None, :, :]
    lower = lax.broadcasted_iota(jnp.int32, pair.shape, 2) < wide // 2
    paired = jnp.where(lower, left_wide * right_wide, left_wide - right_wide)
    paired = paired.astype(jnp.bfloat16).reshape(block_rows * tile_cols, wide)
    flat = pair[...].reshape(block_rows * tile_cols, wide).astype(jnp.float32)
    mid = flat + jnp.dot(paired, w_pairout[...], preferred_element_type=jnp.float32)
    mid = mid.astype(jnp.bfloat16)
    normed = matmul_norm(mid)
    hidden = jnp.dot(normed, w_up[...], preferred_element_type=jnp.float32)
    hidden = jnp.maximum(hidden, 0.0).astype(jnp.bfloat16)
    out = mid.astype(jnp.float32) + jnp.dot(
        hidden, w_down[...], preferred_element_type=jnp.float32
    )
    updated[...] = out.astype(jnp.bfloat16).reshape(pair.shape)


def update_pair(pair, left, right, w_pairout, w_up, w_down):
    tile_rows, tile_cols, wide = pair.shape
    block = math.gcd(tile_rows, max(8, 1024 // tile_cols))
    tile = pl.BlockSpec((block, tile_cols, wide), lambda step: (step, 0, 0))

    def whole(array):
        return pl.BlockSpec(array.shape, lambda step: (0, 0))

    return pl.pallas_call(
        pair_kernel,
        out_shape=jax.ShapeDtypeStruct(pair.shape, jnp.bfloat16),
        grid=(tile_rows // block,),
        in_specs=[
            tile,
            pl.BlockSpec((block, wide), lambda step: (step, 0)),
            whole(right),
            whole(w_pairout),
            whole(w_up),
            whole(w_down),
        ],
        out_specs=tile,
        name="update_pair",
    )(pair, left, right, w_pairout, w_up, w_down)


def layer_norm(values):
    values = values.astype(jnp.float32)
    centred = values - jnp.mean(values, -1, keepdims=True)
    return centred * lax.rsqrt(jnp.mean(centred * centred, -1, keepdims=True) + epsilon)


def per_device(
    row_size, col_size,
    single, pair, residue_mask, w_bias, w_project, w_out, w_factors, w_pairout, w_up, w_down
):
    tile_rows = pair.shape[0]
    tile_cols = pair.shape[1]
    normed_pair = norm_rows(
        pair.reshape(tile_rows * tile_cols, pair.shape[2]), math.gcd(tile_rows * tile_cols, 1024)
    ).reshape(pair.shape)
    bias_local = jnp.einsum(
        "rcp,ph->hrc", normed_pair, w_bias, preferred_element_type=jnp.float32
    ).astype(jnp.bfloat16)
    normed_single = layer_norm(single).astype(jnp.bfloat16)
    projected = jnp.einsum(
        "rs,fsc->frc", normed_single, w_project, preferred_element_type=jnp.float32
    )
    query_rows = projected[0].astype(jnp.bfloat16)
    key_local = projected[1].astype(jnp.bfloat16)
    value_local = projected[2].astype(jnp.bfloat16)
    gate_values = jax.nn.sigmoid(projected[3])
    bias_heads = lax.all_to_all(bias_local, "cols", split_axis=0, concat_axis=2, tiled=True)
    both = gather(jnp.concatenate([key_local, value_local], 1), "rows", row_size, 1)
    both = both.reshape(row_size * tile_rows, both.shape[2])
    key_rows, value_rows = both[:, : key_local.shape[1]], both[:, key_local.shape[1] :]
    heads_here = bias_heads.shape[0]
    head_width = query_rows.shape[1] // heads_here
    residues = key_rows.shape[0]
    query_split = query_rows.reshape(tile_rows, heads_here, head_width)
    key_split = key_rows.reshape(residues, heads_here, head_width)
    value_split = value_rows.reshape(residues, heads_here, head_width)
    score_scale = 1.0 / math.sqrt(head_width)
    scores = jnp.einsum(
        "rhd,lhd->hrl", query_split, key_split, preferred_element_type=jnp.float32
    ) * score_scale + bias_heads.astype(jnp.float32)
    key_valid = (residue_mask > 0)[None, None, :]
    scores = jnp.where(key_valid, scores, -jnp.inf)
    weights = jax.nn.softmax(scores, axis=-1).astype(jnp.bfloat16)
    attended = jnp.einsum("hrl,lhd->rhd", weights, value_split, preferred_element_type=jnp.float32)
    attended = attended.reshape(tile_rows, heads_here * head_width)
    mixed = (attended * gate_values).astype(jnp.bfloat16)
    single_out, left, right = update_single(
        mixed, single, w_out, w_factors, row_size, col_size, tile_cols
    )
    return (single_out, update_pair(pair, left, right, w_pairout, w_up, w_down))


LANES = 128
excluded = -1e30


def lane_iota(shape):
    return lax.broadcasted_iota(jnp.int32, shape, len(shape) - 1)


def block_constants(wide, copies):
    size = wide * copies
    row = lax.broadcasted_iota(jnp.int32, (size, size), 0)
    col = lax.broadcasted_iota(jnp.int32, (size, size), 1)
    same = row // wide == col // wide
    share = jnp.where(same, 1.0 / wide, 0.0)
    centre = jnp.where(row == col, 1.0, 0.0) - share
    return centre.astype(jnp.bfloat16), share.astype(jnp.bfloat16)


def norm_centred(values, centre, share):
    centred = jnp.dot(values, centre, preferred_element_type=jnp.float32)
    square = centred * centred
    high = square.astype(jnp.bfloat16)
    low = (square - high.astype(jnp.float32)).astype(jnp.bfloat16)
    spread_out = jnp.dot(high, share, preferred_element_type=jnp.float32)
    spread_out = spread_out + jnp.dot(low, share, preferred_element_type=jnp.float32)
    return (centred * lax.rsqrt(spread_out + epsilon)).astype(jnp.bfloat16)


def attend_kernel(
    row_size, col_size, heads, tile_cols, stride,
    single, pair, mask, w_bias, w_project, w_out, w_factors,
    single_out, left_out, right_out,
    single_v, pair_v, mask_v, bias_w, project_v, out_v, factors_v, own_single,
    kv_send, kv_recv, q_recv, gate_send, gate_recv, bias_v, o_send, o_recv,
    st_send, st_recv, left_send, right_send, left_recv, right_recv, so_send, consts, spread_v,
    load_sems, pair_sems, col_send, col_recv, fan_send, fan_recv,
    kv_sent, kv_came, kv_relayed, q_sent, q_came, o_sent, o_came,
):
    me_row = lax.axis_index("rows")
    me_col = lax.axis_index("cols")
    total = row_size * col_size
    barrier = pltpu.get_barrier_semaphore()
    me = me_row * col_size + me_col
    for step in range(1, total):
        to = lax.rem(me + step, total)
        pl.semaphore_signal(
            barrier,
            inc=1,
            device_id={"rows": to // col_size, "cols": lax.rem(to, col_size)},
            device_id_type=pl.DeviceIdType.MESH,
        )
    halves, depth, _, wide = pair.shape
    tile_rows, width = single.shape
    group = w_project.shape[2]
    rows_each = depth // col_size
    heads_here = heads // col_size
    head_width = group // heads_here
    chunk = depth // pair_sems.shape[0]
    loads = [
        pltpu.make_async_copy(source, target, load_sems.at[index])
        for index, (source, target) in enumerate(
            [(single, single_v)]
            + [(w_project.at[part], project_v.at[part]) for part in (1, 2, 0, 3)]
            + [(w_bias, bias_w), (mask, mask_v)]
            + [
                (single.at[pl.ds(half * depth + me_col * rows_each, rows_each)], own_single.at[half])
                for half in range(halves)
            ]
            + [(w_out, out_v), (w_factors, factors_v)]
        )
    ]
    for copy in loads[:7]:
        copy.start()

    def pair_load(step):
        part = pl.ds(step * chunk, chunk)
        return pltpu.make_async_copy(pair.at[:, part], pair_v.at[:, part], pair_sems.at[step])

    for step in range(depth // chunk):
        pair_load(step).start()
    for copy in loads[7:]:
        copy.start()

    centre, share = block_constants(wide, halves)
    consts[0] = centre
    consts[1] = share

    def to_cols(kind, source_of, target):
        copies = []
        for step in range(1, col_size):
            to = lax.rem(me_col + step, col_size)
            copy = pltpu.make_async_remote_copy(
                src_ref=source_of(to),
                dst_ref=target,
                send_sem=col_send.at[kind, step - 1],
                recv_sem=col_recv.at[kind, step - 1],
                device_id={"cols": to},
                device_id_type=pl.DeviceIdType.MESH,
            )
            copy.start()
            copies.append(copy)
        return copies

    owner = me_col // halves
    mine = owner == me_row
    half_mine = lax.rem(me_col, halves)

    def fan_copies(kind, source_of, target):
        copies = []
        for step in range(row_size):
            for half in range(halves):
                to = halves * me_row + half
                copy = pltpu.make_async_remote_copy(
                    src_ref=source_of(half),
                    dst_ref=target.at[me_col],
                    send_sem=fan_send.at[kind, step * halves + half],
                    recv_sem=fan_recv.at[kind, me_col],
                    device_id={"rows": lax.rem(me_row + step, row_size), "cols": to},
                    device_id_type=pl.DeviceIdType.MESH,
                )
                copies.append((copy, step, to))
        return copies

    def on_some(copies, act):
        for copy, condition in copies:
            if condition is None:
                act(copy)
            else:
                pl.when(condition)(functools.partial(act, copy))

    kind_mine = lax.rem(me_row, 2)
    row_mate = me_row + 1 - 2 * kind_mine
    col_mate = me_col + 1 - 2 * lax.rem(me_col, 2)

    def relay_keys(part, kind, slot):
        return pltpu.make_async_remote_copy(
            src_ref=kv_recv.at[part, kind],
            dst_ref=kv_recv.at[part, kind],
            send_sem=kv_relayed.at[slot],
            recv_sem=kv_came.at[kind, part],
            device_id={"rows": row_mate},
            device_id_type=pl.DeviceIdType.MESH,
        )

    def send_query(part, to, slot):
        return pltpu.make_async_remote_copy(
            src_ref=q_recv.at[part],
            dst_ref=q_recv.at[part],
            send_sem=q_sent.at[slot],
            recv_sem=q_came.at[part],
            device_id={"cols": to},
            device_id_type=pl.DeviceIdType.MESH,
        )

    def on_fan(copies, act):
        for copy, step, to in copies:
            if step:
                act(copy)
            else:
                pl.when(to != me_col)(functools.partial(act, copy))

    def fan_wait(kind, source_of, target):
        for part in range(col_size):
            copy = pltpu.make_async_remote_copy(
                src_ref=source_of(0),
                dst_ref=target.at[part],
                send_sem=fan_send.at[kind, 0],
                recv_sem=fan_recv.at[kind, part],
                device_id={"rows": lax.rem(me_row + 1, row_size)},
                device_id_type=pl.DeviceIdType.MESH,
            )
            pl.when(jnp.logical_not(jnp.logical_and(mine, part == me_col)))(copy.wait_recv)

    loads[0].wait()
    normed = layer_norm(single_v[...]).astype(jnp.bfloat16)
    loads[1].wait()
    loads[2].wait()
    key_value = jnp.dot(
        normed,
        jnp.concatenate([project_v[1], project_v[2]], axis=1),
        preferred_element_type=jnp.float32,
    ).astype(jnp.bfloat16)
    for half in range(halves):
        for kind in range(2):
            kv_send[half, kind] = key_value[
                half * tile_cols : (half + 1) * tile_cols, kind * group : (kind + 1) * group
            ]
    pl.semaphore_wait(barrier, total - 1)
    kv_copies = []
    for step in range(row_size // 2):
        for kind in range(2):
            for half in range(halves):
                to = halves * me_row + half
                row = 2 * lax.rem(me_row // 2 + step, row_size // 2) + kind
                copy = pltpu.make_async_remote_copy(
                    src_ref=kv_send.at[half, kind],
                    dst_ref=kv_recv.at[me_col, kind],
                    send_sem=kv_sent.at[(step * 2 + kind) * halves + half],
                    recv_sem=kv_came.at[kind, me_col],
                    device_id={"rows": row, "cols": to},
                    device_id_type=pl.DeviceIdType.MESH,
                )
                here = jnp.logical_and(row == me_row, to == me_col)
                copies_of = (copy, None if step else jnp.logical_not(here))
                kv_copies.append(copies_of)
    on_some(kv_copies, lambda copy: copy.start())

    @pl.when(mine)
    def _():
        kv_recv[me_col, kind_mine] = kv_send[half_mine, kind_mine]

    loads[3].wait()
    loads[4].wait()
    query_gate = jnp.dot(
        normed,
        jnp.concatenate([project_v[0], project_v[3]], axis=1),
        preferred_element_type=jnp.float32,
    )
    q_recv[me_col] = query_gate[:, :group].astype(jnp.bfloat16)
    peers = [lax.rem(me_col + 2 * step, col_size) for step in range(1, col_size // 2)]
    mates = [lax.rem(col_mate + 2 * step, col_size) for step in range(1, col_size // 2)]
    q_copies = [send_query(me_col, to, slot) for slot, to in enumerate(peers)]
    q_copies.append(send_query(me_col, col_mate, len(peers)))
    for copy in q_copies:
        copy.start()
    gate_send[...] = jax.nn.sigmoid(query_gate[:, group:]).reshape(halves, depth, group)

    def own_rows(to):
        return pl.ds(pl.multiple_of(to * rows_each, rows_each), rows_each)

    gate_copies = to_cols(1, lambda to: gate_send.at[:, own_rows(to)], gate_recv.at[me_col])
    gate_recv[me_col] = gate_send[:, own_rows(me_col)]

    loads[5].wait()
    loads[6].wait()

    def bias_step(step, _):
        pair_load(step).wait()
        parts = [
            pair_v[half, pl.ds(step * chunk, chunk)].reshape(chunk * tile_cols, wide)
            for half in range(halves)
        ]
        normed_pair = norm_centred(jnp.concatenate(parts, axis=1), consts[0], consts[1])
        parts = [
            normed_pair[:, half * wide : (half + 1) * wide].reshape(chunk, 1, tile_cols, wide)
            for half in range(halves)
        ]
        normed_pair = jnp.concatenate(parts, axis=1).reshape(chunk * halves * tile_cols, wide)
        bias = lax.dot_general(
            bias_w[...], normed_pair, (((1,), (1,)), ((), ())), preferred_element_type=jnp.float32
        )
        bias = bias.astype(jnp.bfloat16).astype(jnp.float32)
        for part in range(chunk):
            bias_v[pl.ds(step * chunk + part, heads, stride=stride), :] = bias[
                :, part * LANES : (part + 1) * LANES
            ]
        return 0

    lax.fori_loop(0, depth // chunk, bias_step, 0)

    lane_row = lane_iota((2 * halves * heads, width))
    place = lax.broadcasted_iota(jnp.int32, (2 * halves * heads, width), 0)
    for half in range(halves):
        picked = jnp.where(place == half * heads + lane_row // head_width, 1.0, 0.0)
        spread_v[half, :LANES] = picked.astype(jnp.bfloat16)
        spread_v[half, LANES:] = picked.astype(jnp.bfloat16)

    relays = []
    for part in range(col_size):
        copy = relay_keys(part, kind_mine, part)
        pl.when(jnp.logical_not(jnp.logical_and(mine, part == me_col)))(copy.wait_recv)
        copy.start()
        relays.append(copy)
    for slot, peer in enumerate(peers):
        copy = send_query(peer, col_mate, col_size // 2 + slot)
        copy.wait_recv()
        copy.start()
        relays.append(copy)
    for part in range(col_size):
        relay_keys(part, 1 - kind_mine, part).wait_recv()
    for part in [col_mate] + mates:
        send_query(part, col_mate, 0).wait_recv()

    length = jnp.sum(jnp.sum(mask_v[...], axis=1, keepdims=True), axis=0, keepdims=True)
    lane = lane_iota((depth, LANES))
    low = lane < tile_cols
    valid = me_col * tile_cols + lax.rem(lane, tile_cols) < length
    head_of = lane_iota((tile_cols, group)) // head_width
    head_masks = [
        jnp.where(head_of == head, 1.0, 0.0).astype(jnp.bfloat16) for head in range(heads_here)
    ]
    zeros = jnp.zeros((tile_cols, group), jnp.bfloat16)
    scale = 1.0 / math.sqrt(head_width)
    st_send[...] = jnp.zeros_like(st_send)
    block_place = lax.broadcasted_iota(jnp.int32, (heads_here * LANES, LANES), 0) // tile_cols
    block_target = (
        halves * heads + lax.rem(block_place, halves) * heads + block_place // halves
    )
    block_lane = lane_iota((heads_here * LANES, LANES))

    def attend_part(part):
        query = q_recv[part]
        query = jnp.concatenate([query[:depth], query[depth:]], axis=1)
        key, value = kv_recv[part, 0], kv_recv[part, 1]
        weights, value_rows = [], []
        stats = st_send[...]
        for first in range(0, heads_here, 2):
            key_rows = []
            for head in (first, first + 1):
                masked = key * head_masks[head]
                key_rows.append(jnp.concatenate([masked, zeros], axis=1))
                key_rows.append(jnp.concatenate([zeros, masked], axis=1))
            raw = lax.dot_general(
                query,
                jnp.concatenate(key_rows, axis=0),
                (((1,), (1,)), ((), ())),
                preferred_element_type=jnp.float32,
            )
            for head in (first, first + 1):
                index = part * heads_here + head
                bias = bias_v[pl.ds(pl.multiple_of(index * stride, 8), depth), :]
                scores = raw[:, (head - first) * LANES : (head - first + 1) * LANES] * scale + bias
                scores = jnp.where(valid, scores, excluded)
                top0 = jnp.max(jnp.where(low, scores, excluded), axis=1, keepdims=True)
                top1 = jnp.max(jnp.where(low, excluded, scores), axis=1, keepdims=True)
                weights.append(
                    jnp.exp(scores - jnp.where(low, top0, top1)).astype(jnp.bfloat16)
                )
                stats = jnp.where(lane == index, top0, stats)
                stats = jnp.where(lane == heads + index, top1, stats)
        for head in range(heads_here):
            masked = value * head_masks[head]
            value_rows.append(jnp.concatenate([masked, zeros], axis=1))
            value_rows.append(jnp.concatenate([zeros, masked], axis=1))
        weights = jnp.concatenate(weights, axis=1)
        mixed = jnp.dot(
            weights, jnp.concatenate(value_rows, axis=0), preferred_element_type=jnp.float32
        )
        ones = jnp.where(block_lane == block_target + part * heads_here, 1.0, 0.0)
        sums = jnp.dot(weights, ones.astype(jnp.bfloat16), preferred_element_type=jnp.float32)
        st_send[...] = stats + sums
        pieces = [
            mixed[:, half * group : (half + 1) * group].reshape(col_size, rows_each, group)
            for half in range(halves)
        ]
        return jnp.concatenate(pieces, axis=1).astype(jnp.bfloat16)

    parts, _, _, part_width = o_send.shape
    each = part_width // group

    def o_copy(step, shift):
        to = lax.rem(me_col + shift, col_size)
        return pltpu.make_async_remote_copy(
            src_ref=o_send.at[step, to],
            dst_ref=o_recv.at[step, me_col],
            send_sem=o_sent.at[step, shift - 1],
            recv_sem=o_came.at[step, shift - 1],
            device_id={"cols": to},
            device_id_type=pl.DeviceIdType.MESH,
        )

    def attend_step(step, _):
        for index in range(each):
            o_send[step, :, :, index * group : (index + 1) * group] = attend_part(
                step * each + index
            )
        for shift in range(1, col_size):
            o_copy(step, shift).start()
        return 0

    lax.fori_loop(0, parts, attend_step, 0)

    st_copies = to_cols(2, lambda to: st_send.at[own_rows(to)], st_recv.at[me_col])
    st_recv[me_col] = st_send[own_rows(me_col)]
    for step in range(parts):
        o_recv[step, me_col] = o_send[step, me_col]
    o_copies = [o_copy(step, shift) for step in range(parts) for shift in range(1, col_size)]
    for copy in gate_copies + st_copies:
        copy.wait_recv()
    stats = st_recv[...]
    lane = lane_iota(stats.shape)
    top = jnp.max(stats, axis=0, keepdims=True)
    factor = jnp.exp(stats - top)
    sums = jnp.sum(factor * pltpu.roll(stats, halves * heads, axis=2), axis=0, keepdims=True)
    factor = jnp.where(lane < halves * heads, factor / sums, 0.0)
    factor = factor.reshape(col_size * rows_each, LANES)
    high = factor.astype(jnp.bfloat16)
    rest = (factor - high.astype(jnp.float32)).astype(jnp.bfloat16)
    factor = jnp.concatenate([high, rest], axis=1)
    scales = [
        jnp.dot(factor, spread_v[half], preferred_element_type=jnp.float32) for half in range(halves)
    ]
    gate = jnp.concatenate(
        [gate_recv[part].reshape(halves * rows_each, group) for part in range(col_size)], axis=1
    )
    for copy in o_copies:
        copy.wait_recv()
    attended = jnp.zeros((halves * rows_each, width), jnp.float32)
    for part in range(col_size):
        rows = slice(part * rows_each, (part + 1) * rows_each)
        part_scale = jnp.concatenate([scales[half][rows] for half in range(halves)], axis=0)
        whole = jnp.concatenate([o_recv[step, part] for step in range(parts)], axis=1)
        attended = attended + part_scale * whole.astype(jnp.float32)
    mixed = (attended * gate).astype(jnp.bfloat16)
    for copy in loads[7:]:
        copy.wait()
    added = jnp.dot(mixed, out_v[...], preferred_element_type=jnp.float32)
    own = own_single[...].astype(jnp.float32).reshape(halves * rows_each, width)
    updated = (own + added).astype(jnp.bfloat16)
    so_send[...] = updated.astype(jnp.float32).reshape(halves, rows_each, width).astype(jnp.bfloat16)
    factors = jnp.dot(
        layer_norm(updated).astype(jnp.bfloat16),
        factors_v[...],
        preferred_element_type=jnp.float32,
    )
    factors = factors.astype(jnp.bfloat16).astype(jnp.float32)
    first, second = factors[:rows_each], factors[rows_each:]
    shift = factors.shape[1] // 2
    low = lane_iota(first.shape) < shift
    left = jnp.where(low, first, pltpu.roll(second, shift, axis=1))
    right = jnp.where(low, pltpu.roll(first, shift, axis=1), second)
    left_send[...] = left
    right_send[...] = right
    right_copies = fan_copies(1, lambda half: right_send, right_recv)
    on_fan(right_copies, lambda copy: copy.start())
    left_copies = to_cols(4, lambda to: left_send, left_recv.at[me_col])
    so_copies = to_cols(5, lambda to: so_send, single_out.at[:, me_col])
    own_copy = pltpu.make_async_copy(so_send, single_out.at[:, me_col], load_sems.at[0])
    own_copy.start()
    left_recv[me_col] = left

    @pl.when(mine)
    def _():
        right_recv[me_col] = right_send[...]

    fan_wait(1, lambda half: right_send, right_recv)
    for copy in left_copies:
        copy.wait_recv()
    left = left_recv[...].reshape(depth, LANES)
    turned = pltpu.roll(left, shift, axis=1)
    low = lane_iota(left.shape) < shift
    left_out[:depth] = jnp.where(low, left, turned)
    left_out[depth:] = jnp.where(low, turned, left)
    right = right_recv[...].reshape(tile_cols, LANES)
    turned = pltpu.roll(right, shift, axis=1)
    right_out[...] = jnp.where(lane_iota(right.shape) // shift == half_mine, right, turned)

    for copies in (q_copies, relays, gate_copies, st_copies, o_copies, left_copies, so_copies):
        for copy in copies:
            copy.wait_send()
    on_some(kv_copies, lambda copy: copy.wait_send())
    on_fan(right_copies, lambda copy: copy.wait_send())
    for copy in so_copies:
        copy.wait_recv()
    own_copy.wait()


def attend(single, pair, mask, w_bias, w_project, w_out, w_factors, row_size, col_size):
    tile_rows, tile_cols, wide = pair.shape
    width = single.shape[1]
    heads = w_bias.shape[1]
    halves = tile_rows // tile_cols
    depth = tile_rows // halves
    rows_each = depth // col_size
    group = w_project.shape[2]
    steps = 8
    parts = col_size // 2
    stride = depth + 8
    any_spec = pl.BlockSpec(memory_space=pl.ANY)
    vmem_spec = pl.BlockSpec(memory_space=pltpu.VMEM)
    bf16, f32 = jnp.bfloat16, jnp.float32
    single_out, left, right = pl.pallas_call(
        functools.partial(attend_kernel, row_size, col_size, heads, tile_cols, stride),
        out_shape=(
            jax.ShapeDtypeStruct((halves, col_size, rows_each, width), bf16),
            jax.ShapeDtypeStruct((tile_rows, wide), f32),
            jax.ShapeDtypeStruct((tile_cols, wide), f32),
        ),
        in_specs=[any_spec] * 7,
        out_specs=[any_spec, vmem_spec, vmem_spec],
        scratch_shapes=[
            pltpu.VMEM((tile_rows, width), bf16),
            pltpu.VMEM((halves, depth, tile_cols, wide), bf16),
            pltpu.VMEM((mask.shape[0] // LANES, LANES), jnp.int32),
            pltpu.VMEM((heads, wide), bf16),
            pltpu.VMEM(w_project.shape, bf16),
            pltpu.VMEM(w_out.shape, bf16),
            pltpu.VMEM(w_factors.shape, bf16),
            pltpu.VMEM((halves, rows_each, width), bf16),
            pltpu.VMEM((halves, 2, tile_cols, group), bf16),
            pltpu.VMEM((col_size, 2, tile_cols, group), bf16),
            pltpu.VMEM((col_size, tile_rows, group), bf16),
            pltpu.VMEM((halves, depth, group), f32),
            pltpu.VMEM((col_size, halves, rows_each, group), f32),
            pltpu.VMEM((heads * stride, LANES), f32),
            pltpu.VMEM((parts, col_size, halves * rows_each, width // parts), bf16),
            pltpu.VMEM((parts, col_size, halves * rows_each, width // parts), bf16),
            pltpu.VMEM((depth, LANES), f32),
            pltpu.VMEM((col_size, rows_each, LANES), f32),
            pltpu.VMEM((rows_each, LANES), f32),
            pltpu.VMEM((rows_each, LANES), f32),
            pltpu.VMEM((col_size, rows_each, LANES), f32),
            pltpu.VMEM((col_size, rows_each, LANES), f32),
            pltpu.VMEM((halves, rows_each, width), bf16),
            pltpu.VMEM((2, halves * wide, halves * wide), bf16),
            pltpu.VMEM((halves, 2 * LANES, width), bf16),
            pltpu.SemaphoreType.DMA((9 + halves,)),
            pltpu.SemaphoreType.DMA((steps,)),
            pltpu.SemaphoreType.DMA((6, col_size - 1)),
            pltpu.SemaphoreType.DMA((6, col_size - 1)),
            pltpu.SemaphoreType.DMA((2, row_size * halves)),
            pltpu.SemaphoreType.DMA((2, col_size)),
            pltpu.SemaphoreType.DMA((row_size * halves,)),
            pltpu.SemaphoreType.DMA((2, col_size)),
            pltpu.SemaphoreType.DMA((col_size,)),
            pltpu.SemaphoreType.DMA((col_size,)),
            pltpu.SemaphoreType.DMA((col_size,)),
            pltpu.SemaphoreType.DMA((parts, col_size - 1)),
            pltpu.SemaphoreType.DMA((parts, col_size - 1)),
        ],
        compiler_params=pltpu.CompilerParams(collective_id=3, has_side_effects=True),
        name="attend",
    )(
        single,
        pair.reshape(halves, depth, tile_cols, wide),
        mask.reshape(mask.shape[0] // LANES, LANES),
        w_bias.T,
        w_project,
        w_out,
        w_factors,
    )
    return single_out.reshape(tile_rows, width), left, right


def fits(row_size, col_size, single, pair, mask, w_bias, w_project, w_factors):
    tile_rows, tile_cols, wide = pair.shape
    heads = w_bias.shape[1]
    return (
        tile_rows == 2 * tile_cols
        and 2 * tile_cols == LANES
        and wide == LANES
        and w_factors.shape[1] == LANES
        and w_project.shape[2] == LANES
        and 4 * heads == LANES
        and heads % (2 * col_size) == 0
        and tile_cols % (8 * col_size) == 0
        and col_size == 2 * row_size
        and row_size % 2 == 0
        and mask.shape[0] % LANES == 0
    )


def per_device_keys(
    row_size, col_size,
    single, pair, residue_mask, w_bias, w_project, w_out, w_factors, w_pairout, w_up, w_down
):
    single_out, left, right = attend(
        single, pair, residue_mask, w_bias, w_project, w_out, w_factors, row_size, col_size
    )
    return (single_out, update_pair(pair, left, right, w_pairout, w_up, w_down))


def dispatch(row_size, col_size, *arrays):
    single, pair, residue_mask, w_bias, w_project, w_out, w_factors = arrays[:7]
    if fits(row_size, col_size, single, pair, residue_mask, w_bias, w_project, w_factors):
        return per_device_keys(row_size, col_size, *arrays)
    return per_device(row_size, col_size, *arrays)


def solution(mesh):
    return jax.shard_map(
        functools.partial(dispatch, mesh.shape["rows"], mesh.shape["cols"]),
        mesh=mesh,
        in_specs=(
            P("rows", None),
            P("rows", "cols", None),
            P(),
            P(),
            P(None, None, "cols"),
            P(),
            P(),
            P(),
            P(),
            P(),
        ),
        out_specs=(P("rows", None), P("rows", "cols", None)),
        check_vma=False,
    )
```

```python
import functools
import math

import jax
import jax.numpy as jnp
from jax import lax
from jax.experimental import pallas as pl
from jax.experimental.pallas import tpu as pltpu
from jax.sharding import PartitionSpec as P

epsilon = 1e-05


def enter(axes):
    barrier = pltpu.get_barrier_semaphore()
    total = 0
    for axis, size in axes:
        me = lax.axis_index(axis)
        for step in range(1, size):
            pl.semaphore_signal(
                barrier,
                inc=1,
                device_id={axis: lax.rem(me + step, size)},
                device_id_type=pl.DeviceIdType.MESH,
            )
        total += size - 1
    pl.semaphore_wait(barrier, total)


def spread(axis, size, source, landing, send_sems, recv_sems):
    me = lax.axis_index(axis)
    copies = []
    for step in range(1, size):
        copy = pltpu.make_async_remote_copy(
            src_ref=source,
            dst_ref=landing.at[me],
            send_sem=send_sems.at[step - 1],
            recv_sem=recv_sems.at[step - 1],
            device_id={axis: lax.rem(me + step, size)},
            device_id_type=pl.DeviceIdType.MESH,
        )
        copy.start()
        copies.append(copy)
    return copies


def gather_kernel(axis, size, source, gathered, send_sems, recv_sems, own_sem):
    enter([(axis, size)])
    copies = spread(axis, size, source, gathered, send_sems, recv_sems)
    own = pltpu.make_async_copy(source, gathered.at[lax.axis_index(axis)], own_sem)
    own.start()
    own.wait()
    for copy in copies:
        copy.wait()


def gather(values, axis, size, collective_id):
    return pl.pallas_call(
        functools.partial(gather_kernel, axis, size),
        out_shape=jax.ShapeDtypeStruct((size, *values.shape), values.dtype),
        in_specs=[pl.BlockSpec(memory_space=pltpu.VMEM)],
        out_specs=pl.BlockSpec(memory_space=pltpu.VMEM),
        scratch_shapes=[
            pltpu.SemaphoreType.DMA((size - 1,)),
            pltpu.SemaphoreType.DMA((size - 1,)),
            pltpu.SemaphoreType.DMA,
        ],
        compiler_params=pltpu.CompilerParams(collective_id=collective_id, has_side_effects=True),
        name="gather_" + axis,
    )(values)


def single_kernel(
    row_size, col_size, tile_cols,
    mixed, single, w_out, w_factors, single_out, left_out, right_out,
    gathered, factor_right, send_sems, recv_sems, row_send, row_recv, own_sem,
):
    enter([("cols", col_size), ("rows", row_size)])
    tile_rows, width = mixed.shape
    me_col = lax.axis_index("cols")
    me_row = lax.axis_index("rows")
    copies = spread("cols", col_size, mixed, gathered, send_sems, recv_sems)
    own = pltpu.make_async_copy(mixed, gathered.at[me_col], own_sem)
    own.start()
    own.wait()
    for copy in copies:
        copy.wait()
    whole = jnp.concatenate([gathered[part] for part in range(col_size)], axis=1)
    total = jnp.dot(whole, w_out[...], preferred_element_type=jnp.float32)
    updated = (single[...].astype(jnp.float32) + total).astype(jnp.bfloat16)
    single_out[...] = updated
    normed = layer_norm(updated).astype(jnp.bfloat16)
    factors = jnp.dot(normed, w_factors[...], preferred_element_type=jnp.float32)
    factors = factors.astype(jnp.bfloat16).astype(jnp.float32)
    half = factors.shape[1] // 2
    swapped = jnp.concatenate([factors[:, half:], factors[:, :half]], axis=1)
    lower = lax.broadcasted_iota(jnp.int32, factors.shape, 1) < half
    left_out[...] = jnp.where(lower, factors, swapped)
    factor_right[...] = jnp.where(lower, swapped, factors).astype(jnp.bfloat16)
    first = me_col * tile_cols
    owner = first // tile_rows
    offset = pl.multiple_of(first - owner * tile_rows, tile_cols)
    piece = factor_right.at[pl.ds(offset, tile_cols)]

    @pl.when(me_row == owner)
    def _():
        local = pltpu.make_async_copy(piece, right_out, own_sem)
        local.start()
        sends = []
        for step in range(1, row_size):
            send = pltpu.make_async_remote_copy(
                src_ref=piece,
                dst_ref=right_out,
                send_sem=row_send.at[step - 1],
                recv_sem=row_recv,
                device_id={"rows": lax.rem(me_row + step, row_size)},
                device_id_type=pl.DeviceIdType.MESH,
            )
            send.start()
            sends.append(send)
        local.wait()
        for send in sends:
            send.wait_send()

    @pl.when(me_row != owner)
    def _():
        pltpu.make_async_remote_copy(
            src_ref=piece,
            dst_ref=right_out,
            send_sem=row_send.at[0],
            recv_sem=row_recv,
            device_id={"rows": lax.rem(me_row + 1, row_size)},
            device_id_type=pl.DeviceIdType.MESH,
        ).wait_recv()


def update_single(mixed, single, w_out, w_factors, row_size, col_size, tile_cols):
    tile_rows, width = single.shape
    wide = w_factors.shape[1]
    return pl.pallas_call(
        functools.partial(single_kernel, row_size, col_size, tile_cols),
        out_shape=(
            jax.ShapeDtypeStruct((tile_rows, width), jnp.bfloat16),
            jax.ShapeDtypeStruct((tile_rows, wide), jnp.float32),
            jax.ShapeDtypeStruct((tile_cols, wide), jnp.bfloat16),
        ),
        in_specs=[pl.BlockSpec(memory_space=pltpu.VMEM)] * 4,
        out_specs=[pl.BlockSpec(memory_space=pltpu.VMEM)] * 3,
        scratch_shapes=[
            pltpu.VMEM((col_size, *mixed.shape), jnp.bfloat16),
            pltpu.VMEM((tile_rows, wide), jnp.bfloat16),
            pltpu.SemaphoreType.DMA((col_size - 1,)),
            pltpu.SemaphoreType.DMA((col_size - 1,)),
            pltpu.SemaphoreType.DMA((row_size - 1,)),
            pltpu.SemaphoreType.DMA,
            pltpu.SemaphoreType.DMA,
        ],
        compiler_params=pltpu.CompilerParams(collective_id=2, has_side_effects=True),
        name="update_single",
    )(mixed, single, w_out, w_factors)


def matmul_norm(values):
    wide = values.shape[1]
    share = jnp.full((2 * wide, wide), 1.0 / wide, jnp.bfloat16)
    mean = jnp.dot(values, share[:wide], preferred_element_type=jnp.float32)
    centred = values.astype(jnp.float32) - mean
    square = centred * centred
    high = square.astype(jnp.bfloat16)
    low = (square - high.astype(jnp.float32)).astype(jnp.bfloat16)
    spread_out = jnp.dot(
        jnp.concatenate([high, low], 1), share, preferred_element_type=jnp.float32
    )
    return (centred * lax.rsqrt(spread_out + epsilon)).astype(jnp.bfloat16)


def norm_kernel(values, normed):
    normed[...] = matmul_norm(values[...])


def norm_rows(values, block):
    spec = pl.BlockSpec((block, values.shape[1]), lambda step: (step, 0))
    return pl.pallas_call(
        norm_kernel,
        out_shape=jax.ShapeDtypeStruct(values.shape, jnp.bfloat16),
        grid=(values.shape[0] // block,),
        in_specs=[spec],
        out_specs=spec,
        name="norm_pair",
    )(values)


def pair_kernel(pair, left, right, w_pairout, w_up, w_down, updated):
    block_rows, tile_cols, wide = pair.shape
    left_wide = left[...][:, None, :]
    right_wide = right[...].astype(jnp.float32)[None, :, :]
    lower = lax.broadcasted_iota(jnp.int32, pair.shape, 2) < wide // 2
    paired = jnp.where(lower, left_wide * right_wide, left_wide - right_wide)
    paired = paired.astype(jnp.bfloat16).reshape(block_rows * tile_cols, wide)
    flat = pair[...].reshape(block_rows * tile_cols, wide).astype(jnp.float32)
    mid = flat + jnp.dot(paired, w_pairout[...], preferred_element_type=jnp.float32)
    mid = mid.astype(jnp.bfloat16)
    normed = matmul_norm(mid)
    hidden = jnp.dot(normed, w_up[...], preferred_element_type=jnp.float32)
    hidden = jnp.maximum(hidden, 0.0).astype(jnp.bfloat16)
    out = mid.astype(jnp.float32) + jnp.dot(
        hidden, w_down[...], preferred_element_type=jnp.float32
    )
    updated[...] = out.astype(jnp.bfloat16).reshape(pair.shape)


def update_pair(pair, left, right, w_pairout, w_up, w_down):
    tile_rows, tile_cols, wide = pair.shape
    block = math.gcd(tile_rows, max(8, 1024 // tile_cols))
    tile = pl.BlockSpec((block, tile_cols, wide), lambda step: (step, 0, 0))

    def whole(array):
        return pl.BlockSpec(array.shape, lambda step: (0, 0))

    return pl.pallas_call(
        pair_kernel,
        out_shape=jax.ShapeDtypeStruct(pair.shape, jnp.bfloat16),
        grid=(tile_rows // block,),
        in_specs=[
            tile,
            pl.BlockSpec((block, wide), lambda step: (step, 0)),
            whole(right),
            whole(w_pairout),
            whole(w_up),
            whole(w_down),
        ],
        out_specs=tile,
        name="update_pair",
    )(pair, left, right, w_pairout, w_up, w_down)


def layer_norm(values):
    values = values.astype(jnp.float32)
    centred = values - jnp.mean(values, -1, keepdims=True)
    return centred * lax.rsqrt(jnp.mean(centred * centred, -1, keepdims=True) + epsilon)


def per_device(
    row_size, col_size,
    single, pair, residue_mask, w_bias, w_project, w_out, w_factors, w_pairout, w_up, w_down
):
    tile_rows = pair.shape[0]
    tile_cols = pair.shape[1]
    normed_pair = norm_rows(
        pair.reshape(tile_rows * tile_cols, pair.shape[2]), math.gcd(tile_rows * tile_cols, 1024)
    ).reshape(pair.shape)
    bias_local = jnp.einsum(
        "rcp,ph->hrc", normed_pair, w_bias, preferred_element_type=jnp.float32
    ).astype(jnp.bfloat16)
    normed_single = layer_norm(single).astype(jnp.bfloat16)
    projected = jnp.einsum(
        "rs,fsc->frc", normed_single, w_project, preferred_element_type=jnp.float32
    )
    query_rows = projected[0].astype(jnp.bfloat16)
    key_local = projected[1].astype(jnp.bfloat16)
    value_local = projected[2].astype(jnp.bfloat16)
    gate_values = jax.nn.sigmoid(projected[3])
    bias_heads = lax.all_to_all(bias_local, "cols", split_axis=0, concat_axis=2, tiled=True)
    both = gather(jnp.concatenate([key_local, value_local], 1), "rows", row_size, 1)
    both = both.reshape(row_size * tile_rows, both.shape[2])
    key_rows, value_rows = both[:, : key_local.shape[1]], both[:, key_local.shape[1] :]
    heads_here = bias_heads.shape[0]
    head_width = query_rows.shape[1] // heads_here
    residues = key_rows.shape[0]
    query_split = query_rows.reshape(tile_rows, heads_here, head_width)
    key_split = key_rows.reshape(residues, heads_here, head_width)
    value_split = value_rows.reshape(residues, heads_here, head_width)
    score_scale = 1.0 / math.sqrt(head_width)
    scores = jnp.einsum(
        "rhd,lhd->hrl", query_split, key_split, preferred_element_type=jnp.float32
    ) * score_scale + bias_heads.astype(jnp.float32)
    key_valid = (residue_mask > 0)[None, None, :]
    scores = jnp.where(key_valid, scores, -jnp.inf)
    weights = jax.nn.softmax(scores, axis=-1).astype(jnp.bfloat16)
    attended = jnp.einsum("hrl,lhd->rhd", weights, value_split, preferred_element_type=jnp.float32)
    attended = attended.reshape(tile_rows, heads_here * head_width)
    mixed = (attended * gate_values).astype(jnp.bfloat16)
    single_out, left, right = update_single(
        mixed, single, w_out, w_factors, row_size, col_size, tile_cols
    )
    return (single_out, update_pair(pair, left, right, w_pairout, w_up, w_down))


LANES = 128
excluded = -1e30
update_block = 16


def lane_iota(shape):
    return lax.broadcasted_iota(jnp.int32, shape, len(shape) - 1)


def centre_matrix(wide, copies):
    size = wide * copies
    row = lax.broadcasted_iota(jnp.int32, (size, size), 0)
    col = lax.broadcasted_iota(jnp.int32, (size, size), 1)
    share = jnp.where(row // wide == col // wide, 1.0 / wide, 0.0)
    return (jnp.where(row == col, 1.0, 0.0) - share).astype(jnp.bfloat16)


def norm_centred(values, centre, copies):
    centred = jnp.dot(values, centre, preferred_element_type=jnp.float32)
    wide = values.shape[1] // copies
    parts = []
    for index in range(copies):
        part = centred[:, index * wide : (index + 1) * wide]
        square = jnp.sum(part * part, axis=1, keepdims=True) * (1.0 / wide)
        parts.append((part * lax.rsqrt(square + epsilon)).astype(jnp.bfloat16))
    return parts


def twice(weights):
    zeros = jnp.zeros_like(weights)
    upper = jnp.concatenate([weights, zeros], axis=1)
    return jnp.concatenate([upper, jnp.concatenate([zeros, weights], axis=1)], axis=0)


def update_rows(pair_of, left_of, right, rows, centre, w_pairout, w_up, w_down):
    tile_cols, wide = right.shape
    lower = lane_iota((rows, tile_cols, wide)) < wide // 2

    def paired(index):
        left_wide = left_of(index)[:, None, :]
        right_wide = right[None, :, :]
        chosen = jnp.where(lower, left_wide * right_wide, left_wide - right_wide)
        return chosen.astype(jnp.bfloat16).reshape(rows * tile_cols, wide)

    flat = [pair_of(index).reshape(rows * tile_cols, wide) for index in range(2)]
    mid = jnp.concatenate(flat, axis=1).astype(jnp.float32) + jnp.dot(
        jnp.concatenate([paired(0), paired(1)], axis=1),
        w_pairout,
        preferred_element_type=jnp.float32,
    )
    mid = mid.astype(jnp.bfloat16)
    normed = jnp.concatenate(norm_centred(mid, centre, 2), axis=0)
    mid = jnp.concatenate([mid[:, :wide], mid[:, wide:]], axis=0)
    hidden = jnp.dot(normed, w_up, preferred_element_type=jnp.float32)
    hidden = jnp.maximum(hidden, 0.0).astype(jnp.bfloat16)
    out = mid.astype(jnp.float32) + jnp.dot(hidden, w_down, preferred_element_type=jnp.float32)
    return out.astype(jnp.bfloat16).reshape(2 * rows, tile_cols, wide)


def attend_kernel(
    row_size, col_size, heads, tile_cols, stride,
    single, pair, mask, w_bias, w_project, w_out, w_factors, w_pairout, w_up, w_down,
    single_out, left_out, right_out, part_out,
    single_v, pair_v, mask_v, bias_w, project_v, out_v, factors_v, own_single,
    kv_send, kv_recv, q_recv, gate_send, gate_recv, bias_v, o_send, o_recv,
    st_send, st_recv, left_send, right_send, left_recv, right_recv, so_send, centre_v, spread_v,
    pairout_v, twice_v, up_v, down_v, part_v,
    load_sems, pair_sems, col_send, col_recv, fan_send, fan_recv,
    kv_sent, kv_came, kv_relayed, q_sent, q_came, o_sent, o_came,
):
    me_row = lax.axis_index("rows")
    me_col = lax.axis_index("cols")
    total = row_size * col_size
    barrier = pltpu.get_barrier_semaphore()
    me = me_row * col_size + me_col
    for step in range(1, total):
        to = lax.rem(me + step, total)
        pl.semaphore_signal(
            barrier,
            inc=1,
            device_id={"rows": to // col_size, "cols": lax.rem(to, col_size)},
            device_id_type=pl.DeviceIdType.MESH,
        )
    halves, depth, _, wide = pair.shape
    tile_rows, width = single.shape
    group = w_project.shape[2]
    rows_each = depth // col_size
    heads_here = heads // col_size
    head_width = group // heads_here
    chunk = depth // pair_sems.shape[0]
    loads = [
        pltpu.make_async_copy(source, target, load_sems.at[index])
        for index, (source, target) in enumerate(
            [(single, single_v)]
            + [(w_project.at[part], project_v.at[part]) for part in (1, 2, 0, 3)]
            + [(w_bias, bias_w), (mask, mask_v)]
            + [
                (single.at[pl.ds(half * depth + me_col * rows_each, rows_each)], own_single.at[half])
                for half in range(halves)
            ]
            + [(w_out, out_v), (w_factors, factors_v)]
            + [(w_pairout, pairout_v), (w_up, up_v), (w_down, down_v)]
        )
    ]
    for copy in loads[:7]:
        copy.start()

    def pair_load(step):
        part = pl.ds(step * chunk, chunk)
        return pltpu.make_async_copy(pair.at[:, part], pair_v.at[:, part], pair_sems.at[step])

    for step in range(depth // chunk):
        pair_load(step).start()
    for copy in loads[7:]:
        copy.start()

    centre_v[...] = centre_matrix(wide, halves)

    def to_cols(kind, source_of, target):
        copies = []
        for step in range(1, col_size):
            to = lax.rem(me_col + step, col_size)
            copy = pltpu.make_async_remote_copy(
                src_ref=source_of(to),
                dst_ref=target,
                send_sem=col_send.at[kind, step - 1],
                recv_sem=col_recv.at[kind, step - 1],
                device_id={"cols": to},
                device_id_type=pl.DeviceIdType.MESH,
            )
            copy.start()
            copies.append(copy)
        return copies

    owner = me_col // halves
    mine = owner == me_row
    half_mine = lax.rem(me_col, halves)

    def fan_copies(kind, source_of, target):
        copies = []
        for step in range(row_size):
            for half in range(halves):
                to = halves * me_row + half
                copy = pltpu.make_async_remote_copy(
                    src_ref=source_of(half),
                    dst_ref=target.at[me_col],
                    send_sem=fan_send.at[kind, step * halves + half],
                    recv_sem=fan_recv.at[kind, me_col],
                    device_id={"rows": lax.rem(me_row + step, row_size), "cols": to},
                    device_id_type=pl.DeviceIdType.MESH,
                )
                copies.append((copy, step, to))
        return copies

    def on_some(copies, act):
        for copy, condition in copies:
            if condition is None:
                act(copy)
            else:
                pl.when(condition)(functools.partial(act, copy))

    kind_mine = lax.rem(me_row, 2)
    row_mate = me_row + 1 - 2 * kind_mine
    col_mate = me_col + 1 - 2 * lax.rem(me_col, 2)

    def relay_keys(part, kind, slot):
        return pltpu.make_async_remote_copy(
            src_ref=kv_recv.at[part, kind],
            dst_ref=kv_recv.at[part, kind],
            send_sem=kv_relayed.at[slot],
            recv_sem=kv_came.at[kind, part],
            device_id={"rows": row_mate},
            device_id_type=pl.DeviceIdType.MESH,
        )

    def send_query(part, to, slot):
        return pltpu.make_async_remote_copy(
            src_ref=q_recv.at[part],
            dst_ref=q_recv.at[part],
            send_sem=q_sent.at[slot],
            recv_sem=q_came.at[part],
            device_id={"cols": to},
            device_id_type=pl.DeviceIdType.MESH,
        )

    def on_fan(copies, act):
        for copy, step, to in copies:
            if step:
                act(copy)
            else:
                pl.when(to != me_col)(functools.partial(act, copy))

    def fan_wait(kind, source_of, target):
        for part in range(col_size):
            copy = pltpu.make_async_remote_copy(
                src_ref=source_of(0),
                dst_ref=target.at[part],
                send_sem=fan_send.at[kind, 0],
                recv_sem=fan_recv.at[kind, part],
                device_id={"rows": lax.rem(me_row + 1, row_size)},
                device_id_type=pl.DeviceIdType.MESH,
            )
            pl.when(jnp.logical_not(jnp.logical_and(mine, part == me_col)))(copy.wait_recv)

    loads[0].wait()
    normed = layer_norm(single_v[...]).astype(jnp.bfloat16)
    loads[1].wait()
    loads[2].wait()
    key_value = jnp.dot(
        normed,
        jnp.concatenate([project_v[1], project_v[2]], axis=1),
        preferred_element_type=jnp.float32,
    ).astype(jnp.bfloat16)
    for half in range(halves):
        for kind in range(2):
            kv_send[half, kind] = key_value[
                half * tile_cols : (half + 1) * tile_cols, kind * group : (kind + 1) * group
            ]
    pl.semaphore_wait(barrier, total - 1)
    kv_copies = []
    for step in range(row_size // 2):
        for kind in range(2):
            for half in range(halves):
                to = halves * me_row + half
                row = 2 * lax.rem(me_row // 2 + step, row_size // 2) + kind
                copy = pltpu.make_async_remote_copy(
                    src_ref=kv_send.at[half, kind],
                    dst_ref=kv_recv.at[me_col, kind],
                    send_sem=kv_sent.at[(step * 2 + kind) * halves + half],
                    recv_sem=kv_came.at[kind, me_col],
                    device_id={"rows": row, "cols": to},
                    device_id_type=pl.DeviceIdType.MESH,
                )
                here = jnp.logical_and(row == me_row, to == me_col)
                copies_of = (copy, None if step else jnp.logical_not(here))
                kv_copies.append(copies_of)
    on_some(kv_copies, lambda copy: copy.start())

    @pl.when(mine)
    def _():
        kv_recv[me_col, kind_mine] = kv_send[half_mine, kind_mine]

    loads[3].wait()
    loads[4].wait()
    query_gate = jnp.dot(
        normed,
        jnp.concatenate([project_v[0], project_v[3]], axis=1),
        preferred_element_type=jnp.float32,
    )
    q_recv[me_col] = query_gate[:, :group].astype(jnp.bfloat16)
    peers = [lax.rem(me_col + 2 * step, col_size) for step in range(1, col_size // 2)]
    mates = [lax.rem(col_mate + 2 * step, col_size) for step in range(1, col_size // 2)]
    q_copies = [send_query(me_col, to, slot) for slot, to in enumerate(peers)]
    q_copies.append(send_query(me_col, col_mate, len(peers)))
    for copy in q_copies:
        copy.start()
    gate_send[...] = jax.nn.sigmoid(query_gate[:, group:]).reshape(halves, depth, group)

    def own_rows(to):
        return pl.ds(pl.multiple_of(to * rows_each, rows_each), rows_each)

    loads[5].wait()
    loads[6].wait()

    def bias_step(step, _):
        pair_load(step).wait()
        parts = [
            pair_v[half, pl.ds(step * chunk, chunk)].reshape(chunk * tile_cols, wide)
            for half in range(halves)
        ]
        parts = norm_centred(jnp.concatenate(parts, axis=1), centre_v[...], halves)
        parts = [part.reshape(chunk, 1, tile_cols, wide) for part in parts]
        normed_pair = jnp.concatenate(parts, axis=1).reshape(chunk * halves * tile_cols, wide)
        bias = lax.dot_general(
            bias_w[...], normed_pair, (((1,), (1,)), ((), ())), preferred_element_type=jnp.float32
        )
        bias = bias.astype(jnp.bfloat16).astype(jnp.float32)
        for part in range(chunk):
            bias_v[pl.ds(step * chunk + part, heads, stride=stride), :] = bias[
                :, part * LANES : (part + 1) * LANES
            ]
        return 0

    lax.fori_loop(0, depth // chunk, bias_step, 0)

    lane_row = lane_iota((2 * halves * heads, width))
    place = lax.broadcasted_iota(jnp.int32, (2 * halves * heads, width), 0)
    for half in range(halves):
        picked = jnp.where(place == half * heads + lane_row // head_width, 1.0, 0.0)
        spread_v[half, :LANES] = picked.astype(jnp.bfloat16)
        spread_v[half, LANES:] = picked.astype(jnp.bfloat16)

    relays = []
    for part in range(col_size):
        copy = relay_keys(part, kind_mine, part)
        pl.when(jnp.logical_not(jnp.logical_and(mine, part == me_col)))(copy.wait_recv)
        copy.start()
        relays.append(copy)
    for slot, peer in enumerate(peers):
        copy = send_query(peer, col_mate, col_size // 2 + slot)
        copy.wait_recv()
        copy.start()
        relays.append(copy)
    for part in range(col_size):
        relay_keys(part, 1 - kind_mine, part).wait_recv()
    for part in [col_mate] + mates:
        send_query(part, col_mate, 0).wait_recv()
    gate_copies = to_cols(1, lambda to: gate_send.at[:, own_rows(to)], gate_recv.at[me_col])
    gate_recv[me_col] = gate_send[:, own_rows(me_col)]

    length = jnp.sum(jnp.sum(mask_v[...], axis=1, keepdims=True), axis=0, keepdims=True)
    lane = lane_iota((depth, LANES))
    low = lane < tile_cols
    valid = me_col * tile_cols + lax.rem(lane, tile_cols) < length
    head_of = lane_iota((tile_cols, group)) // head_width
    head_masks = [
        jnp.where(head_of == head, 1.0, 0.0).astype(jnp.bfloat16) for head in range(heads_here)
    ]
    zeros = jnp.zeros((tile_cols, group), jnp.bfloat16)
    scale = 1.0 / math.sqrt(head_width)
    st_send[...] = jnp.zeros_like(st_send)
    block_place = lax.broadcasted_iota(jnp.int32, (heads_here * LANES, LANES), 0) // tile_cols
    block_target = (
        halves * heads + lax.rem(block_place, halves) * heads + block_place // halves
    )
    block_lane = lane_iota((heads_here * LANES, LANES))

    def attend_part(part):
        query = q_recv[part]
        query = jnp.concatenate([query[:depth], query[depth:]], axis=1)
        key, value = kv_recv[part, 0], kv_recv[part, 1]
        weights, value_rows = [], []
        stats = st_send[...]
        for first in range(0, heads_here, 2):
            key_rows = []
            for head in (first, first + 1):
                masked = key * head_masks[head]
                key_rows.append(jnp.concatenate([masked, zeros], axis=1))
                key_rows.append(jnp.concatenate([zeros, masked], axis=1))
            raw = lax.dot_general(
                query,
                jnp.concatenate(key_rows, axis=0),
                (((1,), (1,)), ((), ())),
                preferred_element_type=jnp.float32,
            )
            for head in (first, first + 1):
                index = part * heads_here + head
                bias = bias_v[pl.ds(pl.multiple_of(index * stride, 8), depth), :]
                scores = raw[:, (head - first) * LANES : (head - first + 1) * LANES] * scale + bias
                scores = jnp.where(valid, scores, excluded)
                top0 = jnp.max(jnp.where(low, scores, excluded), axis=1, keepdims=True)
                top1 = jnp.max(jnp.where(low, excluded, scores), axis=1, keepdims=True)
                weights.append(
                    jnp.exp(scores - jnp.where(low, top0, top1)).astype(jnp.bfloat16)
                )
                stats = jnp.where(lane == index, top0, stats)
                stats = jnp.where(lane == heads + index, top1, stats)
        for head in range(heads_here):
            masked = value * head_masks[head]
            value_rows.append(jnp.concatenate([masked, zeros], axis=1))
            value_rows.append(jnp.concatenate([zeros, masked], axis=1))
        weights = jnp.concatenate(weights, axis=1)
        mixed = jnp.dot(
            weights, jnp.concatenate(value_rows, axis=0), preferred_element_type=jnp.float32
        )
        ones = jnp.where(block_lane == block_target + part * heads_here, 1.0, 0.0)
        sums = jnp.dot(weights, ones.astype(jnp.bfloat16), preferred_element_type=jnp.float32)
        st_send[...] = stats + sums
        pieces = [
            mixed[:, half * group : (half + 1) * group].reshape(col_size, rows_each, group)
            for half in range(halves)
        ]
        return jnp.concatenate(pieces, axis=1).astype(jnp.bfloat16)

    parts, _, _, part_width = o_send.shape
    each = part_width // group

    def o_copy(step, shift):
        to = lax.rem(me_col + shift, col_size)
        return pltpu.make_async_remote_copy(
            src_ref=o_send.at[step, to],
            dst_ref=o_recv.at[step, me_col],
            send_sem=o_sent.at[step, shift - 1],
            recv_sem=o_came.at[step, shift - 1],
            device_id={"cols": to},
            device_id_type=pl.DeviceIdType.MESH,
        )

    def attend_step(step, _):
        for index in range(each):
            o_send[step, :, :, index * group : (index + 1) * group] = attend_part(
                step * each + index
            )
        for shift in range(1, col_size):
            o_copy(step, shift).start()
        return 0

    lax.fori_loop(0, parts, attend_step, 0)

    st_copies = to_cols(2, lambda to: st_send.at[own_rows(to)], st_recv.at[me_col])
    st_recv[me_col] = st_send[own_rows(me_col)]
    for step in range(parts):
        o_recv[step, me_col] = o_send[step, me_col]
    o_copies = [o_copy(step, shift) for step in range(parts) for shift in range(1, col_size)]
    for copy in gate_copies + st_copies:
        copy.wait_recv()
    stats = st_recv[...]
    lane = lane_iota(stats.shape)
    top = jnp.max(stats, axis=0, keepdims=True)
    factor = jnp.exp(stats - top)
    sums = jnp.sum(factor * pltpu.roll(stats, halves * heads, axis=2), axis=0, keepdims=True)
    factor = jnp.where(lane < halves * heads, factor / sums, 0.0)
    factor = factor.reshape(col_size * rows_each, LANES)
    high = factor.astype(jnp.bfloat16)
    rest = (factor - high.astype(jnp.float32)).astype(jnp.bfloat16)
    factor = jnp.concatenate([high, rest], axis=1)
    scales = [
        jnp.dot(factor, spread_v[half], preferred_element_type=jnp.float32) for half in range(halves)
    ]
    gate = jnp.concatenate(
        [gate_recv[part].reshape(halves * rows_each, group) for part in range(col_size)], axis=1
    )
    for copy in o_copies:
        copy.wait_recv()
    attended = jnp.zeros((halves * rows_each, width), jnp.float32)
    for part in range(col_size):
        rows = slice(part * rows_each, (part + 1) * rows_each)
        part_scale = jnp.concatenate([scales[half][rows] for half in range(halves)], axis=0)
        whole = jnp.concatenate([o_recv[step, part] for step in range(parts)], axis=1)
        attended = attended + part_scale * whole.astype(jnp.float32)
    mixed = (attended * gate).astype(jnp.bfloat16)
    for copy in loads[7:]:
        copy.wait()
    added = jnp.dot(mixed, out_v[...], preferred_element_type=jnp.float32)
    own = own_single[...].astype(jnp.float32).reshape(halves * rows_each, width)
    updated = (own + added).astype(jnp.bfloat16)
    so_send[...] = updated.astype(jnp.float32).reshape(halves, rows_each, width).astype(jnp.bfloat16)
    factors = jnp.dot(
        layer_norm(updated).astype(jnp.bfloat16),
        factors_v[...],
        preferred_element_type=jnp.float32,
    )
    factors = factors.astype(jnp.bfloat16).astype(jnp.float32)
    first, second = factors[:rows_each], factors[rows_each:]
    shift = factors.shape[1] // 2
    low = lane_iota(first.shape) < shift
    left = jnp.where(low, first, pltpu.roll(second, shift, axis=1))
    right = jnp.where(low, pltpu.roll(first, shift, axis=1), second)
    left_send[...] = left
    right_send[...] = right
    right_copies = fan_copies(1, lambda half: right_send, right_recv)
    on_fan(right_copies, lambda copy: copy.start())
    left_copies = to_cols(4, lambda to: left_send, left_recv.at[me_col])
    so_copies = to_cols(5, lambda to: so_send, single_out.at[:, me_col])
    own_copy = pltpu.make_async_copy(so_send, single_out.at[:, me_col], load_sems.at[0])
    own_copy.start()
    left_recv[me_col] = left

    @pl.when(mine)
    def _():
        right_recv[me_col] = right_send[...]

    fan_wait(1, lambda half: right_send, right_recv)
    for copy in left_copies:
        copy.wait_recv()
    left = left_recv[...].reshape(depth, LANES)
    turned = pltpu.roll(left, shift, axis=1)
    low = lane_iota(left.shape) < shift
    left_out[:depth] = jnp.where(low, left, turned)
    left_out[depth:] = jnp.where(low, turned, left)
    right = right_recv[...].reshape(tile_cols, LANES)
    turned = pltpu.roll(right, shift, axis=1)
    right_out[...] = jnp.where(lane_iota(right.shape) // shift == half_mine, right, turned)

    twice_v[...] = twice(pairout_v[...])
    block = update_block
    starts = depth // (2 * block)

    def part_copy(step):
        rows = pl.ds(step * 2 * block, 2 * block)
        return pltpu.make_async_copy(part_v.at[rows], part_out.at[rows], pair_sems.at[step])

    def update_step(step, _):
        first = step * 2 * block
        part_v[pl.ds(first, 2 * block)] = update_rows(
            lambda index: pair_v[0, pl.ds(first + index * block, block)],
            lambda index: left_out[pl.ds(pl.multiple_of(first + index * block, 8), block)],
            right_out[...],
            block,
            centre_v[...],
            twice_v[...],
            up_v[...],
            down_v[...],
        )
        part_copy(step).start()
        return 0

    lax.fori_loop(0, starts, update_step, 0)

    for copies in (q_copies, relays, gate_copies, st_copies, o_copies, left_copies, so_copies):
        for copy in copies:
            copy.wait_send()
    on_some(kv_copies, lambda copy: copy.wait_send())
    on_fan(right_copies, lambda copy: copy.wait_send())
    for copy in so_copies:
        copy.wait_recv()
    own_copy.wait()
    for step in range(starts):
        part_copy(step).wait()


def finish_kernel(
    single, pair, part, left, right, w_pairout, w_up, w_down,
    single_out, pair_out,
    single_v, pair_v, part_v, done_v, centre_v, twice_v, sems, out_sems,
):
    _, depth, tile_cols, wide = pair.shape
    block = update_block
    steps = depth // (2 * block)

    def rows(step):
        return pl.ds(step * 2 * block, 2 * block)

    loads = [
        pltpu.make_async_copy(pair.at[1, rows(step)], pair_v.at[rows(step)], sems.at[2 + step])
        for step in range(steps)
    ]
    through = [
        (pltpu.make_async_copy(part, part_v, sems.at[0]),
         pltpu.make_async_copy(part_v, pair_out.at[0], out_sems.at[0])),
        (pltpu.make_async_copy(single, single_v, sems.at[1]),
         pltpu.make_async_copy(single_v, single_out, out_sems.at[1])),
    ]
    for copy in loads:
        copy.start()
    for copy, _ in through:
        copy.start()
    centre_v[...] = centre_matrix(wide, 2)
    twice_v[...] = twice(w_pairout[...])
    stores = []
    for step in range(steps):
        loads[step].wait()
        first = step * 2 * block
        done_v[rows(step)] = update_rows(
            lambda index: pair_v[first + index * block : first + (index + 1) * block],
            lambda index: left[depth + first + index * block : depth + first + (index + 1) * block],
            right[...],
            block,
            centre_v[...],
            twice_v[...],
            w_up[...],
            w_down[...],
        )
        store = pltpu.make_async_copy(
            done_v.at[rows(step)], pair_out.at[1, rows(step)], out_sems.at[2 + step]
        )
        store.start()
        stores.append(store)
        if step == 0:
            for load, later in through:
                load.wait()
                later.start()
                stores.append(later)
    for store in stores:
        store.wait()


def finish(single, pair, part, left, right, w_pairout, w_up, w_down):
    halves, depth, tile_cols, wide = pair.shape
    steps = depth // (2 * update_block)
    any_spec = pl.BlockSpec(memory_space=pl.ANY)
    vmem_spec = pl.BlockSpec(memory_space=pltpu.VMEM)
    bf16 = jnp.bfloat16
    return pl.pallas_call(
        finish_kernel,
        out_shape=(
            jax.ShapeDtypeStruct(single.shape, bf16),
            jax.ShapeDtypeStruct(pair.shape, bf16),
        ),
        in_specs=[any_spec] * 3 + [vmem_spec] * 5,
        out_specs=[any_spec] * 2,
        scratch_shapes=[
            pltpu.VMEM(single.shape, bf16),
            pltpu.VMEM((depth, tile_cols, wide), bf16),
            pltpu.VMEM((depth, tile_cols, wide), bf16),
            pltpu.VMEM((depth, tile_cols, wide), bf16),
            pltpu.VMEM((2 * wide, 2 * wide), bf16),
            pltpu.VMEM((2 * wide, 2 * wide), bf16),
            pltpu.SemaphoreType.DMA((2 + steps,)),
            pltpu.SemaphoreType.DMA((2 + steps,)),
        ],
        name="finish",
    )(single, pair, part, left, right, w_pairout, w_up, w_down)


def attend(
    single, pair, mask, w_bias, w_project, w_out, w_factors, w_pairout, w_up, w_down,
    row_size, col_size,
):
    halves, depth, tile_cols, wide = pair.shape
    tile_rows, width = single.shape
    heads = w_bias.shape[1]
    rows_each = depth // col_size
    group = w_project.shape[2]
    steps = depth // 16
    parts = col_size // 2
    stride = depth + 8
    any_spec = pl.BlockSpec(memory_space=pl.ANY)
    vmem_spec = pl.BlockSpec(memory_space=pltpu.VMEM)
    bf16, f32 = jnp.bfloat16, jnp.float32
    single_out, left, right, part = pl.pallas_call(
        functools.partial(attend_kernel, row_size, col_size, heads, tile_cols, stride),
        out_shape=(
            jax.ShapeDtypeStruct((halves, col_size, rows_each, width), bf16),
            jax.ShapeDtypeStruct((tile_rows, wide), f32),
            jax.ShapeDtypeStruct((tile_cols, wide), f32),
            jax.ShapeDtypeStruct((depth, tile_cols, wide), bf16),
        ),
        in_specs=[any_spec] * 10,
        out_specs=[any_spec, vmem_spec, vmem_spec, any_spec],
        scratch_shapes=[
            pltpu.VMEM((tile_rows, width), bf16),
            pltpu.VMEM((halves, depth, tile_cols, wide), bf16),
            pltpu.VMEM((mask.shape[0] // LANES, LANES), jnp.int32),
            pltpu.VMEM((heads, wide), bf16),
            pltpu.VMEM(w_project.shape, bf16),
            pltpu.VMEM(w_out.shape, bf16),
            pltpu.VMEM(w_factors.shape, bf16),
            pltpu.VMEM((halves, rows_each, width), bf16),
            pltpu.VMEM((halves, 2, tile_cols, group), bf16),
            pltpu.VMEM((col_size, 2, tile_cols, group), bf16),
            pltpu.VMEM((col_size, tile_rows, group), bf16),
            pltpu.VMEM((halves, depth, group), f32),
            pltpu.VMEM((col_size, halves, rows_each, group), f32),
            pltpu.VMEM((heads * stride, LANES), f32),
            pltpu.VMEM((parts, col_size, halves * rows_each, width // parts), bf16),
            pltpu.VMEM((parts, col_size, halves * rows_each, width // parts), bf16),
            pltpu.VMEM((depth, LANES), f32),
            pltpu.VMEM((col_size, rows_each, LANES), f32),
            pltpu.VMEM((rows_each, LANES), f32),
            pltpu.VMEM((rows_each, LANES), f32),
            pltpu.VMEM((col_size, rows_each, LANES), f32),
            pltpu.VMEM((col_size, rows_each, LANES), f32),
            pltpu.VMEM((halves, rows_each, width), bf16),
            pltpu.VMEM((halves * wide, halves * wide), bf16),
            pltpu.VMEM((halves, 2 * LANES, width), bf16),
            pltpu.VMEM(w_pairout.shape, bf16),
            pltpu.VMEM((2 * wide, 2 * wide), bf16),
            pltpu.VMEM(w_up.shape, bf16),
            pltpu.VMEM(w_down.shape, bf16),
            pltpu.VMEM((depth, tile_cols, wide), bf16),
            pltpu.SemaphoreType.DMA((12 + halves,)),
            pltpu.SemaphoreType.DMA((steps,)),
            pltpu.SemaphoreType.DMA((6, col_size - 1)),
            pltpu.SemaphoreType.DMA((6, col_size - 1)),
            pltpu.SemaphoreType.DMA((2, row_size * halves)),
            pltpu.SemaphoreType.DMA((2, col_size)),
            pltpu.SemaphoreType.DMA((row_size * halves,)),
            pltpu.SemaphoreType.DMA((2, col_size)),
            pltpu.SemaphoreType.DMA((col_size,)),
            pltpu.SemaphoreType.DMA((col_size,)),
            pltpu.SemaphoreType.DMA((col_size,)),
            pltpu.SemaphoreType.DMA((parts, col_size - 1)),
            pltpu.SemaphoreType.DMA((parts, col_size - 1)),
        ],
        compiler_params=pltpu.CompilerParams(collective_id=3, has_side_effects=True),
        name="attend",
    )(
        single,
        pair,
        mask.reshape(mask.shape[0] // LANES, LANES),
        w_bias.T,
        w_project,
        w_out,
        w_factors,
        w_pairout,
        w_up,
        w_down,
    )
    return single_out.reshape(tile_rows, width), left, right, part


def fits(row_size, col_size, single, pair, mask, w_bias, w_project, w_factors):
    tile_rows, tile_cols, wide = pair.shape
    heads = w_bias.shape[1]
    return (
        tile_rows == 2 * tile_cols
        and 2 * tile_cols == LANES
        and wide == LANES
        and w_factors.shape[1] == LANES
        and w_project.shape[2] == LANES
        and 4 * heads == LANES
        and heads % (2 * col_size) == 0
        and tile_cols % (8 * col_size) == 0
        and col_size == 2 * row_size
        and row_size % 2 == 0
        and tile_cols % (2 * update_block) == 0
        and mask.shape[0] % LANES == 0
    )


def per_device_keys(
    row_size, col_size,
    single, pair, residue_mask, w_bias, w_project, w_out, w_factors, w_pairout, w_up, w_down
):
    shape = pair.shape
    pair = pair.reshape(2, shape[0] // 2, *shape[1:])
    single_out, left, right, part = attend(
        single, pair, residue_mask, w_bias, w_project, w_out, w_factors, w_pairout, w_up, w_down,
        row_size, col_size,
    )
    single_out, pair = finish(single_out, pair, part, left, right, w_pairout, w_up, w_down)
    return single_out, pair.reshape(shape)


def dispatch(row_size, col_size, *arrays):
    single, pair, residue_mask, w_bias, w_project, w_out, w_factors = arrays[:7]
    if fits(row_size, col_size, single, pair, residue_mask, w_bias, w_project, w_factors):
        return per_device_keys(row_size, col_size, *arrays)
    return per_device(row_size, col_size, *arrays)


def solution(mesh):
    return jax.shard_map(
        functools.partial(dispatch, mesh.shape["rows"], mesh.shape["cols"]),
        mesh=mesh,
        in_specs=(
            P("rows", None),
            P("rows", "cols", None),
            P(),
            P(),
            P(None, None, "cols"),
            P(),
            P(),
            P(),
            P(),
            P(),
        ),
        out_specs=(P("rows", None), P("rows", "cols", None)),
        check_vma=False,
    )
```

```python
import functools
import math

import jax
import jax.numpy as jnp
from jax import lax
from jax.experimental import pallas as pl
from jax.experimental.pallas import tpu as pltpu
from jax.sharding import PartitionSpec as P

epsilon = 1e-05


def enter(axes):
    barrier = pltpu.get_barrier_semaphore()
    total = 0
    for axis, size in axes:
        me = lax.axis_index(axis)
        for step in range(1, size):
            pl.semaphore_signal(
                barrier,
                inc=1,
                device_id={axis: lax.rem(me + step, size)},
                device_id_type=pl.DeviceIdType.MESH,
            )
        total += size - 1
    pl.semaphore_wait(barrier, total)


def spread(axis, size, source, landing, send_sems, recv_sems):
    me = lax.axis_index(axis)
    copies = []
    for step in range(1, size):
        copy = pltpu.make_async_remote_copy(
            src_ref=source,
            dst_ref=landing.at[me],
            send_sem=send_sems.at[step - 1],
            recv_sem=recv_sems.at[step - 1],
            device_id={axis: lax.rem(me + step, size)},
            device_id_type=pl.DeviceIdType.MESH,
        )
        copy.start()
        copies.append(copy)
    return copies


def gather_kernel(axis, size, source, gathered, send_sems, recv_sems, own_sem):
    enter([(axis, size)])
    copies = spread(axis, size, source, gathered, send_sems, recv_sems)
    own = pltpu.make_async_copy(source, gathered.at[lax.axis_index(axis)], own_sem)
    own.start()
    own.wait()
    for copy in copies:
        copy.wait()


def gather(values, axis, size, collective_id):
    return pl.pallas_call(
        functools.partial(gather_kernel, axis, size),
        out_shape=jax.ShapeDtypeStruct((size, *values.shape), values.dtype),
        in_specs=[pl.BlockSpec(memory_space=pltpu.VMEM)],
        out_specs=pl.BlockSpec(memory_space=pltpu.VMEM),
        scratch_shapes=[
            pltpu.SemaphoreType.DMA((size - 1,)),
            pltpu.SemaphoreType.DMA((size - 1,)),
            pltpu.SemaphoreType.DMA,
        ],
        compiler_params=pltpu.CompilerParams(collective_id=collective_id, has_side_effects=True),
        name="gather_" + axis,
    )(values)


def single_kernel(
    row_size, col_size, tile_cols,
    mixed, single, w_out, w_factors, single_out, left_out, right_out,
    gathered, factor_right, send_sems, recv_sems, row_send, row_recv, own_sem,
):
    enter([("cols", col_size), ("rows", row_size)])
    tile_rows, width = mixed.shape
    me_col = lax.axis_index("cols")
    me_row = lax.axis_index("rows")
    copies = spread("cols", col_size, mixed, gathered, send_sems, recv_sems)
    own = pltpu.make_async_copy(mixed, gathered.at[me_col], own_sem)
    own.start()
    own.wait()
    for copy in copies:
        copy.wait()
    whole = jnp.concatenate([gathered[part] for part in range(col_size)], axis=1)
    total = jnp.dot(whole, w_out[...], preferred_element_type=jnp.float32)
    updated = (single[...].astype(jnp.float32) + total).astype(jnp.bfloat16)
    single_out[...] = updated
    normed = layer_norm(updated).astype(jnp.bfloat16)
    factors = jnp.dot(normed, w_factors[...], preferred_element_type=jnp.float32)
    factors = factors.astype(jnp.bfloat16).astype(jnp.float32)
    half = factors.shape[1] // 2
    swapped = jnp.concatenate([factors[:, half:], factors[:, :half]], axis=1)
    lower = lax.broadcasted_iota(jnp.int32, factors.shape, 1) < half
    left_out[...] = jnp.where(lower, factors, swapped)
    factor_right[...] = jnp.where(lower, swapped, factors).astype(jnp.bfloat16)
    first = me_col * tile_cols
    owner = first // tile_rows
    offset = pl.multiple_of(first - owner * tile_rows, tile_cols)
    piece = factor_right.at[pl.ds(offset, tile_cols)]

    @pl.when(me_row == owner)
    def _():
        local = pltpu.make_async_copy(piece, right_out, own_sem)
        local.start()
        sends = []
        for step in range(1, row_size):
            send = pltpu.make_async_remote_copy(
                src_ref=piece,
                dst_ref=right_out,
                send_sem=row_send.at[step - 1],
                recv_sem=row_recv,
                device_id={"rows": lax.rem(me_row + step, row_size)},
                device_id_type=pl.DeviceIdType.MESH,
            )
            send.start()
            sends.append(send)
        local.wait()
        for send in sends:
            send.wait_send()

    @pl.when(me_row != owner)
    def _():
        pltpu.make_async_remote_copy(
            src_ref=piece,
            dst_ref=right_out,
            send_sem=row_send.at[0],
            recv_sem=row_recv,
            device_id={"rows": lax.rem(me_row + 1, row_size)},
            device_id_type=pl.DeviceIdType.MESH,
        ).wait_recv()


def update_single(mixed, single, w_out, w_factors, row_size, col_size, tile_cols):
    tile_rows, width = single.shape
    wide = w_factors.shape[1]
    return pl.pallas_call(
        functools.partial(single_kernel, row_size, col_size, tile_cols),
        out_shape=(
            jax.ShapeDtypeStruct((tile_rows, width), jnp.bfloat16),
            jax.ShapeDtypeStruct((tile_rows, wide), jnp.float32),
            jax.ShapeDtypeStruct((tile_cols, wide), jnp.bfloat16),
        ),
        in_specs=[pl.BlockSpec(memory_space=pltpu.VMEM)] * 4,
        out_specs=[pl.BlockSpec(memory_space=pltpu.VMEM)] * 3,
        scratch_shapes=[
            pltpu.VMEM((col_size, *mixed.shape), jnp.bfloat16),
            pltpu.VMEM((tile_rows, wide), jnp.bfloat16),
            pltpu.SemaphoreType.DMA((col_size - 1,)),
            pltpu.SemaphoreType.DMA((col_size - 1,)),
            pltpu.SemaphoreType.DMA((row_size - 1,)),
            pltpu.SemaphoreType.DMA,
            pltpu.SemaphoreType.DMA,
        ],
        compiler_params=pltpu.CompilerParams(collective_id=2, has_side_effects=True),
        name="update_single",
    )(mixed, single, w_out, w_factors)


def matmul_norm(values):
    wide = values.shape[1]
    share = jnp.full((2 * wide, wide), 1.0 / wide, jnp.bfloat16)
    mean = jnp.dot(values, share[:wide], preferred_element_type=jnp.float32)
    centred = values.astype(jnp.float32) - mean
    square = centred * centred
    high = square.astype(jnp.bfloat16)
    low = (square - high.astype(jnp.float32)).astype(jnp.bfloat16)
    spread_out = jnp.dot(
        jnp.concatenate([high, low], 1), share, preferred_element_type=jnp.float32
    )
    return (centred * lax.rsqrt(spread_out + epsilon)).astype(jnp.bfloat16)


def norm_kernel(values, normed):
    normed[...] = matmul_norm(values[...])


def norm_rows(values, block):
    spec = pl.BlockSpec((block, values.shape[1]), lambda step: (step, 0))
    return pl.pallas_call(
        norm_kernel,
        out_shape=jax.ShapeDtypeStruct(values.shape, jnp.bfloat16),
        grid=(values.shape[0] // block,),
        in_specs=[spec],
        out_specs=spec,
        name="norm_pair",
    )(values)


def pair_kernel(pair, left, right, w_pairout, w_up, w_down, updated):
    block_rows, tile_cols, wide = pair.shape
    left_wide = left[...][:, None, :]
    right_wide = right[...].astype(jnp.float32)[None, :, :]
    lower = lax.broadcasted_iota(jnp.int32, pair.shape, 2) < wide // 2
    paired = jnp.where(lower, left_wide * right_wide, left_wide - right_wide)
    paired = paired.astype(jnp.bfloat16).reshape(block_rows * tile_cols, wide)
    flat = pair[...].reshape(block_rows * tile_cols, wide).astype(jnp.float32)
    mid = flat + jnp.dot(paired, w_pairout[...], preferred_element_type=jnp.float32)
    mid = mid.astype(jnp.bfloat16)
    normed = matmul_norm(mid)
    hidden = jnp.dot(normed, w_up[...], preferred_element_type=jnp.float32)
    hidden = jnp.maximum(hidden, 0.0).astype(jnp.bfloat16)
    out = mid.astype(jnp.float32) + jnp.dot(
        hidden, w_down[...], preferred_element_type=jnp.float32
    )
    updated[...] = out.astype(jnp.bfloat16).reshape(pair.shape)


def update_pair(pair, left, right, w_pairout, w_up, w_down):
    tile_rows, tile_cols, wide = pair.shape
    block = math.gcd(tile_rows, max(8, 1024 // tile_cols))
    tile = pl.BlockSpec((block, tile_cols, wide), lambda step: (step, 0, 0))

    def whole(array):
        return pl.BlockSpec(array.shape, lambda step: (0, 0))

    return pl.pallas_call(
        pair_kernel,
        out_shape=jax.ShapeDtypeStruct(pair.shape, jnp.bfloat16),
        grid=(tile_rows // block,),
        in_specs=[
            tile,
            pl.BlockSpec((block, wide), lambda step: (step, 0)),
            whole(right),
            whole(w_pairout),
            whole(w_up),
            whole(w_down),
        ],
        out_specs=tile,
        name="update_pair",
    )(pair, left, right, w_pairout, w_up, w_down)


def layer_norm(values):
    values = values.astype(jnp.float32)
    centred = values - jnp.mean(values, -1, keepdims=True)
    return centred * lax.rsqrt(jnp.mean(centred * centred, -1, keepdims=True) + epsilon)


def per_device(
    row_size, col_size,
    single, pair, residue_mask, w_bias, w_project, w_out, w_factors, w_pairout, w_up, w_down
):
    tile_rows = pair.shape[0]
    tile_cols = pair.shape[1]
    normed_pair = norm_rows(
        pair.reshape(tile_rows * tile_cols, pair.shape[2]), math.gcd(tile_rows * tile_cols, 1024)
    ).reshape(pair.shape)
    bias_local = jnp.einsum(
        "rcp,ph->hrc", normed_pair, w_bias, preferred_element_type=jnp.float32
    ).astype(jnp.bfloat16)
    normed_single = layer_norm(single).astype(jnp.bfloat16)
    projected = jnp.einsum(
        "rs,fsc->frc", normed_single, w_project, preferred_element_type=jnp.float32
    )
    query_rows = projected[0].astype(jnp.bfloat16)
    key_local = projected[1].astype(jnp.bfloat16)
    value_local = projected[2].astype(jnp.bfloat16)
    gate_values = jax.nn.sigmoid(projected[3])
    bias_heads = lax.all_to_all(bias_local, "cols", split_axis=0, concat_axis=2, tiled=True)
    both = gather(jnp.concatenate([key_local, value_local], 1), "rows", row_size, 1)
    both = both.reshape(row_size * tile_rows, both.shape[2])
    key_rows, value_rows = both[:, : key_local.shape[1]], both[:, key_local.shape[1] :]
    heads_here = bias_heads.shape[0]
    head_width = query_rows.shape[1] // heads_here
    residues = key_rows.shape[0]
    query_split = query_rows.reshape(tile_rows, heads_here, head_width)
    key_split = key_rows.reshape(residues, heads_here, head_width)
    value_split = value_rows.reshape(residues, heads_here, head_width)
    score_scale = 1.0 / math.sqrt(head_width)
    scores = jnp.einsum(
        "rhd,lhd->hrl", query_split, key_split, preferred_element_type=jnp.float32
    ) * score_scale + bias_heads.astype(jnp.float32)
    key_valid = (residue_mask > 0)[None, None, :]
    scores = jnp.where(key_valid, scores, -jnp.inf)
    weights = jax.nn.softmax(scores, axis=-1).astype(jnp.bfloat16)
    attended = jnp.einsum("hrl,lhd->rhd", weights, value_split, preferred_element_type=jnp.float32)
    attended = attended.reshape(tile_rows, heads_here * head_width)
    mixed = (attended * gate_values).astype(jnp.bfloat16)
    single_out, left, right = update_single(
        mixed, single, w_out, w_factors, row_size, col_size, tile_cols
    )
    return (single_out, update_pair(pair, left, right, w_pairout, w_up, w_down))


LANES = 128
excluded = -1e30
update_block = 16


def lane_iota(shape):
    return lax.broadcasted_iota(jnp.int32, shape, len(shape) - 1)


def centre_matrix(wide, copies):
    size = wide * copies
    row = lax.broadcasted_iota(jnp.int32, (size, size), 0)
    col = lax.broadcasted_iota(jnp.int32, (size, size), 1)
    share = jnp.where(row // wide == col // wide, 1.0 / wide, 0.0)
    return (jnp.where(row == col, 1.0, 0.0) - share).astype(jnp.bfloat16)


def norm_centred(values, centre, copies):
    centred = jnp.dot(values, centre, preferred_element_type=jnp.float32)
    wide = values.shape[1] // copies
    parts = []
    for index in range(copies):
        part = centred[:, index * wide : (index + 1) * wide]
        square = jnp.sum(part * part, axis=1, keepdims=True) * (1.0 / wide)
        parts.append((part * lax.rsqrt(square + epsilon)).astype(jnp.bfloat16))
    return parts


def twice(weights):
    zeros = jnp.zeros_like(weights)
    upper = jnp.concatenate([weights, zeros], axis=1)
    return jnp.concatenate([upper, jnp.concatenate([zeros, weights], axis=1)], axis=0)


def update_rows(pair_of, left_of, right, rows, centre, w_pairout, w_up, w_down):
    tile_cols, wide = right.shape
    lower = lane_iota((rows, tile_cols, wide)) < wide // 2

    def paired(index):
        left_wide = left_of(index)[:, None, :]
        right_wide = right[None, :, :]
        chosen = jnp.where(lower, left_wide * right_wide, left_wide - right_wide)
        return chosen.astype(jnp.bfloat16).reshape(rows * tile_cols, wide)

    flat = [pair_of(index).reshape(rows * tile_cols, wide) for index in range(2)]
    mid = jnp.concatenate(flat, axis=1).astype(jnp.float32) + jnp.dot(
        jnp.concatenate([paired(0), paired(1)], axis=1),
        w_pairout,
        preferred_element_type=jnp.float32,
    )
    mid = mid.astype(jnp.bfloat16)
    normed = jnp.concatenate(norm_centred(mid, centre, 2), axis=0)
    mid = jnp.concatenate([mid[:, :wide], mid[:, wide:]], axis=0)
    hidden = jnp.dot(normed, w_up, preferred_element_type=jnp.float32)
    hidden = jnp.maximum(hidden, 0.0).astype(jnp.bfloat16)
    out = mid.astype(jnp.float32) + jnp.dot(hidden, w_down, preferred_element_type=jnp.float32)
    return out.astype(jnp.bfloat16).reshape(2 * rows, tile_cols, wide)


def attend_kernel(
    row_size, col_size, heads, tile_cols, stride,
    single, pair, mask, w_bias, w_project, w_out, w_factors, w_pairout, w_up, w_down,
    single_out, left_out, right_out, part_out,
    single_v, pair_v, mask_v, bias_w, project_v, out_v, factors_v, own_single,
    kv_send, kv_recv, q_recv, gate_send, gate_recv, bias_v, o_send, o_recv,
    st_send, st_recv, left_send, right_send, left_recv, right_recv, so_send, centre_v, spread_v,
    pairout_v, twice_v, up_v, down_v, part_v,
    load_sems, pair_sems, col_send, col_recv, fan_send, fan_recv,
    plane_sent, plane_came, kv_sent, kv_came, kv_relayed, q_sent, q_came, o_sent, o_came,
):
    me_row = lax.axis_index("rows")
    me_col = lax.axis_index("cols")
    total = row_size * col_size
    barrier = pltpu.get_barrier_semaphore()
    me = me_row * col_size + me_col
    for step in range(1, total):
        to = lax.rem(me + step, total)
        pl.semaphore_signal(
            barrier,
            inc=1,
            device_id={"rows": to // col_size, "cols": lax.rem(to, col_size)},
            device_id_type=pl.DeviceIdType.MESH,
        )
    halves, depth, _, wide = pair.shape
    tile_rows, width = single.shape
    group = w_project.shape[2]
    rows_each = depth // col_size
    heads_here = heads // col_size
    head_width = group // heads_here
    chunk = depth // pair_sems.shape[0]
    loads = [
        pltpu.make_async_copy(source, target, load_sems.at[index])
        for index, (source, target) in enumerate(
            [(single, single_v)]
            + [(w_project.at[part], project_v.at[part]) for part in range(4)]
            + [(w_bias, bias_w), (mask, mask_v)]
            + [
                (single.at[pl.ds(half * depth + me_col * rows_each, rows_each)], own_single.at[half])
                for half in range(halves)
            ]
            + [(w_out, out_v), (w_factors, factors_v)]
            + [(w_pairout, pairout_v), (w_up, up_v), (w_down, down_v)]
        )
    ]
    for copy in loads[:7]:
        copy.start()

    def pair_load(step):
        part = pl.ds(step * chunk, chunk)
        return pltpu.make_async_copy(pair.at[:, part], pair_v.at[:, part], pair_sems.at[step])

    for step in range(depth // chunk):
        pair_load(step).start()
    for copy in loads[7:]:
        copy.start()

    centre_v[...] = centre_matrix(wide, halves)

    def to_cols(kind, source_of, target):
        copies = []
        for step in range(1, col_size):
            to = lax.rem(me_col + step, col_size)
            copy = pltpu.make_async_remote_copy(
                src_ref=source_of(to),
                dst_ref=target,
                send_sem=col_send.at[kind, step - 1],
                recv_sem=col_recv.at[kind, step - 1],
                device_id={"cols": to},
                device_id_type=pl.DeviceIdType.MESH,
            )
            copy.start()
            copies.append(copy)
        return copies

    owner = me_col // halves
    mine = owner == me_row
    half_mine = lax.rem(me_col, halves)

    def fan_copies(kind, source_of, target):
        copies = []
        for step in range(row_size):
            for half in range(halves):
                to = halves * me_row + half
                copy = pltpu.make_async_remote_copy(
                    src_ref=source_of(half),
                    dst_ref=target.at[me_col],
                    send_sem=fan_send.at[kind, step * halves + half],
                    recv_sem=fan_recv.at[kind, me_col],
                    device_id={"rows": lax.rem(me_row + step, row_size), "cols": to},
                    device_id_type=pl.DeviceIdType.MESH,
                )
                copies.append((copy, step, to))
        return copies

    def on_some(copies, act):
        for copy, condition in copies:
            if condition is None:
                act(copy)
            else:
                pl.when(condition)(functools.partial(act, copy))

    kind_mine = lax.rem(me_row, 2)
    me_plane = me_row // 2
    row_mate = me_row + 1 - 2 * kind_mine
    col_mate = me_col + 1 - 2 * lax.rem(me_col, 2)

    def relay_keys(part, kind, slot):
        return pltpu.make_async_remote_copy(
            src_ref=kv_recv.at[part, kind],
            dst_ref=kv_recv.at[part, kind],
            send_sem=kv_relayed.at[slot],
            recv_sem=kv_came.at[kind, part],
            device_id={"rows": row_mate},
            device_id_type=pl.DeviceIdType.MESH,
        )

    def send_query(part, to, slot):
        return pltpu.make_async_remote_copy(
            src_ref=q_recv.at[part],
            dst_ref=q_recv.at[part],
            send_sem=q_sent.at[slot],
            recv_sem=q_came.at[part],
            device_id={"cols": to},
            device_id_type=pl.DeviceIdType.MESH,
        )

    def on_fan(copies, act):
        for copy, step, to in copies:
            if step:
                act(copy)
            else:
                pl.when(to != me_col)(functools.partial(act, copy))

    def fan_wait(kind, source_of, target):
        for part in range(col_size):
            copy = pltpu.make_async_remote_copy(
                src_ref=source_of(0),
                dst_ref=target.at[part],
                send_sem=fan_send.at[kind, 0],
                recv_sem=fan_recv.at[kind, part],
                device_id={"rows": lax.rem(me_row + 1, row_size)},
                device_id_type=pl.DeviceIdType.MESH,
            )
            pl.when(jnp.logical_not(jnp.logical_and(mine, part == me_col)))(copy.wait_recv)

    loads[0].wait()
    normed = layer_norm(single_v[...]).astype(jnp.bfloat16)
    def project(*kinds):
        weights = [project_v[kind] for kind in kinds]
        return jnp.dot(
            normed, jnp.concatenate(weights, axis=1), preferred_element_type=jnp.float32
        )

    loads[1].wait()
    q_recv[me_col] = project(0).astype(jnp.bfloat16)
    pl.semaphore_wait(barrier, total - 1)
    peers = [lax.rem(me_col + 2 * step, col_size) for step in range(1, col_size // 2)]
    q_copies = [send_query(me_col, to, slot) for slot, to in enumerate(peers)]
    q_copies.append(send_query(me_col, col_mate, len(peers)))
    for copy in q_copies:
        copy.start()
    loads[2].wait()
    loads[3].wait()
    key_value = project(1, 2).astype(jnp.bfloat16)
    for half in range(halves):
        for kind in range(2):
            kv_send[me_plane, half, kind] = key_value[
                half * tile_cols : (half + 1) * tile_cols, kind * group : (kind + 1) * group
            ]
    planes = row_size // 2
    plane_copies = []
    for step in range(1, planes):
        plane = lax.rem(me_plane + step, planes)
        copy = pltpu.make_async_remote_copy(
            src_ref=kv_send.at[me_plane],
            dst_ref=kv_send.at[me_plane],
            send_sem=plane_sent.at[step - 1],
            recv_sem=plane_came.at[step - 1],
            device_id={"rows": 2 * plane + kind_mine},
            device_id_type=pl.DeviceIdType.MESH,
        )
        copy.start()
        plane_copies.append(copy)
    kv_copies = []

    def send_keys(step):
        plane = lax.rem(me_plane + planes - step, planes)
        for half in range(halves):
            for kind in range(2):
                to = halves * (2 * plane + kind_mine) + half
                row = 2 * me_plane + kind
                copy = pltpu.make_async_remote_copy(
                    src_ref=kv_send.at[plane, half, kind],
                    dst_ref=kv_recv.at[me_col, kind],
                    send_sem=kv_sent.at[(step * 2 + kind) * halves + half],
                    recv_sem=kv_came.at[kind, me_col],
                    device_id={"rows": row, "cols": to},
                    device_id_type=pl.DeviceIdType.MESH,
                )
                here = jnp.logical_and(row == me_row, to == me_col)
                kv_copies.append((copy, jnp.logical_not(here)))
        on_some(kv_copies[-2 * halves :], lambda copy: copy.start())

    send_keys(0)
    loads[4].wait()
    gate_send[...] = jax.nn.sigmoid(project(3)).reshape(halves, depth, group)

    def own_rows(to):
        return pl.ds(pl.multiple_of(to * rows_each, rows_each), rows_each)

    loads[5].wait()
    loads[6].wait()

    def bias_step(step, _):
        pair_load(step).wait()
        parts = [
            pair_v[half, pl.ds(step * chunk, chunk)].reshape(chunk * tile_cols, wide)
            for half in range(halves)
        ]
        parts = norm_centred(jnp.concatenate(parts, axis=1), centre_v[...], halves)
        parts = [part.reshape(chunk, 1, tile_cols, wide) for part in parts]
        normed_pair = jnp.concatenate(parts, axis=1).reshape(chunk * halves * tile_cols, wide)
        bias = lax.dot_general(
            bias_w[...], normed_pair, (((1,), (1,)), ((), ())), preferred_element_type=jnp.float32
        )
        bias = bias.astype(jnp.bfloat16).astype(jnp.float32)
        for part in range(chunk):
            bias_v[pl.ds(step * chunk + part, heads, stride=stride), :] = bias[
                :, part * LANES : (part + 1) * LANES
            ]
        return 0

    lax.fori_loop(0, depth // chunk, bias_step, 0)

    lane_row = lane_iota((2 * halves * heads, width))
    place = lax.broadcasted_iota(jnp.int32, (2 * halves * heads, width), 0)
    for half in range(halves):
        picked = jnp.where(place == half * heads + lane_row // head_width, 1.0, 0.0)
        spread_v[half, :LANES] = picked.astype(jnp.bfloat16)
        spread_v[half, LANES:] = picked.astype(jnp.bfloat16)

    for step in range(1, planes):
        plane_copies[step - 1].wait_recv()
        send_keys(step)
    own_key = lax.rem(owner, 2) == kind_mine

    @pl.when(own_key)
    def _():
        kv_recv[me_col, kind_mine] = kv_send[owner // 2, half_mine, kind_mine]

    length = jnp.sum(jnp.sum(mask_v[...], axis=1, keepdims=True), axis=0, keepdims=True)
    lane = lane_iota((depth, LANES))
    low = lane < tile_cols
    valid = me_col * tile_cols + lax.rem(lane, tile_cols) < length
    head_of = lane_iota((tile_cols, group)) // head_width
    head_masks = [
        jnp.where(head_of == head, 1.0, 0.0).astype(jnp.bfloat16) for head in range(heads_here)
    ]
    zeros = jnp.zeros((tile_cols, group), jnp.bfloat16)
    scale = 1.0 / math.sqrt(head_width)
    st_send[...] = jnp.zeros_like(st_send)
    block_place = lax.broadcasted_iota(jnp.int32, (heads_here * LANES, LANES), 0) // tile_cols
    block_target = (
        halves * heads + lax.rem(block_place, halves) * heads + block_place // halves
    )
    block_lane = lane_iota((heads_here * LANES, LANES))

    def attend_part(part):
        query = q_recv[part]
        query = jnp.concatenate([query[:depth], query[depth:]], axis=1)
        key, value = kv_recv[part, 0], kv_recv[part, 1]
        weights, value_rows = [], []
        stats = st_send[...]
        for first in range(0, heads_here, 2):
            key_rows = []
            for head in (first, first + 1):
                masked = key * head_masks[head]
                key_rows.append(jnp.concatenate([masked, zeros], axis=1))
                key_rows.append(jnp.concatenate([zeros, masked], axis=1))
            raw = lax.dot_general(
                query,
                jnp.concatenate(key_rows, axis=0),
                (((1,), (1,)), ((), ())),
                preferred_element_type=jnp.float32,
            )
            for head in (first, first + 1):
                index = part * heads_here + head
                bias = bias_v[pl.ds(pl.multiple_of(index * stride, 8), depth), :]
                scores = raw[:, (head - first) * LANES : (head - first + 1) * LANES] * scale + bias
                scores = jnp.where(valid, scores, excluded)
                top0 = jnp.max(jnp.where(low, scores, excluded), axis=1, keepdims=True)
                top1 = jnp.max(jnp.where(low, excluded, scores), axis=1, keepdims=True)
                weights.append(
                    jnp.exp(scores - jnp.where(low, top0, top1)).astype(jnp.bfloat16)
                )
                stats = jnp.where(lane == index, top0, stats)
                stats = jnp.where(lane == heads + index, top1, stats)
        for head in range(heads_here):
            masked = value * head_masks[head]
            value_rows.append(jnp.concatenate([masked, zeros], axis=1))
            value_rows.append(jnp.concatenate([zeros, masked], axis=1))
        weights = jnp.concatenate(weights, axis=1)
        mixed = jnp.dot(
            weights, jnp.concatenate(value_rows, axis=0), preferred_element_type=jnp.float32
        )
        ones = jnp.where(block_lane == block_target + part * heads_here, 1.0, 0.0)
        sums = jnp.dot(weights, ones.astype(jnp.bfloat16), preferred_element_type=jnp.float32)
        st_send[...] = stats + sums
        pieces = [
            mixed[:, half * group : (half + 1) * group].reshape(col_size, rows_each, group)
            for half in range(halves)
        ]
        return jnp.concatenate(pieces, axis=1).astype(jnp.bfloat16)

    parts, _, _, part_width = o_send.shape
    each = part_width // group
    col_side = lax.rem(me_col, each)

    def o_copy(step, shift):
        to = lax.rem(me_col + shift, col_size)
        return pltpu.make_async_remote_copy(
            src_ref=o_send.at[step, to],
            dst_ref=o_recv.at[step, me_col],
            send_sem=o_sent.at[step, shift - 1],
            recv_sem=o_came.at[step, shift - 1],
            device_id={"cols": to},
            device_id_type=pl.DeviceIdType.MESH,
        )

    def relay_query(part):
        return send_query(part, col_mate, col_size // 2 + part // each)

    def attend_step(turn, _):
        step = lax.rem(me_col // each + turn, parts)
        near = step * each + col_side
        far = step * each + 1 - col_side

        @pl.when(turn > 0)
        def _():
            relay_query(near).wait_recv()
            relay_query(near).start()

        for index in range(each):
            part = step * each + index
            copy = relay_keys(part, kind_mine, part)
            own = jnp.logical_and(own_key, part == me_col)
            pl.when(jnp.logical_not(own))(copy.wait_recv)
            copy.start()
        relay_query(far).wait_recv()
        for index in range(each):
            part = step * each + index
            relay_keys(part, 1 - kind_mine, part).wait_recv()
        for index in range(each):
            o_send[step, :, :, index * group : (index + 1) * group] = attend_part(
                step * each + index
            )
        for shift in range(1, col_size):
            o_copy(step, shift).start()
        return 0

    lax.fori_loop(0, parts, attend_step, 0)
    relays = [relay_keys(part, kind_mine, part) for part in range(col_size)]
    relays += [relay_query(peer) for peer in peers]
    gate_copies = to_cols(1, lambda to: gate_send.at[:, own_rows(to)], gate_recv.at[me_col])
    gate_recv[me_col] = gate_send[:, own_rows(me_col)]

    st_copies = to_cols(2, lambda to: st_send.at[own_rows(to)], st_recv.at[me_col])
    st_recv[me_col] = st_send[own_rows(me_col)]
    for step in range(parts):
        o_recv[step, me_col] = o_send[step, me_col]
    o_copies = [o_copy(step, shift) for step in range(parts) for shift in range(1, col_size)]
    for copy in gate_copies + st_copies:
        copy.wait_recv()
    stats = st_recv[...]
    lane = lane_iota(stats.shape)
    top = jnp.max(stats, axis=0, keepdims=True)
    factor = jnp.exp(stats - top)
    sums = jnp.sum(factor * pltpu.roll(stats, halves * heads, axis=2), axis=0, keepdims=True)
    factor = jnp.where(lane < halves * heads, factor / sums, 0.0)
    factor = factor.reshape(col_size * rows_each, LANES)
    high = factor.astype(jnp.bfloat16)
    rest = (factor - high.astype(jnp.float32)).astype(jnp.bfloat16)
    factor = jnp.concatenate([high, rest], axis=1)
    scales = [
        jnp.dot(factor, spread_v[half], preferred_element_type=jnp.float32) for half in range(halves)
    ]
    gate = jnp.concatenate(
        [gate_recv[part].reshape(halves * rows_each, group) for part in range(col_size)], axis=1
    )
    for copy in o_copies:
        copy.wait_recv()
    attended = jnp.zeros((halves * rows_each, width), jnp.float32)
    for part in range(col_size):
        rows = slice(part * rows_each, (part + 1) * rows_each)
        part_scale = jnp.concatenate([scales[half][rows] for half in range(halves)], axis=0)
        whole = jnp.concatenate([o_recv[step, part] for step in range(parts)], axis=1)
        attended = attended + part_scale * whole.astype(jnp.float32)
    mixed = (attended * gate).astype(jnp.bfloat16)
    for copy in loads[7:]:
        copy.wait()
    added = jnp.dot(mixed, out_v[...], preferred_element_type=jnp.float32)
    own = own_single[...].astype(jnp.float32).reshape(halves * rows_each, width)
    updated = (own + added).astype(jnp.bfloat16)
    so_send[...] = updated.astype(jnp.float32).reshape(halves, rows_each, width).astype(jnp.bfloat16)
    factors = jnp.dot(
        layer_norm(updated).astype(jnp.bfloat16),
        factors_v[...],
        preferred_element_type=jnp.float32,
    )
    factors = factors.astype(jnp.bfloat16).astype(jnp.float32)
    first, second = factors[:rows_each], factors[rows_each:]
    shift = factors.shape[1] // 2
    low = lane_iota(first.shape) < shift
    left = jnp.where(low, first, pltpu.roll(second, shift, axis=1))
    right = jnp.where(low, pltpu.roll(first, shift, axis=1), second)
    left_send[...] = left
    right_send[...] = right
    right_copies = fan_copies(1, lambda half: right_send, right_recv)
    on_fan(right_copies, lambda copy: copy.start())
    left_copies = to_cols(4, lambda to: left_send, left_recv.at[me_col])
    so_copies = to_cols(5, lambda to: so_send, single_out.at[:, me_col])
    own_copy = pltpu.make_async_copy(so_send, single_out.at[:, me_col], load_sems.at[0])
    own_copy.start()
    left_recv[me_col] = left

    @pl.when(mine)
    def _():
        right_recv[me_col] = right_send[...]

    fan_wait(1, lambda half: right_send, right_recv)
    for copy in left_copies:
        copy.wait_recv()
    left = left_recv[...].reshape(depth, LANES)
    turned = pltpu.roll(left, shift, axis=1)
    low = lane_iota(left.shape) < shift
    left_out[:depth] = jnp.where(low, left, turned)
    left_out[depth:] = jnp.where(low, turned, left)
    right = right_recv[...].reshape(tile_cols, LANES)
    turned = pltpu.roll(right, shift, axis=1)
    right_out[...] = jnp.where(lane_iota(right.shape) // shift == half_mine, right, turned)

    twice_v[...] = twice(pairout_v[...])
    block = update_block
    starts = part_v.shape[0] // (2 * block)

    def part_copy(step):
        rows = pl.ds(step * 2 * block, 2 * block)
        return pltpu.make_async_copy(part_v.at[rows], part_out.at[rows], pair_sems.at[step])

    def update_step(step, _):
        first = step * 2 * block
        half = first // depth
        part_v[pl.ds(first, 2 * block)] = update_rows(
            lambda index: pair_v[half, pl.ds(first - half * depth + index * block, block)],
            lambda index: left_out[pl.ds(pl.multiple_of(first + index * block, 8), block)],
            right_out[...],
            block,
            centre_v[...],
            twice_v[...],
            up_v[...],
            down_v[...],
        )
        part_copy(step).start()
        return 0

    lax.fori_loop(0, starts, update_step, 0)

    for copies in (q_copies, relays, plane_copies, gate_copies, st_copies, o_copies, left_copies, so_copies):
        for copy in copies:
            copy.wait_send()
    on_some(kv_copies, lambda copy: copy.wait_send())
    on_fan(right_copies, lambda copy: copy.wait_send())
    for copy in so_copies:
        copy.wait_recv()
    own_copy.wait()
    for step in range(starts):
        part_copy(step).wait()


def finish_kernel(
    single, pair, part, left, right, w_pairout, w_up, w_down,
    single_out, pair_out,
    single_v, pair_v, part_v, done_v, left_v, right_v, pairout_v, up_v, down_v,
    centre_v, twice_v, sems, out_sems,
):
    tile_rows, tile_cols, wide = pair.shape
    done = part.shape[0]
    block = (tile_rows - done) // 2
    rows = pl.ds(done, 2 * block)
    loads = [
        pltpu.make_async_copy(source, target, sems.at[index])
        for index, (source, target) in enumerate(
            [
                (w_pairout, pairout_v),
                (pair.at[rows], pair_v),
                (left.at[rows], left_v),
                (right, right_v),
                (w_up, up_v),
                (w_down, down_v),
                (part, part_v),
                (single, single_v),
            ]
        )
    ]
    for copy in loads:
        copy.start()
    stores = [
        pltpu.make_async_copy(part_v, pair_out.at[pl.ds(0, done)], out_sems.at[0]),
        pltpu.make_async_copy(single_v, single_out, out_sems.at[1]),
        pltpu.make_async_copy(done_v, pair_out.at[rows], out_sems.at[2]),
    ]
    centre_v[...] = centre_matrix(wide, 2)
    for copy in loads[:6]:
        copy.wait()
    twice_v[...] = twice(pairout_v[...])
    for copy, store in zip(loads[6:], stores):
        copy.wait()
        store.start()
    done_v[...] = update_rows(
        lambda index: pair_v[index * block : (index + 1) * block],
        lambda index: left_v[index * block : (index + 1) * block],
        right_v[...],
        block,
        centre_v[...],
        twice_v[...],
        up_v[...],
        down_v[...],
    )
    stores[2].start()
    for store in stores:
        store.wait()


def finish(single, pair, part, left, right, w_pairout, w_up, w_down):
    tile_rows, tile_cols, wide = pair.shape
    done = part.shape[0]
    any_spec = pl.BlockSpec(memory_space=pl.ANY)
    bf16, f32 = jnp.bfloat16, jnp.float32
    return pl.pallas_call(
        finish_kernel,
        out_shape=(
            jax.ShapeDtypeStruct(single.shape, bf16),
            jax.ShapeDtypeStruct(pair.shape, bf16),
        ),
        in_specs=[any_spec] * 8,
        out_specs=[any_spec] * 2,
        scratch_shapes=[
            pltpu.VMEM(single.shape, bf16),
            pltpu.VMEM((tile_rows - done, tile_cols, wide), bf16),
            pltpu.VMEM(part.shape, bf16),
            pltpu.VMEM((tile_rows - done, tile_cols, wide), bf16),
            pltpu.VMEM((tile_rows - done, wide), f32),
            pltpu.VMEM(right.shape, f32),
            pltpu.VMEM(w_pairout.shape, bf16),
            pltpu.VMEM(w_up.shape, bf16),
            pltpu.VMEM(w_down.shape, bf16),
            pltpu.VMEM((2 * wide, 2 * wide), bf16),
            pltpu.VMEM((2 * wide, 2 * wide), bf16),
            pltpu.SemaphoreType.DMA((8,)),
            pltpu.SemaphoreType.DMA((3,)),
        ],
        name="finish",
    )(single, pair, part, left, right, w_pairout, w_up, w_down)


def attend(
    single, pair, mask, w_bias, w_project, w_out, w_factors, w_pairout, w_up, w_down,
    row_size, col_size,
):
    halves, depth, tile_cols, wide = pair.shape
    tile_rows, width = single.shape
    heads = w_bias.shape[1]
    rows_each = depth // col_size
    group = w_project.shape[2]
    steps = depth // 16
    parts = col_size // 2
    part_rows = tile_rows - 2 * update_block
    stride = depth + 8
    any_spec = pl.BlockSpec(memory_space=pl.ANY)
    vmem_spec = pl.BlockSpec(memory_space=pltpu.VMEM)
    bf16, f32 = jnp.bfloat16, jnp.float32
    single_out, left, right, part = pl.pallas_call(
        functools.partial(attend_kernel, row_size, col_size, heads, tile_cols, stride),
        out_shape=(
            jax.ShapeDtypeStruct((halves, col_size, rows_each, width), bf16),
            jax.ShapeDtypeStruct((tile_rows, wide), f32),
            jax.ShapeDtypeStruct((tile_cols, wide), f32),
            jax.ShapeDtypeStruct((part_rows, tile_cols, wide), bf16),
        ),
        in_specs=[any_spec] * 10,
        out_specs=[any_spec, vmem_spec, vmem_spec, any_spec],
        scratch_shapes=[
            pltpu.VMEM((tile_rows, width), bf16),
            pltpu.VMEM((halves, depth, tile_cols, wide), bf16),
            pltpu.VMEM((mask.shape[0] // LANES, LANES), jnp.int32),
            pltpu.VMEM((heads, wide), bf16),
            pltpu.VMEM(w_project.shape, bf16),
            pltpu.VMEM(w_out.shape, bf16),
            pltpu.VMEM(w_factors.shape, bf16),
            pltpu.VMEM((halves, rows_each, width), bf16),
            pltpu.VMEM((row_size // 2, halves, 2, tile_cols, group), bf16),
            pltpu.VMEM((col_size, 2, tile_cols, group), bf16),
            pltpu.VMEM((col_size, tile_rows, group), bf16),
            pltpu.VMEM((halves, depth, group), f32),
            pltpu.VMEM((col_size, halves, rows_each, group), f32),
            pltpu.VMEM((heads * stride, LANES), f32),
            pltpu.VMEM((parts, col_size, halves * rows_each, width // parts), bf16),
            pltpu.VMEM((parts, col_size, halves * rows_each, width // parts), bf16),
            pltpu.VMEM((depth, LANES), f32),
            pltpu.VMEM((col_size, rows_each, LANES), f32),
            pltpu.VMEM((rows_each, LANES), f32),
            pltpu.VMEM((rows_each, LANES), f32),
            pltpu.VMEM((col_size, rows_each, LANES), f32),
            pltpu.VMEM((col_size, rows_each, LANES), f32),
            pltpu.VMEM((halves, rows_each, width), bf16),
            pltpu.VMEM((halves * wide, halves * wide), bf16),
            pltpu.VMEM((halves, 2 * LANES, width), bf16),
            pltpu.VMEM(w_pairout.shape, bf16),
            pltpu.VMEM((2 * wide, 2 * wide), bf16),
            pltpu.VMEM(w_up.shape, bf16),
            pltpu.VMEM(w_down.shape, bf16),
            pltpu.VMEM((part_rows, tile_cols, wide), bf16),
            pltpu.SemaphoreType.DMA((12 + halves,)),
            pltpu.SemaphoreType.DMA((steps,)),
            pltpu.SemaphoreType.DMA((6, col_size - 1)),
            pltpu.SemaphoreType.DMA((6, col_size - 1)),
            pltpu.SemaphoreType.DMA((2, row_size * halves)),
            pltpu.SemaphoreType.DMA((2, col_size)),
            pltpu.SemaphoreType.DMA((row_size // 2 - 1,)),
            pltpu.SemaphoreType.DMA((row_size // 2 - 1,)),
            pltpu.SemaphoreType.DMA((row_size * halves,)),
            pltpu.SemaphoreType.DMA((2, col_size)),
            pltpu.SemaphoreType.DMA((col_size,)),
            pltpu.SemaphoreType.DMA((2 * col_size,)),
            pltpu.SemaphoreType.DMA((col_size,)),
            pltpu.SemaphoreType.DMA((parts, col_size - 1)),
            pltpu.SemaphoreType.DMA((parts, col_size - 1)),
        ],
        compiler_params=pltpu.CompilerParams(collective_id=3, has_side_effects=True),
        name="attend",
    )(
        single,
        pair,
        mask.reshape(mask.shape[0] // LANES, LANES),
        w_bias.T,
        w_project,
        w_out,
        w_factors,
        w_pairout,
        w_up,
        w_down,
    )
    return single_out.reshape(tile_rows, width), left, right, part


def fits(row_size, col_size, single, pair, mask, w_bias, w_project, w_factors):
    tile_rows, tile_cols, wide = pair.shape
    heads = w_bias.shape[1]
    return (
        tile_rows == 2 * tile_cols
        and 2 * tile_cols == LANES
        and wide == LANES
        and w_factors.shape[1] == LANES
        and w_project.shape[2] == LANES
        and 4 * heads == LANES
        and heads % (2 * col_size) == 0
        and tile_cols % (8 * col_size) == 0
        and col_size == 2 * row_size
        and row_size % 2 == 0
        and tile_cols % (2 * update_block) == 0
        and mask.shape[0] % LANES == 0
    )


def per_device_keys(
    row_size, col_size,
    single, pair, residue_mask, w_bias, w_project, w_out, w_factors, w_pairout, w_up, w_down
):
    shape = pair.shape
    single_out, left, right, part = attend(
        single, pair.reshape(2, shape[0] // 2, *shape[1:]), residue_mask,
        w_bias, w_project, w_out, w_factors, w_pairout, w_up, w_down, row_size, col_size,
    )
    return tuple(finish(single_out, pair, part, left, right, w_pairout, w_up, w_down))


def dispatch(row_size, col_size, *arrays):
    single, pair, residue_mask, w_bias, w_project, w_out, w_factors = arrays[:7]
    if fits(row_size, col_size, single, pair, residue_mask, w_bias, w_project, w_factors):
        return per_device_keys(row_size, col_size, *arrays)
    return per_device(row_size, col_size, *arrays)


def solution(mesh):
    return jax.shard_map(
        functools.partial(dispatch, mesh.shape["rows"], mesh.shape["cols"]),
        mesh=mesh,
        in_specs=(
            P("rows", None),
            P("rows", "cols", None),
            P(),
            P(),
            P(None, None, "cols"),
            P(),
            P(),
            P(),
            P(),
            P(),
        ),
        out_specs=(P("rows", None), P("rows", "cols", None)),
        check_vma=False,
    )
```

```python
import functools
import math

import jax
import jax.numpy as jnp
from jax import lax
from jax.experimental import pallas as pl
from jax.experimental.pallas import tpu as pltpu
from jax.sharding import PartitionSpec as P

epsilon = 1e-05


def enter(axes):
    barrier = pltpu.get_barrier_semaphore()
    total = 0
    for axis, size in axes:
        me = lax.axis_index(axis)
        for step in range(1, size):
            pl.semaphore_signal(
                barrier,
                inc=1,
                device_id={axis: lax.rem(me + step, size)},
                device_id_type=pl.DeviceIdType.MESH,
            )
        total += size - 1
    pl.semaphore_wait(barrier, total)


def spread(axis, size, source, landing, send_sems, recv_sems):
    me = lax.axis_index(axis)
    copies = []
    for step in range(1, size):
        copy = pltpu.make_async_remote_copy(
            src_ref=source,
            dst_ref=landing.at[me],
            send_sem=send_sems.at[step - 1],
            recv_sem=recv_sems.at[step - 1],
            device_id={axis: lax.rem(me + step, size)},
            device_id_type=pl.DeviceIdType.MESH,
        )
        copy.start()
        copies.append(copy)
    return copies


def gather_kernel(axis, size, source, gathered, send_sems, recv_sems, own_sem):
    enter([(axis, size)])
    copies = spread(axis, size, source, gathered, send_sems, recv_sems)
    own = pltpu.make_async_copy(source, gathered.at[lax.axis_index(axis)], own_sem)
    own.start()
    own.wait()
    for copy in copies:
        copy.wait()


def gather(values, axis, size, collective_id):
    return pl.pallas_call(
        functools.partial(gather_kernel, axis, size),
        out_shape=jax.ShapeDtypeStruct((size, *values.shape), values.dtype),
        in_specs=[pl.BlockSpec(memory_space=pltpu.VMEM)],
        out_specs=pl.BlockSpec(memory_space=pltpu.VMEM),
        scratch_shapes=[
            pltpu.SemaphoreType.DMA((size - 1,)),
            pltpu.SemaphoreType.DMA((size - 1,)),
            pltpu.SemaphoreType.DMA,
        ],
        compiler_params=pltpu.CompilerParams(collective_id=collective_id, has_side_effects=True),
        name="gather_" + axis,
    )(values)


def single_kernel(
    row_size, col_size, tile_cols,
    mixed, single, w_out, w_factors, single_out, left_out, right_out,
    gathered, factor_right, send_sems, recv_sems, row_send, row_recv, own_sem,
):
    enter([("cols", col_size), ("rows", row_size)])
    tile_rows, width = mixed.shape
    me_col = lax.axis_index("cols")
    me_row = lax.axis_index("rows")
    copies = spread("cols", col_size, mixed, gathered, send_sems, recv_sems)
    own = pltpu.make_async_copy(mixed, gathered.at[me_col], own_sem)
    own.start()
    own.wait()
    for copy in copies:
        copy.wait()
    whole = jnp.concatenate([gathered[part] for part in range(col_size)], axis=1)
    total = jnp.dot(whole, w_out[...], preferred_element_type=jnp.float32)
    updated = (single[...].astype(jnp.float32) + total).astype(jnp.bfloat16)
    single_out[...] = updated
    normed = layer_norm(updated).astype(jnp.bfloat16)
    factors = jnp.dot(normed, w_factors[...], preferred_element_type=jnp.float32)
    factors = factors.astype(jnp.bfloat16).astype(jnp.float32)
    half = factors.shape[1] // 2
    swapped = jnp.concatenate([factors[:, half:], factors[:, :half]], axis=1)
    lower = lax.broadcasted_iota(jnp.int32, factors.shape, 1) < half
    left_out[...] = jnp.where(lower, factors, swapped)
    factor_right[...] = jnp.where(lower, swapped, factors).astype(jnp.bfloat16)
    first = me_col * tile_cols
    owner = first // tile_rows
    offset = pl.multiple_of(first - owner * tile_rows, tile_cols)
    piece = factor_right.at[pl.ds(offset, tile_cols)]

    @pl.when(me_row == owner)
    def _():
        local = pltpu.make_async_copy(piece, right_out, own_sem)
        local.start()
        sends = []
        for step in range(1, row_size):
            send = pltpu.make_async_remote_copy(
                src_ref=piece,
                dst_ref=right_out,
                send_sem=row_send.at[step - 1],
                recv_sem=row_recv,
                device_id={"rows": lax.rem(me_row + step, row_size)},
                device_id_type=pl.DeviceIdType.MESH,
            )
            send.start()
            sends.append(send)
        local.wait()
        for send in sends:
            send.wait_send()

    @pl.when(me_row != owner)
    def _():
        pltpu.make_async_remote_copy(
            src_ref=piece,
            dst_ref=right_out,
            send_sem=row_send.at[0],
            recv_sem=row_recv,
            device_id={"rows": lax.rem(me_row + 1, row_size)},
            device_id_type=pl.DeviceIdType.MESH,
        ).wait_recv()


def update_single(mixed, single, w_out, w_factors, row_size, col_size, tile_cols):
    tile_rows, width = single.shape
    wide = w_factors.shape[1]
    return pl.pallas_call(
        functools.partial(single_kernel, row_size, col_size, tile_cols),
        out_shape=(
            jax.ShapeDtypeStruct((tile_rows, width), jnp.bfloat16),
            jax.ShapeDtypeStruct((tile_rows, wide), jnp.float32),
            jax.ShapeDtypeStruct((tile_cols, wide), jnp.bfloat16),
        ),
        in_specs=[pl.BlockSpec(memory_space=pltpu.VMEM)] * 4,
        out_specs=[pl.BlockSpec(memory_space=pltpu.VMEM)] * 3,
        scratch_shapes=[
            pltpu.VMEM((col_size, *mixed.shape), jnp.bfloat16),
            pltpu.VMEM((tile_rows, wide), jnp.bfloat16),
            pltpu.SemaphoreType.DMA((col_size - 1,)),
            pltpu.SemaphoreType.DMA((col_size - 1,)),
            pltpu.SemaphoreType.DMA((row_size - 1,)),
            pltpu.SemaphoreType.DMA,
            pltpu.SemaphoreType.DMA,
        ],
        compiler_params=pltpu.CompilerParams(collective_id=2, has_side_effects=True),
        name="update_single",
    )(mixed, single, w_out, w_factors)


def matmul_norm(values):
    wide = values.shape[1]
    share = jnp.full((2 * wide, wide), 1.0 / wide, jnp.bfloat16)
    mean = jnp.dot(values, share[:wide], preferred_element_type=jnp.float32)
    centred = values.astype(jnp.float32) - mean
    square = centred * centred
    high = square.astype(jnp.bfloat16)
    low = (square - high.astype(jnp.float32)).astype(jnp.bfloat16)
    spread_out = jnp.dot(
        jnp.concatenate([high, low], 1), share, preferred_element_type=jnp.float32
    )
    return (centred * lax.rsqrt(spread_out + epsilon)).astype(jnp.bfloat16)


def norm_kernel(values, normed):
    normed[...] = matmul_norm(values[...])


def norm_rows(values, block):
    spec = pl.BlockSpec((block, values.shape[1]), lambda step: (step, 0))
    return pl.pallas_call(
        norm_kernel,
        out_shape=jax.ShapeDtypeStruct(values.shape, jnp.bfloat16),
        grid=(values.shape[0] // block,),
        in_specs=[spec],
        out_specs=spec,
        name="norm_pair",
    )(values)


def pair_kernel(pair, left, right, w_pairout, w_up, w_down, updated):
    block_rows, tile_cols, wide = pair.shape
    left_wide = left[...][:, None, :]
    right_wide = right[...].astype(jnp.float32)[None, :, :]
    lower = lax.broadcasted_iota(jnp.int32, pair.shape, 2) < wide // 2
    paired = jnp.where(lower, left_wide * right_wide, left_wide - right_wide)
    paired = paired.astype(jnp.bfloat16).reshape(block_rows * tile_cols, wide)
    flat = pair[...].reshape(block_rows * tile_cols, wide).astype(jnp.float32)
    mid = flat + jnp.dot(paired, w_pairout[...], preferred_element_type=jnp.float32)
    mid = mid.astype(jnp.bfloat16)
    normed = matmul_norm(mid)
    hidden = jnp.dot(normed, w_up[...], preferred_element_type=jnp.float32)
    hidden = jnp.maximum(hidden, 0.0).astype(jnp.bfloat16)
    out = mid.astype(jnp.float32) + jnp.dot(
        hidden, w_down[...], preferred_element_type=jnp.float32
    )
    updated[...] = out.astype(jnp.bfloat16).reshape(pair.shape)


def update_pair(pair, left, right, w_pairout, w_up, w_down):
    tile_rows, tile_cols, wide = pair.shape
    block = math.gcd(tile_rows, max(8, 1024 // tile_cols))
    tile = pl.BlockSpec((block, tile_cols, wide), lambda step: (step, 0, 0))

    def whole(array):
        return pl.BlockSpec(array.shape, lambda step: (0, 0))

    return pl.pallas_call(
        pair_kernel,
        out_shape=jax.ShapeDtypeStruct(pair.shape, jnp.bfloat16),
        grid=(tile_rows // block,),
        in_specs=[
            tile,
            pl.BlockSpec((block, wide), lambda step: (step, 0)),
            whole(right),
            whole(w_pairout),
            whole(w_up),
            whole(w_down),
        ],
        out_specs=tile,
        name="update_pair",
    )(pair, left, right, w_pairout, w_up, w_down)


def layer_norm(values):
    values = values.astype(jnp.float32)
    centred = values - jnp.mean(values, -1, keepdims=True)
    return centred * lax.rsqrt(jnp.mean(centred * centred, -1, keepdims=True) + epsilon)


def per_device(
    row_size, col_size,
    single, pair, residue_mask, w_bias, w_project, w_out, w_factors, w_pairout, w_up, w_down
):
    tile_rows = pair.shape[0]
    tile_cols = pair.shape[1]
    normed_pair = norm_rows(
        pair.reshape(tile_rows * tile_cols, pair.shape[2]), math.gcd(tile_rows * tile_cols, 1024)
    ).reshape(pair.shape)
    bias_local = jnp.einsum(
        "rcp,ph->hrc", normed_pair, w_bias, preferred_element_type=jnp.float32
    ).astype(jnp.bfloat16)
    normed_single = layer_norm(single).astype(jnp.bfloat16)
    projected = jnp.einsum(
        "rs,fsc->frc", normed_single, w_project, preferred_element_type=jnp.float32
    )
    query_rows = projected[0].astype(jnp.bfloat16)
    key_local = projected[1].astype(jnp.bfloat16)
    value_local = projected[2].astype(jnp.bfloat16)
    gate_values = jax.nn.sigmoid(projected[3])
    bias_heads = lax.all_to_all(bias_local, "cols", split_axis=0, concat_axis=2, tiled=True)
    both = gather(jnp.concatenate([key_local, value_local], 1), "rows", row_size, 1)
    both = both.reshape(row_size * tile_rows, both.shape[2])
    key_rows, value_rows = both[:, : key_local.shape[1]], both[:, key_local.shape[1] :]
    heads_here = bias_heads.shape[0]
    head_width = query_rows.shape[1] // heads_here
    residues = key_rows.shape[0]
    query_split = query_rows.reshape(tile_rows, heads_here, head_width)
    key_split = key_rows.reshape(residues, heads_here, head_width)
    value_split = value_rows.reshape(residues, heads_here, head_width)
    score_scale = 1.0 / math.sqrt(head_width)
    scores = jnp.einsum(
        "rhd,lhd->hrl", query_split, key_split, preferred_element_type=jnp.float32
    ) * score_scale + bias_heads.astype(jnp.float32)
    key_valid = (residue_mask > 0)[None, None, :]
    scores = jnp.where(key_valid, scores, -jnp.inf)
    weights = jax.nn.softmax(scores, axis=-1).astype(jnp.bfloat16)
    attended = jnp.einsum("hrl,lhd->rhd", weights, value_split, preferred_element_type=jnp.float32)
    attended = attended.reshape(tile_rows, heads_here * head_width)
    mixed = (attended * gate_values).astype(jnp.bfloat16)
    single_out, left, right = update_single(
        mixed, single, w_out, w_factors, row_size, col_size, tile_cols
    )
    return (single_out, update_pair(pair, left, right, w_pairout, w_up, w_down))


LANES = 128
excluded = -1e30
update_block = 16


def lane_iota(shape):
    return lax.broadcasted_iota(jnp.int32, shape, len(shape) - 1)


def centre_matrix(wide, copies):
    size = wide * copies
    row = lax.broadcasted_iota(jnp.int32, (size, size), 0)
    col = lax.broadcasted_iota(jnp.int32, (size, size), 1)
    share = jnp.where(row // wide == col // wide, 1.0 / wide, 0.0)
    return (jnp.where(row == col, 1.0, 0.0) - share).astype(jnp.bfloat16)


def norm_centred(values, centre, copies):
    centred = jnp.dot(values, centre, preferred_element_type=jnp.float32)
    wide = values.shape[1] // copies
    parts = []
    for index in range(copies):
        part = centred[:, index * wide : (index + 1) * wide]
        square = jnp.sum(part * part, axis=1, keepdims=True) * (1.0 / wide)
        parts.append((part * lax.rsqrt(square + epsilon)).astype(jnp.bfloat16))
    return parts


def twice(weights):
    zeros = jnp.zeros_like(weights)
    upper = jnp.concatenate([weights, zeros], axis=1)
    return jnp.concatenate([upper, jnp.concatenate([zeros, weights], axis=1)], axis=0)


def update_rows(pair_of, left_of, right, rows, centre, w_pairout, w_up, w_down):
    tile_cols, wide = right.shape
    lower = lane_iota((rows, tile_cols, wide)) < wide // 2

    def paired(index):
        left_wide = left_of(index)[:, None, :]
        right_wide = right[None, :, :]
        chosen = jnp.where(lower, left_wide * right_wide, left_wide - right_wide)
        return chosen.astype(jnp.bfloat16).reshape(rows * tile_cols, wide)

    flat = [pair_of(index).reshape(rows * tile_cols, wide) for index in range(2)]
    mid = jnp.concatenate(flat, axis=1).astype(jnp.float32) + jnp.dot(
        jnp.concatenate([paired(0), paired(1)], axis=1),
        w_pairout,
        preferred_element_type=jnp.float32,
    )
    mid = mid.astype(jnp.bfloat16)
    normed = jnp.concatenate(norm_centred(mid, centre, 2), axis=0)
    mid = jnp.concatenate([mid[:, :wide], mid[:, wide:]], axis=0)
    hidden = jnp.dot(normed, w_up, preferred_element_type=jnp.float32)
    hidden = jnp.maximum(hidden, 0.0).astype(jnp.bfloat16)
    out = mid.astype(jnp.float32) + jnp.dot(hidden, w_down, preferred_element_type=jnp.float32)
    return out.astype(jnp.bfloat16).reshape(2 * rows, tile_cols, wide)


def attend_kernel(
    row_size, col_size, heads, tile_cols, stride,
    single, pair, mask, w_bias, w_project, w_out, w_factors, w_pairout, w_up, w_down,
    single_out, left_out, right_out, part_out,
    single_v, pair_v, mask_v, bias_w, project_v, out_v, factors_v, own_single,
    kv_send, kv_recv, q_recv, gate_send, gate_recv, bias_v, o_send, o_recv,
    st_send, st_recv, left_send, right_send, left_recv, right_recv, so_send, centre_v, spread_v,
    pairout_v, twice_v, up_v, down_v, part_v,
    load_sems, pair_sems, col_send, col_recv, fan_send, fan_recv,
    plane_sent, plane_came, kv_sent, kv_came, kv_relayed, q_sent, q_came, o_sent, o_came,
):
    me_row = lax.axis_index("rows")
    me_col = lax.axis_index("cols")
    total = row_size * col_size
    halves, depth, _, wide = pair.shape
    tile_rows, width = single.shape
    group = w_project.shape[2]
    rows_each = depth // col_size
    heads_here = heads // col_size
    head_width = group // heads_here
    chunk = depth // pair_sems.shape[0]
    loads = [
        pltpu.make_async_copy(source, target, load_sems.at[index])
        for index, (source, target) in enumerate(
            [(single, single_v)]
            + [(w_project.at[part], project_v.at[part]) for part in range(4)]
            + [(w_bias, bias_w), (mask, mask_v)]
            + [
                (single.at[pl.ds(half * depth + me_col * rows_each, rows_each)], own_single.at[half])
                for half in range(halves)
            ]
            + [(w_out, out_v), (w_factors, factors_v)]
            + [(w_pairout, pairout_v), (w_up, up_v), (w_down, down_v)]
        )
    ]
    for copy in loads[:7]:
        copy.start()
    barrier = pltpu.get_barrier_semaphore()
    me = me_row * col_size + me_col
    for step in range(1, total):
        to = lax.rem(me + step, total)
        pl.semaphore_signal(
            barrier,
            inc=1,
            device_id={"rows": to // col_size, "cols": lax.rem(to, col_size)},
            device_id_type=pl.DeviceIdType.MESH,
        )

    def pair_load(step):
        part = pl.ds(step * chunk, chunk)
        return pltpu.make_async_copy(pair.at[:, part], pair_v.at[:, part], pair_sems.at[step])

    for step in range(depth // chunk):
        pair_load(step).start()
    for copy in loads[7:]:
        copy.start()

    centre_v[...] = centre_matrix(wide, halves)

    def to_cols(kind, source_of, target):
        copies = []
        for step in range(1, col_size):
            to = lax.rem(me_col + step, col_size)
            copy = pltpu.make_async_remote_copy(
                src_ref=source_of(to),
                dst_ref=target,
                send_sem=col_send.at[kind, step - 1],
                recv_sem=col_recv.at[kind, step - 1],
                device_id={"cols": to},
                device_id_type=pl.DeviceIdType.MESH,
            )
            copy.start()
            copies.append(copy)
        return copies

    owner = me_col // halves
    mine = owner == me_row
    half_mine = lax.rem(me_col, halves)

    def fan_copies(kind, source_of, target):
        copies = []
        for step in range(row_size):
            for half in range(halves):
                to = halves * me_row + half
                copy = pltpu.make_async_remote_copy(
                    src_ref=source_of(half),
                    dst_ref=target.at[me_col],
                    send_sem=fan_send.at[kind, step * halves + half],
                    recv_sem=fan_recv.at[kind, me_col],
                    device_id={"rows": lax.rem(me_row + step, row_size), "cols": to},
                    device_id_type=pl.DeviceIdType.MESH,
                )
                copies.append((copy, step, to))
        return copies

    def on_some(copies, act):
        for copy, condition in copies:
            if condition is None:
                act(copy)
            else:
                pl.when(condition)(functools.partial(act, copy))

    kind_mine = lax.rem(me_row, 2)
    me_plane = me_row // 2
    row_mate = me_row + 1 - 2 * kind_mine
    col_mate = me_col + 1 - 2 * lax.rem(me_col, 2)

    def relay_keys(part, kind, slot):
        return pltpu.make_async_remote_copy(
            src_ref=kv_recv.at[part, kind],
            dst_ref=kv_recv.at[part, kind],
            send_sem=kv_relayed.at[slot],
            recv_sem=kv_came.at[kind, part],
            device_id={"rows": row_mate},
            device_id_type=pl.DeviceIdType.MESH,
        )

    def send_query(part, to, slot):
        return pltpu.make_async_remote_copy(
            src_ref=q_recv.at[part],
            dst_ref=q_recv.at[part],
            send_sem=q_sent.at[slot],
            recv_sem=q_came.at[part],
            device_id={"cols": to},
            device_id_type=pl.DeviceIdType.MESH,
        )

    def on_fan(copies, act):
        for copy, step, to in copies:
            if step:
                act(copy)
            else:
                pl.when(to != me_col)(functools.partial(act, copy))

    def fan_wait(kind, source_of, target):
        for part in range(col_size):
            copy = pltpu.make_async_remote_copy(
                src_ref=source_of(0),
                dst_ref=target.at[part],
                send_sem=fan_send.at[kind, 0],
                recv_sem=fan_recv.at[kind, part],
                device_id={"rows": lax.rem(me_row + 1, row_size)},
                device_id_type=pl.DeviceIdType.MESH,
            )
            pl.when(jnp.logical_not(jnp.logical_and(mine, part == me_col)))(copy.wait_recv)

    loads[0].wait()
    normed = layer_norm(single_v[...]).astype(jnp.bfloat16)
    def project(*kinds):
        weights = [project_v[kind] for kind in kinds]
        return jnp.dot(
            normed, jnp.concatenate(weights, axis=1), preferred_element_type=jnp.float32
        )

    loads[1].wait()
    q_recv[me_col] = project(0).astype(jnp.bfloat16)
    pl.semaphore_wait(barrier, total - 1)
    peers = [lax.rem(me_col + 2 * step, col_size) for step in range(1, col_size // 2)]
    q_copies = [send_query(me_col, to, slot) for slot, to in enumerate(peers)]
    q_copies.append(send_query(me_col, col_mate, len(peers)))
    for copy in q_copies:
        copy.start()
    loads[2].wait()
    loads[3].wait()
    key_value = project(1, 2).astype(jnp.bfloat16)
    for half in range(halves):
        for kind in range(2):
            kv_send[me_plane, half, kind] = key_value[
                half * tile_cols : (half + 1) * tile_cols, kind * group : (kind + 1) * group
            ]
    planes = row_size // 2
    plane_copies = []
    for step in range(1, planes):
        plane = lax.rem(me_plane + step, planes)
        copy = pltpu.make_async_remote_copy(
            src_ref=kv_send.at[me_plane],
            dst_ref=kv_send.at[me_plane],
            send_sem=plane_sent.at[step - 1],
            recv_sem=plane_came.at[step - 1],
            device_id={"rows": 2 * plane + kind_mine},
            device_id_type=pl.DeviceIdType.MESH,
        )
        copy.start()
        plane_copies.append(copy)
    kv_copies = []

    def send_keys(step):
        plane = lax.rem(me_plane + planes - step, planes)
        for half in range(halves):
            for kind in range(2):
                to = halves * (2 * plane + kind_mine) + half
                row = 2 * me_plane + kind
                copy = pltpu.make_async_remote_copy(
                    src_ref=kv_send.at[plane, half, kind],
                    dst_ref=kv_recv.at[me_col, kind],
                    send_sem=kv_sent.at[(step * 2 + kind) * halves + half],
                    recv_sem=kv_came.at[kind, me_col],
                    device_id={"rows": row, "cols": to},
                    device_id_type=pl.DeviceIdType.MESH,
                )
                here = jnp.logical_and(row == me_row, to == me_col)
                kv_copies.append((copy, jnp.logical_not(here)))
        on_some(kv_copies[-2 * halves :], lambda copy: copy.start())

    send_keys(0)
    loads[4].wait()
    gate_send[...] = jax.nn.sigmoid(project(3)).reshape(halves, depth, group)

    def own_rows(to):
        return pl.ds(pl.multiple_of(to * rows_each, rows_each), rows_each)

    loads[5].wait()
    loads[6].wait()

    parts, _, _, part_width = o_send.shape
    each = part_width // group
    col_side = lax.rem(me_col, each)

    def relay_query(part):
        return send_query(part, col_mate, col_size // 2 + part // each)

    def bias_step(step, _):
        pair_load(step).wait()
        parts = [
            pair_v[half, pl.ds(step * chunk, chunk)].reshape(chunk * tile_cols, wide)
            for half in range(halves)
        ]
        parts = norm_centred(jnp.concatenate(parts, axis=1), centre_v[...], halves)
        parts = [part.reshape(chunk, 1, tile_cols, wide) for part in parts]
        normed_pair = jnp.concatenate(parts, axis=1).reshape(chunk * halves * tile_cols, wide)
        bias = lax.dot_general(
            bias_w[...], normed_pair, (((1,), (1,)), ((), ())), preferred_element_type=jnp.float32
        )
        bias = bias.astype(jnp.bfloat16).astype(jnp.float32)
        for part in range(chunk):
            bias_v[pl.ds(step * chunk + part, heads, stride=stride), :] = bias[
                :, part * LANES : (part + 1) * LANES
            ]
        return 0

    bias_steps = depth // chunk
    lax.fori_loop(0, bias_steps // 2, bias_step, 0)
    for step in range(1, planes):
        plane_copies[step - 1].wait_recv()
        send_keys(step)
    own_key = lax.rem(owner, 2) == kind_mine

    @pl.when(own_key)
    def _():
        kv_recv[me_col, kind_mine] = kv_send[owner // 2, half_mine, kind_mine]

    lax.fori_loop(bias_steps // 2, bias_steps, bias_step, 0)
    relays = [relay_query(peer) for peer in peers]
    for copy in relays:
        copy.wait_recv()
        copy.start()
    for turn in range(parts):
        for index in range(each):
            part = lax.rem(me_col // each + turn, parts) * each + index
            copy = relay_keys(part, kind_mine, part)
            own = jnp.logical_and(own_key, part == me_col)
            pl.when(jnp.logical_not(own))(copy.wait_recv)
            copy.start()
            relays.append(copy)
    gate_copies = to_cols(1, lambda to: gate_send.at[:, own_rows(to)], gate_recv.at[me_col])
    gate_recv[me_col] = gate_send[:, own_rows(me_col)]

    lane_row = lane_iota((2 * halves * heads, width))
    place = lax.broadcasted_iota(jnp.int32, (2 * halves * heads, width), 0)
    for half in range(halves):
        picked = jnp.where(place == half * heads + lane_row // head_width, 1.0, 0.0)
        spread_v[half, :LANES] = picked.astype(jnp.bfloat16)
        spread_v[half, LANES:] = picked.astype(jnp.bfloat16)

    length = jnp.sum(jnp.sum(mask_v[...], axis=1, keepdims=True), axis=0, keepdims=True)
    lane = lane_iota((depth, LANES))
    low = lane < tile_cols
    valid = me_col * tile_cols + lax.rem(lane, tile_cols) < length
    head_of = lane_iota((tile_cols, group)) // head_width
    head_masks = [
        jnp.where(head_of == head, 1.0, 0.0).astype(jnp.bfloat16) for head in range(heads_here)
    ]
    zeros = jnp.zeros((tile_cols, group), jnp.bfloat16)
    scale = 1.0 / math.sqrt(head_width)
    st_send[...] = jnp.zeros_like(st_send)
    block_place = lax.broadcasted_iota(jnp.int32, (heads_here * LANES, LANES), 0) // tile_cols
    block_target = (
        halves * heads + lax.rem(block_place, halves) * heads + block_place // halves
    )
    block_lane = lane_iota((heads_here * LANES, LANES))

    def attend_part(part):
        query = q_recv[part]
        query = jnp.concatenate([query[:depth], query[depth:]], axis=1)
        key, value = kv_recv[part, 0], kv_recv[part, 1]
        weights, value_rows = [], []
        stats = st_send[...]
        for first in range(0, heads_here, 2):
            key_rows = []
            for head in (first, first + 1):
                masked = key * head_masks[head]
                key_rows.append(jnp.concatenate([masked, zeros], axis=1))
                key_rows.append(jnp.concatenate([zeros, masked], axis=1))
            raw = lax.dot_general(
                query,
                jnp.concatenate(key_rows, axis=0),
                (((1,), (1,)), ((), ())),
                preferred_element_type=jnp.float32,
            )
            for head in (first, first + 1):
                index = part * heads_here + head
                bias = bias_v[pl.ds(pl.multiple_of(index * stride, 8), depth), :]
                scores = raw[:, (head - first) * LANES : (head - first + 1) * LANES] * scale + bias
                scores = jnp.where(valid, scores, excluded)
                top0 = jnp.max(jnp.where(low, scores, excluded), axis=1, keepdims=True)
                top1 = jnp.max(jnp.where(low, excluded, scores), axis=1, keepdims=True)
                weights.append(
                    jnp.exp(scores - jnp.where(low, top0, top1)).astype(jnp.bfloat16)
                )
                stats = jnp.where(lane == index, top0, stats)
                stats = jnp.where(lane == heads + index, top1, stats)
        for head in range(heads_here):
            masked = value * head_masks[head]
            value_rows.append(jnp.concatenate([masked, zeros], axis=1))
            value_rows.append(jnp.concatenate([zeros, masked], axis=1))
        weights = jnp.concatenate(weights, axis=1)
        mixed = jnp.dot(
            weights, jnp.concatenate(value_rows, axis=0), preferred_element_type=jnp.float32
        )
        ones = jnp.where(block_lane == block_target + part * heads_here, 1.0, 0.0)
        sums = jnp.dot(weights, ones.astype(jnp.bfloat16), preferred_element_type=jnp.float32)
        st_send[...] = stats + sums
        pieces = [
            mixed[:, half * group : (half + 1) * group].reshape(col_size, rows_each, group)
            for half in range(halves)
        ]
        return jnp.concatenate(pieces, axis=1).astype(jnp.bfloat16)

    def o_copy(step, shift):
        to = lax.rem(me_col + shift, col_size)
        return pltpu.make_async_remote_copy(
            src_ref=o_send.at[step, to],
            dst_ref=o_recv.at[step, me_col],
            send_sem=o_sent.at[step, shift - 1],
            recv_sem=o_came.at[step, shift - 1],
            device_id={"cols": to},
            device_id_type=pl.DeviceIdType.MESH,
        )

    def attend_step(turn, _):
        step = lax.rem(me_col // each + turn, parts)
        far = step * each + 1 - col_side
        relay_query(far).wait_recv()
        for index in range(each):
            part = step * each + index
            relay_keys(part, 1 - kind_mine, part).wait_recv()
        for index in range(each):
            o_send[step, :, :, index * group : (index + 1) * group] = attend_part(
                step * each + index
            )
        for shift in range(1, col_size):
            o_copy(step, shift).start()
        return 0

    lax.fori_loop(0, parts, attend_step, 0)
    st_copies = to_cols(2, lambda to: st_send.at[own_rows(to)], st_recv.at[me_col])
    st_recv[me_col] = st_send[own_rows(me_col)]
    for step in range(parts):
        o_recv[step, me_col] = o_send[step, me_col]
    o_copies = [o_copy(step, shift) for step in range(parts) for shift in range(1, col_size)]
    for copy in gate_copies + st_copies:
        copy.wait_recv()
    stats = st_recv[...]
    lane = lane_iota(stats.shape)
    top = jnp.max(stats, axis=0, keepdims=True)
    factor = jnp.exp(stats - top)
    sums = jnp.sum(factor * pltpu.roll(stats, halves * heads, axis=2), axis=0, keepdims=True)
    factor = jnp.where(lane < halves * heads, factor / sums, 0.0)
    factor = factor.reshape(col_size * rows_each, LANES)
    high = factor.astype(jnp.bfloat16)
    rest = (factor - high.astype(jnp.float32)).astype(jnp.bfloat16)
    factor = jnp.concatenate([high, rest], axis=1)
    scales = [
        jnp.dot(factor, spread_v[half], preferred_element_type=jnp.float32) for half in range(halves)
    ]
    gate = jnp.concatenate(
        [gate_recv[part].reshape(halves * rows_each, group) for part in range(col_size)], axis=1
    )
    for copy in o_copies:
        copy.wait_recv()
    attended = jnp.zeros((halves * rows_each, width), jnp.float32)
    for part in range(col_size):
        rows = slice(part * rows_each, (part + 1) * rows_each)
        part_scale = jnp.concatenate([scales[half][rows] for half in range(halves)], axis=0)
        whole = jnp.concatenate([o_recv[step, part] for step in range(parts)], axis=1)
        attended = attended + part_scale * whole.astype(jnp.float32)
    mixed = (attended * gate).astype(jnp.bfloat16)
    for copy in loads[7:]:
        copy.wait()
    added = jnp.dot(mixed, out_v[...], preferred_element_type=jnp.float32)
    own = own_single[...].astype(jnp.float32).reshape(halves * rows_each, width)
    updated = (own + added).astype(jnp.bfloat16)
    so_send[...] = updated.astype(jnp.float32).reshape(halves, rows_each, width).astype(jnp.bfloat16)
    factors = jnp.dot(
        layer_norm(updated).astype(jnp.bfloat16),
        factors_v[...],
        preferred_element_type=jnp.float32,
    )
    factors = factors.astype(jnp.bfloat16).astype(jnp.float32)
    first, second = factors[:rows_each], factors[rows_each:]
    shift = factors.shape[1] // 2
    low = lane_iota(first.shape) < shift
    left = jnp.where(low, first, pltpu.roll(second, shift, axis=1))
    right = jnp.where(low, pltpu.roll(first, shift, axis=1), second)
    left_send[...] = left
    right_send[...] = right
    right_copies = fan_copies(1, lambda half: right_send, right_recv)
    on_fan(right_copies, lambda copy: copy.start())
    left_copies = to_cols(4, lambda to: left_send, left_recv.at[me_col])
    left_recv[me_col] = left

    @pl.when(mine)
    def _():
        right_recv[me_col] = right_send[...]

    fan_wait(1, lambda half: right_send, right_recv)
    for copy in left_copies:
        copy.wait_recv()
    so_copies = to_cols(5, lambda to: so_send, single_out.at[:, me_col])
    own_copy = pltpu.make_async_copy(so_send, single_out.at[:, me_col], load_sems.at[0])
    own_copy.start()
    left = left_recv[...].reshape(depth, LANES)
    turned = pltpu.roll(left, shift, axis=1)
    low = lane_iota(left.shape) < shift
    left_out[:depth] = jnp.where(low, left, turned)
    left_out[depth:] = jnp.where(low, turned, left)
    right = right_recv[...].reshape(tile_cols, LANES)
    turned = pltpu.roll(right, shift, axis=1)
    right_out[...] = jnp.where(lane_iota(right.shape) // shift == half_mine, right, turned)

    twice_v[...] = twice(pairout_v[...])
    block = update_block
    starts = part_v.shape[0] // (2 * block)

    def part_copy(step):
        rows = pl.ds(step * 2 * block, 2 * block)
        return pltpu.make_async_copy(part_v.at[rows], part_out.at[rows], pair_sems.at[step])

    def update_step(step, _):
        first = step * 2 * block
        half = first // depth
        part_v[pl.ds(first, 2 * block)] = update_rows(
            lambda index: pair_v[half, pl.ds(first - half * depth + index * block, block)],
            lambda index: left_out[pl.ds(pl.multiple_of(first + index * block, 8), block)],
            right_out[...],
            block,
            centre_v[...],
            twice_v[...],
            up_v[...],
            down_v[...],
        )
        part_copy(step).start()
        return 0

    lax.fori_loop(0, starts, update_step, 0)

    for copies in (q_copies, relays, plane_copies, gate_copies, st_copies, o_copies, left_copies, so_copies):
        for copy in copies:
            copy.wait_send()
    on_some(kv_copies, lambda copy: copy.wait_send())
    on_fan(right_copies, lambda copy: copy.wait_send())
    for copy in so_copies:
        copy.wait_recv()
    own_copy.wait()
    for step in range(starts):
        part_copy(step).wait()


def finish_kernel(
    single, pair, part, left, right, w_pairout, w_up, w_down,
    single_out, pair_out,
    single_v, pair_v, part_v, done_v, left_v, right_v, pairout_v, up_v, down_v,
    centre_v, twice_v, sems, out_sems,
):
    tile_rows, tile_cols, wide = pair.shape
    done = part.shape[0]
    block = (tile_rows - done) // 2
    rows = pl.ds(done, 2 * block)
    loads = [
        pltpu.make_async_copy(source, target, sems.at[index])
        for index, (source, target) in enumerate(
            [
                (w_pairout, pairout_v),
                (pair.at[rows], pair_v),
                (left.at[rows], left_v),
                (right, right_v),
                (w_up, up_v),
                (w_down, down_v),
                (part, part_v),
                (single, single_v),
            ]
        )
    ]
    for copy in loads:
        copy.start()
    stores = [
        pltpu.make_async_copy(part_v, pair_out.at[pl.ds(0, done)], out_sems.at[0]),
        pltpu.make_async_copy(single_v, single_out, out_sems.at[1]),
        pltpu.make_async_copy(done_v, pair_out.at[rows], out_sems.at[2]),
    ]
    centre_v[...] = centre_matrix(wide, 2)
    for copy in loads[:6]:
        copy.wait()
    twice_v[...] = twice(pairout_v[...])
    for copy, store in zip(loads[6:], stores):
        copy.wait()
        store.start()
    done_v[...] = update_rows(
        lambda index: pair_v[index * block : (index + 1) * block],
        lambda index: left_v[index * block : (index + 1) * block],
        right_v[...],
        block,
        centre_v[...],
        twice_v[...],
        up_v[...],
        down_v[...],
    )
    stores[2].start()
    for store in stores:
        store.wait()


def finish(single, pair, part, left, right, w_pairout, w_up, w_down):
    tile_rows, tile_cols, wide = pair.shape
    done = part.shape[0]
    any_spec = pl.BlockSpec(memory_space=pl.ANY)
    bf16, f32 = jnp.bfloat16, jnp.float32
    return pl.pallas_call(
        finish_kernel,
        out_shape=(
            jax.ShapeDtypeStruct(single.shape, bf16),
            jax.ShapeDtypeStruct(pair.shape, bf16),
        ),
        in_specs=[any_spec] * 8,
        out_specs=[any_spec] * 2,
        scratch_shapes=[
            pltpu.VMEM(single.shape, bf16),
            pltpu.VMEM((tile_rows - done, tile_cols, wide), bf16),
            pltpu.VMEM(part.shape, bf16),
            pltpu.VMEM((tile_rows - done, tile_cols, wide), bf16),
            pltpu.VMEM((tile_rows - done, wide), f32),
            pltpu.VMEM(right.shape, f32),
            pltpu.VMEM(w_pairout.shape, bf16),
            pltpu.VMEM(w_up.shape, bf16),
            pltpu.VMEM(w_down.shape, bf16),
            pltpu.VMEM((2 * wide, 2 * wide), bf16),
            pltpu.VMEM((2 * wide, 2 * wide), bf16),
            pltpu.SemaphoreType.DMA((8,)),
            pltpu.SemaphoreType.DMA((3,)),
        ],
        name="finish",
    )(single, pair, part, left, right, w_pairout, w_up, w_down)


def attend(
    single, pair, mask, w_bias, w_project, w_out, w_factors, w_pairout, w_up, w_down,
    row_size, col_size,
):
    halves, depth, tile_cols, wide = pair.shape
    tile_rows, width = single.shape
    heads = w_bias.shape[1]
    rows_each = depth // col_size
    group = w_project.shape[2]
    steps = depth // 16
    parts = col_size // 2
    part_rows = tile_rows - 2 * update_block
    stride = depth + 8
    any_spec = pl.BlockSpec(memory_space=pl.ANY)
    vmem_spec = pl.BlockSpec(memory_space=pltpu.VMEM)
    bf16, f32 = jnp.bfloat16, jnp.float32
    single_out, left, right, part = pl.pallas_call(
        functools.partial(attend_kernel, row_size, col_size, heads, tile_cols, stride),
        out_shape=(
            jax.ShapeDtypeStruct((halves, col_size, rows_each, width), bf16),
            jax.ShapeDtypeStruct((tile_rows, wide), f32),
            jax.ShapeDtypeStruct((tile_cols, wide), f32),
            jax.ShapeDtypeStruct((part_rows, tile_cols, wide), bf16),
        ),
        in_specs=[any_spec] * 10,
        out_specs=[any_spec, vmem_spec, vmem_spec, any_spec],
        scratch_shapes=[
            pltpu.VMEM((tile_rows, width), bf16),
            pltpu.VMEM((halves, depth, tile_cols, wide), bf16),
            pltpu.VMEM((mask.shape[0] // LANES, LANES), jnp.int32),
            pltpu.VMEM((heads, wide), bf16),
            pltpu.VMEM(w_project.shape, bf16),
            pltpu.VMEM(w_out.shape, bf16),
            pltpu.VMEM(w_factors.shape, bf16),
            pltpu.VMEM((halves, rows_each, width), bf16),
            pltpu.VMEM((row_size // 2, halves, 2, tile_cols, group), bf16),
            pltpu.VMEM((col_size, 2, tile_cols, group), bf16),
            pltpu.VMEM((col_size, tile_rows, group), bf16),
            pltpu.VMEM((halves, depth, group), f32),
            pltpu.VMEM((col_size, halves, rows_each, group), f32),
            pltpu.VMEM((heads * stride, LANES), f32),
            pltpu.VMEM((parts, col_size, halves * rows_each, width // parts), bf16),
            pltpu.VMEM((parts, col_size, halves * rows_each, width // parts), bf16),
            pltpu.VMEM((depth, LANES), f32),
            pltpu.VMEM((col_size, rows_each, LANES), f32),
            pltpu.VMEM((rows_each, LANES), f32),
            pltpu.VMEM((rows_each, LANES), f32),
            pltpu.VMEM((col_size, rows_each, LANES), f32),
            pltpu.VMEM((col_size, rows_each, LANES), f32),
            pltpu.VMEM((halves, rows_each, width), bf16),
            pltpu.VMEM((halves * wide, halves * wide), bf16),
            pltpu.VMEM((halves, 2 * LANES, width), bf16),
            pltpu.VMEM(w_pairout.shape, bf16),
            pltpu.VMEM((2 * wide, 2 * wide), bf16),
            pltpu.VMEM(w_up.shape, bf16),
            pltpu.VMEM(w_down.shape, bf16),
            pltpu.VMEM((part_rows, tile_cols, wide), bf16),
            pltpu.SemaphoreType.DMA((12 + halves,)),
            pltpu.SemaphoreType.DMA((steps,)),
            pltpu.SemaphoreType.DMA((6, col_size - 1)),
            pltpu.SemaphoreType.DMA((6, col_size - 1)),
            pltpu.SemaphoreType.DMA((2, row_size * halves)),
            pltpu.SemaphoreType.DMA((2, col_size)),
            pltpu.SemaphoreType.DMA((row_size // 2 - 1,)),
            pltpu.SemaphoreType.DMA((row_size // 2 - 1,)),
            pltpu.SemaphoreType.DMA((row_size * halves,)),
            pltpu.SemaphoreType.DMA((2, col_size)),
            pltpu.SemaphoreType.DMA((col_size,)),
            pltpu.SemaphoreType.DMA((2 * col_size,)),
            pltpu.SemaphoreType.DMA((col_size,)),
            pltpu.SemaphoreType.DMA((parts, col_size - 1)),
            pltpu.SemaphoreType.DMA((parts, col_size - 1)),
        ],
        compiler_params=pltpu.CompilerParams(collective_id=3, has_side_effects=True),
        name="attend",
    )(
        single,
        pair,
        mask.reshape(mask.shape[0] // LANES, LANES),
        w_bias.T,
        w_project,
        w_out,
        w_factors,
        w_pairout,
        w_up,
        w_down,
    )
    return single_out.reshape(tile_rows, width), left, right, part


def fits(row_size, col_size, single, pair, mask, w_bias, w_project, w_factors):
    tile_rows, tile_cols, wide = pair.shape
    heads = w_bias.shape[1]
    return (
        tile_rows == 2 * tile_cols
        and 2 * tile_cols == LANES
        and wide == LANES
        and w_factors.shape[1] == LANES
        and w_project.shape[2] == LANES
        and 4 * heads == LANES
        and heads % (2 * col_size) == 0
        and tile_cols % (8 * col_size) == 0
        and col_size == 2 * row_size
        and row_size % 2 == 0
        and tile_cols % (2 * update_block) == 0
        and mask.shape[0] % LANES == 0
    )


def per_device_keys(
    row_size, col_size,
    single, pair, residue_mask, w_bias, w_project, w_out, w_factors, w_pairout, w_up, w_down
):
    shape = pair.shape
    single_out, left, right, part = attend(
        single, pair.reshape(2, shape[0] // 2, *shape[1:]), residue_mask,
        w_bias, w_project, w_out, w_factors, w_pairout, w_up, w_down, row_size, col_size,
    )
    return tuple(finish(single_out, pair, part, left, right, w_pairout, w_up, w_down))


def dispatch(row_size, col_size, *arrays):
    single, pair, residue_mask, w_bias, w_project, w_out, w_factors = arrays[:7]
    if fits(row_size, col_size, single, pair, residue_mask, w_bias, w_project, w_factors):
        return per_device_keys(row_size, col_size, *arrays)
    return per_device(row_size, col_size, *arrays)


def solution(mesh):
    return jax.shard_map(
        functools.partial(dispatch, mesh.shape["rows"], mesh.shape["cols"]),
        mesh=mesh,
        in_specs=(
            P("rows", None),
            P("rows", "cols", None),
            P(),
            P(),
            P(None, None, "cols"),
            P(),
            P(),
            P(),
            P(),
            P(),
        ),
        out_specs=(P("rows", None), P("rows", "cols", None)),
        check_vma=False,
    )
```

```python
import functools
import math

import jax
import jax.numpy as jnp
from jax import lax
from jax.experimental import pallas as pl
from jax.experimental.pallas import tpu as pltpu
from jax.sharding import PartitionSpec as P

epsilon = 1e-05


def enter(axes):
    barrier = pltpu.get_barrier_semaphore()
    total = 0
    for axis, size in axes:
        me = lax.axis_index(axis)
        for step in range(1, size):
            pl.semaphore_signal(
                barrier,
                inc=1,
                device_id={axis: lax.rem(me + step, size)},
                device_id_type=pl.DeviceIdType.MESH,
            )
        total += size - 1
    pl.semaphore_wait(barrier, total)


def spread(axis, size, source, landing, send_sems, recv_sems):
    me = lax.axis_index(axis)
    copies = []
    for step in range(1, size):
        copy = pltpu.make_async_remote_copy(
            src_ref=source,
            dst_ref=landing.at[me],
            send_sem=send_sems.at[step - 1],
            recv_sem=recv_sems.at[step - 1],
            device_id={axis: lax.rem(me + step, size)},
            device_id_type=pl.DeviceIdType.MESH,
        )
        copy.start()
        copies.append(copy)
    return copies


def gather_kernel(axis, size, source, gathered, send_sems, recv_sems, own_sem):
    enter([(axis, size)])
    copies = spread(axis, size, source, gathered, send_sems, recv_sems)
    own = pltpu.make_async_copy(source, gathered.at[lax.axis_index(axis)], own_sem)
    own.start()
    own.wait()
    for copy in copies:
        copy.wait()


def gather(values, axis, size, collective_id):
    return pl.pallas_call(
        functools.partial(gather_kernel, axis, size),
        out_shape=jax.ShapeDtypeStruct((size, *values.shape), values.dtype),
        in_specs=[pl.BlockSpec(memory_space=pltpu.VMEM)],
        out_specs=pl.BlockSpec(memory_space=pltpu.VMEM),
        scratch_shapes=[
            pltpu.SemaphoreType.DMA((size - 1,)),
            pltpu.SemaphoreType.DMA((size - 1,)),
            pltpu.SemaphoreType.DMA,
        ],
        compiler_params=pltpu.CompilerParams(collective_id=collective_id, has_side_effects=True),
        name="gather_" + axis,
    )(values)


def single_kernel(
    row_size, col_size, tile_cols,
    mixed, single, w_out, w_factors, single_out, left_out, right_out,
    gathered, factor_right, send_sems, recv_sems, row_send, row_recv, own_sem,
):
    enter([("cols", col_size), ("rows", row_size)])
    tile_rows, width = mixed.shape
    me_col = lax.axis_index("cols")
    me_row = lax.axis_index("rows")
    copies = spread("cols", col_size, mixed, gathered, send_sems, recv_sems)
    own = pltpu.make_async_copy(mixed, gathered.at[me_col], own_sem)
    own.start()
    own.wait()
    for copy in copies:
        copy.wait()
    whole = jnp.concatenate([gathered[part] for part in range(col_size)], axis=1)
    total = jnp.dot(whole, w_out[...], preferred_element_type=jnp.float32)
    updated = (single[...].astype(jnp.float32) + total).astype(jnp.bfloat16)
    single_out[...] = updated
    normed = layer_norm(updated).astype(jnp.bfloat16)
    factors = jnp.dot(normed, w_factors[...], preferred_element_type=jnp.float32)
    factors = factors.astype(jnp.bfloat16).astype(jnp.float32)
    half = factors.shape[1] // 2
    swapped = jnp.concatenate([factors[:, half:], factors[:, :half]], axis=1)
    lower = lax.broadcasted_iota(jnp.int32, factors.shape, 1) < half
    left_out[...] = jnp.where(lower, factors, swapped)
    factor_right[...] = jnp.where(lower, swapped, factors).astype(jnp.bfloat16)
    first = me_col * tile_cols
    owner = first // tile_rows
    offset = pl.multiple_of(first - owner * tile_rows, tile_cols)
    piece = factor_right.at[pl.ds(offset, tile_cols)]

    @pl.when(me_row == owner)
    def _():
        local = pltpu.make_async_copy(piece, right_out, own_sem)
        local.start()
        sends = []
        for step in range(1, row_size):
            send = pltpu.make_async_remote_copy(
                src_ref=piece,
                dst_ref=right_out,
                send_sem=row_send.at[step - 1],
                recv_sem=row_recv,
                device_id={"rows": lax.rem(me_row + step, row_size)},
                device_id_type=pl.DeviceIdType.MESH,
            )
            send.start()
            sends.append(send)
        local.wait()
        for send in sends:
            send.wait_send()

    @pl.when(me_row != owner)
    def _():
        pltpu.make_async_remote_copy(
            src_ref=piece,
            dst_ref=right_out,
            send_sem=row_send.at[0],
            recv_sem=row_recv,
            device_id={"rows": lax.rem(me_row + 1, row_size)},
            device_id_type=pl.DeviceIdType.MESH,
        ).wait_recv()


def update_single(mixed, single, w_out, w_factors, row_size, col_size, tile_cols):
    tile_rows, width = single.shape
    wide = w_factors.shape[1]
    return pl.pallas_call(
        functools.partial(single_kernel, row_size, col_size, tile_cols),
        out_shape=(
            jax.ShapeDtypeStruct((tile_rows, width), jnp.bfloat16),
            jax.ShapeDtypeStruct((tile_rows, wide), jnp.float32),
            jax.ShapeDtypeStruct((tile_cols, wide), jnp.bfloat16),
        ),
        in_specs=[pl.BlockSpec(memory_space=pltpu.VMEM)] * 4,
        out_specs=[pl.BlockSpec(memory_space=pltpu.VMEM)] * 3,
        scratch_shapes=[
            pltpu.VMEM((col_size, *mixed.shape), jnp.bfloat16),
            pltpu.VMEM((tile_rows, wide), jnp.bfloat16),
            pltpu.SemaphoreType.DMA((col_size - 1,)),
            pltpu.SemaphoreType.DMA((col_size - 1,)),
            pltpu.SemaphoreType.DMA((row_size - 1,)),
            pltpu.SemaphoreType.DMA,
            pltpu.SemaphoreType.DMA,
        ],
        compiler_params=pltpu.CompilerParams(collective_id=2, has_side_effects=True),
        name="update_single",
    )(mixed, single, w_out, w_factors)


def matmul_norm(values):
    wide = values.shape[1]
    share = jnp.full((2 * wide, wide), 1.0 / wide, jnp.bfloat16)
    mean = jnp.dot(values, share[:wide], preferred_element_type=jnp.float32)
    centred = values.astype(jnp.float32) - mean
    square = centred * centred
    high = square.astype(jnp.bfloat16)
    low = (square - high.astype(jnp.float32)).astype(jnp.bfloat16)
    spread_out = jnp.dot(
        jnp.concatenate([high, low], 1), share, preferred_element_type=jnp.float32
    )
    return (centred * lax.rsqrt(spread_out + epsilon)).astype(jnp.bfloat16)


def norm_kernel(values, normed):
    normed[...] = matmul_norm(values[...])


def norm_rows(values, block):
    spec = pl.BlockSpec((block, values.shape[1]), lambda step: (step, 0))
    return pl.pallas_call(
        norm_kernel,
        out_shape=jax.ShapeDtypeStruct(values.shape, jnp.bfloat16),
        grid=(values.shape[0] // block,),
        in_specs=[spec],
        out_specs=spec,
        name="norm_pair",
    )(values)


def pair_kernel(pair, left, right, w_pairout, w_up, w_down, updated):
    block_rows, tile_cols, wide = pair.shape
    left_wide = left[...][:, None, :]
    right_wide = right[...].astype(jnp.float32)[None, :, :]
    lower = lax.broadcasted_iota(jnp.int32, pair.shape, 2) < wide // 2
    paired = jnp.where(lower, left_wide * right_wide, left_wide - right_wide)
    paired = paired.astype(jnp.bfloat16).reshape(block_rows * tile_cols, wide)
    flat = pair[...].reshape(block_rows * tile_cols, wide).astype(jnp.float32)
    mid = flat + jnp.dot(paired, w_pairout[...], preferred_element_type=jnp.float32)
    mid = mid.astype(jnp.bfloat16)
    normed = matmul_norm(mid)
    hidden = jnp.dot(normed, w_up[...], preferred_element_type=jnp.float32)
    hidden = jnp.maximum(hidden, 0.0).astype(jnp.bfloat16)
    out = mid.astype(jnp.float32) + jnp.dot(
        hidden, w_down[...], preferred_element_type=jnp.float32
    )
    updated[...] = out.astype(jnp.bfloat16).reshape(pair.shape)


def update_pair(pair, left, right, w_pairout, w_up, w_down):
    tile_rows, tile_cols, wide = pair.shape
    block = math.gcd(tile_rows, max(8, 1024 // tile_cols))
    tile = pl.BlockSpec((block, tile_cols, wide), lambda step: (step, 0, 0))

    def whole(array):
        return pl.BlockSpec(array.shape, lambda step: (0, 0))

    return pl.pallas_call(
        pair_kernel,
        out_shape=jax.ShapeDtypeStruct(pair.shape, jnp.bfloat16),
        grid=(tile_rows // block,),
        in_specs=[
            tile,
            pl.BlockSpec((block, wide), lambda step: (step, 0)),
            whole(right),
            whole(w_pairout),
            whole(w_up),
            whole(w_down),
        ],
        out_specs=tile,
        name="update_pair",
    )(pair, left, right, w_pairout, w_up, w_down)


def layer_norm(values):
    values = values.astype(jnp.float32)
    centred = values - jnp.mean(values, -1, keepdims=True)
    return centred * lax.rsqrt(jnp.mean(centred * centred, -1, keepdims=True) + epsilon)


def per_device(
    row_size, col_size,
    single, pair, residue_mask, w_bias, w_project, w_out, w_factors, w_pairout, w_up, w_down
):
    tile_rows = pair.shape[0]
    tile_cols = pair.shape[1]
    normed_pair = norm_rows(
        pair.reshape(tile_rows * tile_cols, pair.shape[2]), math.gcd(tile_rows * tile_cols, 1024)
    ).reshape(pair.shape)
    bias_local = jnp.einsum(
        "rcp,ph->hrc", normed_pair, w_bias, preferred_element_type=jnp.float32
    ).astype(jnp.bfloat16)
    normed_single = layer_norm(single).astype(jnp.bfloat16)
    projected = jnp.einsum(
        "rs,fsc->frc", normed_single, w_project, preferred_element_type=jnp.float32
    )
    query_rows = projected[0].astype(jnp.bfloat16)
    key_local = projected[1].astype(jnp.bfloat16)
    value_local = projected[2].astype(jnp.bfloat16)
    gate_values = jax.nn.sigmoid(projected[3])
    bias_heads = lax.all_to_all(bias_local, "cols", split_axis=0, concat_axis=2, tiled=True)
    both = gather(jnp.concatenate([key_local, value_local], 1), "rows", row_size, 1)
    both = both.reshape(row_size * tile_rows, both.shape[2])
    key_rows, value_rows = both[:, : key_local.shape[1]], both[:, key_local.shape[1] :]
    heads_here = bias_heads.shape[0]
    head_width = query_rows.shape[1] // heads_here
    residues = key_rows.shape[0]
    query_split = query_rows.reshape(tile_rows, heads_here, head_width)
    key_split = key_rows.reshape(residues, heads_here, head_width)
    value_split = value_rows.reshape(residues, heads_here, head_width)
    score_scale = 1.0 / math.sqrt(head_width)
    scores = jnp.einsum(
        "rhd,lhd->hrl", query_split, key_split, preferred_element_type=jnp.float32
    ) * score_scale + bias_heads.astype(jnp.float32)
    key_valid = (residue_mask > 0)[None, None, :]
    scores = jnp.where(key_valid, scores, -jnp.inf)
    weights = jax.nn.softmax(scores, axis=-1).astype(jnp.bfloat16)
    attended = jnp.einsum("hrl,lhd->rhd", weights, value_split, preferred_element_type=jnp.float32)
    attended = attended.reshape(tile_rows, heads_here * head_width)
    mixed = (attended * gate_values).astype(jnp.bfloat16)
    single_out, left, right = update_single(
        mixed, single, w_out, w_factors, row_size, col_size, tile_cols
    )
    return (single_out, update_pair(pair, left, right, w_pairout, w_up, w_down))


LANES = 128
excluded = -1e30
update_block = 16


def lane_iota(shape):
    return lax.broadcasted_iota(jnp.int32, shape, len(shape) - 1)


def centre_matrix(wide, copies):
    size = wide * copies
    row = lax.broadcasted_iota(jnp.int32, (size, size), 0)
    col = lax.broadcasted_iota(jnp.int32, (size, size), 1)
    share = jnp.where(row // wide == col // wide, 1.0 / wide, 0.0)
    return (jnp.where(row == col, 1.0, 0.0) - share).astype(jnp.bfloat16)


def norm_centred(values, centre, copies):
    centred = jnp.dot(values, centre, preferred_element_type=jnp.float32)
    wide = values.shape[1] // copies
    parts = []
    for index in range(copies):
        part = centred[:, index * wide : (index + 1) * wide]
        square = jnp.sum(part * part, axis=1, keepdims=True) * (1.0 / wide)
        parts.append((part * lax.rsqrt(square + epsilon)).astype(jnp.bfloat16))
    return parts


def twice(weights):
    zeros = jnp.zeros_like(weights)
    upper = jnp.concatenate([weights, zeros], axis=1)
    return jnp.concatenate([upper, jnp.concatenate([zeros, weights], axis=1)], axis=0)


def update_rows(pair_of, left_of, right, rows, centre, w_pairout, w_up, w_down):
    tile_cols, wide = right.shape
    lower = lane_iota((rows, tile_cols, wide)) < wide // 2

    def paired(index):
        left_wide = left_of(index)[:, None, :]
        right_wide = right[None, :, :]
        chosen = jnp.where(lower, left_wide * right_wide, left_wide - right_wide)
        return chosen.astype(jnp.bfloat16).reshape(rows * tile_cols, wide)

    flat = [pair_of(index).reshape(rows * tile_cols, wide) for index in range(2)]
    mid = jnp.concatenate(flat, axis=1).astype(jnp.float32) + jnp.dot(
        jnp.concatenate([paired(0), paired(1)], axis=1),
        w_pairout,
        preferred_element_type=jnp.float32,
    )
    mid = mid.astype(jnp.bfloat16)
    normed = jnp.concatenate(norm_centred(mid, centre, 2), axis=0)
    mid = jnp.concatenate([mid[:, :wide], mid[:, wide:]], axis=0)
    hidden = jnp.dot(normed, w_up, preferred_element_type=jnp.float32)
    hidden = jnp.maximum(hidden, 0.0).astype(jnp.bfloat16)
    out = mid.astype(jnp.float32) + jnp.dot(hidden, w_down, preferred_element_type=jnp.float32)
    return out.astype(jnp.bfloat16).reshape(2 * rows, tile_cols, wide)


def attend_kernel(
    row_size, col_size, heads, tile_cols, stride,
    single, pair, mask, w_bias, w_project, w_out, w_factors, w_pairout, w_up, w_down,
    single_out, pair_out,
    single_v, pair_v, mask_v, bias_w, project_v, out_v, factors_v, own_single,
    kv_send, kv_recv, q_recv, gate_send, gate_recv, bias_v, o_send, o_recv,
    st_send, st_recv, left_send, right_send, left_recv, right_recv, left_out, right_out, so_send, centre_v, spread_v,
    pairout_v, twice_v, up_v, down_v,
    load_sems, pair_sems, col_send, col_recv, fan_send, fan_recv,
    plane_sent, plane_came, kv_sent, kv_came, kv_relayed, q_sent, q_came, o_sent, o_came,
):
    me_row = lax.axis_index("rows")
    me_col = lax.axis_index("cols")
    total = row_size * col_size
    halves, depth, _, wide = pair.shape
    tile_rows, width = single.shape
    group = w_project.shape[2]
    rows_each = depth // col_size
    heads_here = heads // col_size
    head_width = group // heads_here
    chunk = depth // pair_sems.shape[0]
    loads = [
        pltpu.make_async_copy(source, target, load_sems.at[index])
        for index, (source, target) in enumerate(
            [(single, single_v)]
            + [(w_project.at[part], project_v.at[part]) for part in range(4)]
            + [(w_bias, bias_w), (mask, mask_v)]
            + [
                (single.at[pl.ds(half * depth + me_col * rows_each, rows_each)], own_single.at[half])
                for half in range(halves)
            ]
            + [(w_out, out_v), (w_factors, factors_v)]
            + [(w_pairout, pairout_v), (w_up, up_v), (w_down, down_v)]
        )
    ]
    for copy in loads[:7]:
        copy.start()
    barrier = pltpu.get_barrier_semaphore()
    me = me_row * col_size + me_col
    for step in range(1, total):
        to = lax.rem(me + step, total)
        pl.semaphore_signal(
            barrier,
            inc=1,
            device_id={"rows": to // col_size, "cols": lax.rem(to, col_size)},
            device_id_type=pl.DeviceIdType.MESH,
        )

    def pair_load(step):
        part = pl.ds(step * chunk, chunk)
        return pltpu.make_async_copy(pair.at[:, part], pair_v.at[:, part], pair_sems.at[step])

    for step in range(depth // chunk):
        pair_load(step).start()
    for copy in loads[7:]:
        copy.start()

    centre_v[...] = centre_matrix(wide, halves)

    def to_cols(kind, source_of, target):
        copies = []
        for step in range(1, col_size):
            to = lax.rem(me_col + step, col_size)
            copy = pltpu.make_async_remote_copy(
                src_ref=source_of(to),
                dst_ref=target,
                send_sem=col_send.at[kind, step - 1],
                recv_sem=col_recv.at[kind, step - 1],
                device_id={"cols": to},
                device_id_type=pl.DeviceIdType.MESH,
            )
            copy.start()
            copies.append(copy)
        return copies

    owner = me_col // halves
    mine = owner == me_row
    half_mine = lax.rem(me_col, halves)

    def fan_copies(kind, source_of, target):
        copies = []
        for step in range(row_size):
            for half in range(halves):
                to = halves * me_row + half
                copy = pltpu.make_async_remote_copy(
                    src_ref=source_of(half),
                    dst_ref=target.at[me_col],
                    send_sem=fan_send.at[kind, step * halves + half],
                    recv_sem=fan_recv.at[kind, me_col],
                    device_id={"rows": lax.rem(me_row + step, row_size), "cols": to},
                    device_id_type=pl.DeviceIdType.MESH,
                )
                copies.append((copy, step, to))
        return copies

    def on_some(copies, act):
        for copy, condition in copies:
            if condition is None:
                act(copy)
            else:
                pl.when(condition)(functools.partial(act, copy))

    kind_mine = lax.rem(me_row, 2)
    me_plane = me_row // 2
    row_mate = me_row + 1 - 2 * kind_mine
    col_mate = me_col + 1 - 2 * lax.rem(me_col, 2)

    def relay_keys(part, kind, slot):
        return pltpu.make_async_remote_copy(
            src_ref=kv_recv.at[part, kind],
            dst_ref=kv_recv.at[part, kind],
            send_sem=kv_relayed.at[slot],
            recv_sem=kv_came.at[kind, part],
            device_id={"rows": row_mate},
            device_id_type=pl.DeviceIdType.MESH,
        )

    def send_query(part, to, slot):
        return pltpu.make_async_remote_copy(
            src_ref=q_recv.at[part],
            dst_ref=q_recv.at[part],
            send_sem=q_sent.at[slot],
            recv_sem=q_came.at[part],
            device_id={"cols": to},
            device_id_type=pl.DeviceIdType.MESH,
        )

    def on_fan(copies, act):
        for copy, step, to in copies:
            if step:
                act(copy)
            else:
                pl.when(to != me_col)(functools.partial(act, copy))

    def fan_wait(kind, source_of, target):
        for part in range(col_size):
            copy = pltpu.make_async_remote_copy(
                src_ref=source_of(0),
                dst_ref=target.at[part],
                send_sem=fan_send.at[kind, 0],
                recv_sem=fan_recv.at[kind, part],
                device_id={"rows": lax.rem(me_row + 1, row_size)},
                device_id_type=pl.DeviceIdType.MESH,
            )
            pl.when(jnp.logical_not(jnp.logical_and(mine, part == me_col)))(copy.wait_recv)

    loads[0].wait()
    normed = layer_norm(single_v[...]).astype(jnp.bfloat16)
    def project(*kinds):
        weights = [project_v[kind] for kind in kinds]
        return jnp.dot(
            normed, jnp.concatenate(weights, axis=1), preferred_element_type=jnp.float32
        )

    loads[1].wait()
    q_recv[me_col] = project(0).astype(jnp.bfloat16)
    pl.semaphore_wait(barrier, total - 1)
    peers = [lax.rem(me_col + 2 * step, col_size) for step in range(1, col_size // 2)]
    q_copies = [send_query(me_col, to, slot) for slot, to in enumerate(peers)]
    q_copies.append(send_query(me_col, col_mate, len(peers)))
    for copy in q_copies:
        copy.start()
    loads[2].wait()
    loads[3].wait()
    key_value = project(1, 2).astype(jnp.bfloat16)
    for half in range(halves):
        for kind in range(2):
            kv_send[me_plane, half, kind] = key_value[
                half * tile_cols : (half + 1) * tile_cols, kind * group : (kind + 1) * group
            ]
    planes = row_size // 2
    plane_copies = []
    for step in range(1, planes):
        plane = lax.rem(me_plane + step, planes)
        copy = pltpu.make_async_remote_copy(
            src_ref=kv_send.at[me_plane],
            dst_ref=kv_send.at[me_plane],
            send_sem=plane_sent.at[step - 1],
            recv_sem=plane_came.at[step - 1],
            device_id={"rows": 2 * plane + kind_mine},
            device_id_type=pl.DeviceIdType.MESH,
        )
        copy.start()
        plane_copies.append(copy)
    kv_copies = []

    def send_keys(step):
        plane = lax.rem(me_plane + planes - step, planes)
        for half in range(halves):
            for kind in range(2):
                to = halves * (2 * plane + kind_mine) + half
                row = 2 * me_plane + kind
                copy = pltpu.make_async_remote_copy(
                    src_ref=kv_send.at[plane, half, kind],
                    dst_ref=kv_recv.at[me_col, kind],
                    send_sem=kv_sent.at[(step * 2 + kind) * halves + half],
                    recv_sem=kv_came.at[kind, me_col],
                    device_id={"rows": row, "cols": to},
                    device_id_type=pl.DeviceIdType.MESH,
                )
                here = jnp.logical_and(row == me_row, to == me_col)
                kv_copies.append((copy, jnp.logical_not(here)))
        on_some(kv_copies[-2 * halves :], lambda copy: copy.start())

    send_keys(0)
    loads[4].wait()
    gate_send[...] = jax.nn.sigmoid(project(3)).reshape(halves, depth, group)

    def own_rows(to):
        return pl.ds(pl.multiple_of(to * rows_each, rows_each), rows_each)

    loads[5].wait()
    loads[6].wait()

    parts, _, _, part_width = o_send.shape
    each = part_width // group
    col_side = lax.rem(me_col, each)

    def relay_query(part):
        return send_query(part, col_mate, col_size // 2 + part // each)

    def bias_step(step, _):
        pair_load(step).wait()
        parts = [
            pair_v[half, pl.ds(step * chunk, chunk)].reshape(chunk * tile_cols, wide)
            for half in range(halves)
        ]
        parts = norm_centred(jnp.concatenate(parts, axis=1), centre_v[...], halves)
        parts = [part.reshape(chunk, 1, tile_cols, wide) for part in parts]
        normed_pair = jnp.concatenate(parts, axis=1).reshape(chunk * halves * tile_cols, wide)
        bias = lax.dot_general(
            bias_w[...], normed_pair, (((1,), (1,)), ((), ())), preferred_element_type=jnp.float32
        )
        bias = bias.astype(jnp.bfloat16).astype(jnp.float32)
        for part in range(chunk):
            bias_v[pl.ds(step * chunk + part, heads, stride=stride), :] = bias[
                :, part * LANES : (part + 1) * LANES
            ]
        return 0

    lax.fori_loop(0, depth // chunk, bias_step, 0)
    for step in range(1, planes):
        plane_copies[step - 1].wait_recv()
        send_keys(step)
    own_key = lax.rem(owner, 2) == kind_mine

    @pl.when(own_key)
    def _():
        kv_recv[me_col, kind_mine] = kv_send[owner // 2, half_mine, kind_mine]

    relays = [relay_query(peer) for peer in peers]
    for copy in relays:
        copy.wait_recv()
        copy.start()

    def turn_part(turn, index):
        return lax.rem(me_col // each + turn, parts) * each + index

    def relay_turn(turn):
        for index in range(each):
            part = turn_part(turn, index)
            copy = relay_keys(part, kind_mine, part)
            own = jnp.logical_and(own_key, part == me_col)
            pl.when(jnp.logical_not(own))(copy.wait_recv)
            copy.start()

    relay_turn(0)
    gate_copies = to_cols(1, lambda to: gate_send.at[:, own_rows(to)], gate_recv.at[me_col])
    gate_recv[me_col] = gate_send[:, own_rows(me_col)]
    relay_turn(1)
    relays += [relay_keys(part, kind_mine, part) for part in range(col_size)]

    lane_row = lane_iota((2 * halves * heads, width))
    place = lax.broadcasted_iota(jnp.int32, (2 * halves * heads, width), 0)
    for half in range(halves):
        picked = jnp.where(place == half * heads + lane_row // head_width, 1.0, 0.0)
        spread_v[half, :LANES] = picked.astype(jnp.bfloat16)
        spread_v[half, LANES:] = picked.astype(jnp.bfloat16)

    length = jnp.sum(jnp.sum(mask_v[...], axis=1, keepdims=True), axis=0, keepdims=True)
    lane = lane_iota((depth, LANES))
    low = lane < tile_cols
    valid = me_col * tile_cols + lax.rem(lane, tile_cols) < length
    head_of = lane_iota((tile_cols, group)) // head_width
    head_masks = [
        jnp.where(head_of == head, 1.0, 0.0).astype(jnp.bfloat16) for head in range(heads_here)
    ]
    zeros = jnp.zeros((tile_cols, group), jnp.bfloat16)
    scale = 1.0 / math.sqrt(head_width)
    st_send[...] = jnp.zeros_like(st_send)
    block_place = lax.broadcasted_iota(jnp.int32, (heads_here * LANES, LANES), 0) // tile_cols
    block_target = (
        halves * heads + lax.rem(block_place, halves) * heads + block_place // halves
    )
    block_lane = lane_iota((heads_here * LANES, LANES))

    def attend_part(part):
        query = q_recv[part]
        query = jnp.concatenate([query[:depth], query[depth:]], axis=1)
        key, value = kv_recv[part, 0], kv_recv[part, 1]
        weights, value_rows = [], []
        stats = st_send[...]
        for first in range(0, heads_here, 2):
            key_rows = []
            for head in (first, first + 1):
                masked = key * head_masks[head]
                key_rows.append(jnp.concatenate([masked, zeros], axis=1))
                key_rows.append(jnp.concatenate([zeros, masked], axis=1))
            raw = lax.dot_general(
                query,
                jnp.concatenate(key_rows, axis=0),
                (((1,), (1,)), ((), ())),
                preferred_element_type=jnp.float32,
            )
            for head in (first, first + 1):
                index = part * heads_here + head
                bias = bias_v[pl.ds(pl.multiple_of(index * stride, 8), depth), :]
                scores = raw[:, (head - first) * LANES : (head - first + 1) * LANES] * scale + bias
                scores = jnp.where(valid, scores, excluded)
                top0 = jnp.max(jnp.where(low, scores, excluded), axis=1, keepdims=True)
                top1 = jnp.max(jnp.where(low, excluded, scores), axis=1, keepdims=True)
                weights.append(
                    jnp.exp(scores - jnp.where(low, top0, top1)).astype(jnp.bfloat16)
                )
                stats = jnp.where(lane == index, top0, stats)
                stats = jnp.where(lane == heads + index, top1, stats)
        for head in range(heads_here):
            masked = value * head_masks[head]
            value_rows.append(jnp.concatenate([masked, zeros], axis=1))
            value_rows.append(jnp.concatenate([zeros, masked], axis=1))
        weights = jnp.concatenate(weights, axis=1)
        mixed = jnp.dot(
            weights, jnp.concatenate(value_rows, axis=0), preferred_element_type=jnp.float32
        )
        ones = jnp.where(block_lane == block_target + part * heads_here, 1.0, 0.0)
        sums = jnp.dot(weights, ones.astype(jnp.bfloat16), preferred_element_type=jnp.float32)
        st_send[...] = stats + sums
        pieces = [
            mixed[:, half * group : (half + 1) * group].reshape(col_size, rows_each, group)
            for half in range(halves)
        ]
        return jnp.concatenate(pieces, axis=1).astype(jnp.bfloat16)

    def o_copy(step, shift):
        to = lax.rem(me_col + shift, col_size)
        return pltpu.make_async_remote_copy(
            src_ref=o_send.at[step, to],
            dst_ref=o_recv.at[step, me_col],
            send_sem=o_sent.at[step, shift - 1],
            recv_sem=o_came.at[step, shift - 1],
            device_id={"cols": to},
            device_id_type=pl.DeviceIdType.MESH,
        )

    def attend_step(turn, _):
        step = lax.rem(me_col // each + turn, parts)
        far = step * each + 1 - col_side
        relay_query(far).wait_recv()
        for index in range(each):
            part = step * each + index
            relay_keys(part, 1 - kind_mine, part).wait_recv()
        for index in range(each):
            o_send[step, :, :, index * group : (index + 1) * group] = attend_part(
                step * each + index
            )
        for shift in range(1, col_size):
            o_copy(step, shift).start()
        pl.when(turn + 2 < parts)(functools.partial(relay_turn, turn + 2))
        return 0

    lax.fori_loop(0, parts, attend_step, 0)
    st_copies = to_cols(2, lambda to: st_send.at[own_rows(to)], st_recv.at[me_col])
    st_recv[me_col] = st_send[own_rows(me_col)]
    for step in range(parts):
        o_recv[step, me_col] = o_send[step, me_col]
    o_copies = [o_copy(step, shift) for step in range(parts) for shift in range(1, col_size)]
    for copy in gate_copies + st_copies:
        copy.wait_recv()
    stats = st_recv[...]
    lane = lane_iota(stats.shape)
    top = jnp.max(stats, axis=0, keepdims=True)
    factor = jnp.exp(stats - top)
    sums = jnp.sum(factor * pltpu.roll(stats, halves * heads, axis=2), axis=0, keepdims=True)
    factor = jnp.where(lane < halves * heads, factor / sums, 0.0)
    factor = factor.reshape(col_size * rows_each, LANES)
    high = factor.astype(jnp.bfloat16)
    rest = (factor - high.astype(jnp.float32)).astype(jnp.bfloat16)
    factor = jnp.concatenate([high, rest], axis=1)
    scales = [
        jnp.dot(factor, spread_v[half], preferred_element_type=jnp.float32) for half in range(halves)
    ]
    gate = jnp.concatenate(
        [gate_recv[part].reshape(halves * rows_each, group) for part in range(col_size)], axis=1
    )
    for copy in o_copies:
        copy.wait_recv()
    attended = jnp.zeros((halves * rows_each, width), jnp.float32)
    for part in range(col_size):
        rows = slice(part * rows_each, (part + 1) * rows_each)
        part_scale = jnp.concatenate([scales[half][rows] for half in range(halves)], axis=0)
        whole = jnp.concatenate([o_recv[step, part] for step in range(parts)], axis=1)
        attended = attended + part_scale * whole.astype(jnp.float32)
    mixed = (attended * gate).astype(jnp.bfloat16)
    for copy in loads[7:]:
        copy.wait()
    added = jnp.dot(mixed, out_v[...], preferred_element_type=jnp.float32)
    own = own_single[...].astype(jnp.float32).reshape(halves * rows_each, width)
    updated = (own + added).astype(jnp.bfloat16)
    so_send[...] = updated.astype(jnp.float32).reshape(halves, rows_each, width).astype(jnp.bfloat16)
    factors = jnp.dot(
        layer_norm(updated).astype(jnp.bfloat16),
        factors_v[...],
        preferred_element_type=jnp.float32,
    )
    factors = factors.astype(jnp.bfloat16).astype(jnp.float32)
    first, second = factors[:rows_each], factors[rows_each:]
    shift = factors.shape[1] // 2
    low = lane_iota(first.shape) < shift
    left = jnp.where(low, first, pltpu.roll(second, shift, axis=1))
    right = jnp.where(low, pltpu.roll(first, shift, axis=1), second)
    left_send[...] = left.astype(jnp.bfloat16)
    right_send[...] = right.astype(jnp.bfloat16)
    right_copies = fan_copies(1, lambda half: right_send, right_recv)
    on_fan(right_copies, lambda copy: copy.start())
    left_copies = to_cols(4, lambda to: left_send, left_recv.at[me_col])
    left_recv[me_col] = left.astype(jnp.bfloat16)

    @pl.when(mine)
    def _():
        right_recv[me_col] = right_send[...]

    fan_wait(1, lambda half: right_send, right_recv)
    for copy in left_copies:
        copy.wait_recv()
    so_copies = to_cols(5, lambda to: so_send, single_out.at[:, me_col])
    single_out[:, me_col] = so_send[...]
    left = left_recv[...].astype(jnp.float32).reshape(depth, LANES)
    turned = pltpu.roll(left, shift, axis=1)
    low = lane_iota(left.shape) < shift
    left_out[:depth] = jnp.where(low, left, turned)
    left_out[depth:] = jnp.where(low, turned, left)
    right = right_recv[...].astype(jnp.float32).reshape(tile_cols, LANES)
    turned = pltpu.roll(right, shift, axis=1)
    right_out[...] = jnp.where(lane_iota(right.shape) // shift == half_mine, right, turned)

    twice_v[...] = twice(pairout_v[...])
    block = update_block
    def update_step(step, _):
        first = step * 2 * block
        half = first // depth
        pair_out[pl.ds(first, 2 * block)] = update_rows(
            lambda index: pair_v[half, pl.ds(first - half * depth + index * block, block)],
            lambda index: left_out[pl.ds(pl.multiple_of(first + index * block, 8), block)],
            right_out[...],
            block,
            centre_v[...],
            twice_v[...],
            up_v[...],
            down_v[...],
        )
        return 0

    lax.fori_loop(0, tile_rows // (2 * block), update_step, 0)

    for copies in (q_copies, relays, plane_copies, gate_copies, st_copies, o_copies, left_copies, so_copies):
        for copy in copies:
            copy.wait_send()
    on_some(kv_copies, lambda copy: copy.wait_send())
    on_fan(right_copies, lambda copy: copy.wait_send())
    for copy in so_copies:
        copy.wait_recv()


def finish_kernel(single, pair, single_out, pair_out, sems):
    copies = [pltpu.make_async_copy(single, single_out, sems.at[0])]
    steps = sems.shape[0] - 1
    rows = pair.shape[0] // steps
    for step in range(steps):
        part = pl.ds(step * rows, rows)
        copies.append(
            pltpu.make_async_copy(pair.at[part], pair_out.at[part], sems.at[1 + step])
        )
    for copy in copies:
        copy.start()
    for copy in copies:
        copy.wait()


def finish(single, pair):
    return pl.pallas_call(
        finish_kernel,
        out_shape=tuple(jax.ShapeDtypeStruct(array.shape, array.dtype) for array in (single, pair)),
        in_specs=[pl.BlockSpec(memory_space=pltpu.VMEM)] * 2,
        out_specs=[pl.BlockSpec(memory_space=pl.ANY)] * 2,
        scratch_shapes=[pltpu.SemaphoreType.DMA((9,))],
        compiler_params=pltpu.CompilerParams(vmem_limit_bytes=8 * 1024 * 1024),
        name="finish",
    )(single, pair)


def attend(
    single, pair, mask, w_bias, w_project, w_out, w_factors, w_pairout, w_up, w_down,
    row_size, col_size,
):
    halves, depth, tile_cols, wide = pair.shape
    tile_rows, width = single.shape
    heads = w_bias.shape[1]
    rows_each = depth // col_size
    group = w_project.shape[2]
    steps = depth // 16
    parts = col_size // 2
    stride = depth + 8
    any_spec = pl.BlockSpec(memory_space=pltpu.HBM)
    vmem_spec = pl.BlockSpec(memory_space=pltpu.VMEM)
    bf16, f32 = jnp.bfloat16, jnp.float32
    single_out, pair_out = pl.pallas_call(
        functools.partial(attend_kernel, row_size, col_size, heads, tile_cols, stride),
        out_shape=(
            pltpu.VMEM((halves, col_size, rows_each, width), bf16),
            pltpu.VMEM((tile_rows, tile_cols, wide), bf16),
        ),
        in_specs=[any_spec] * 10,
        out_specs=[vmem_spec] * 2,
        scratch_shapes=[
            pltpu.VMEM((tile_rows, width), bf16),
            pltpu.VMEM((halves, depth, tile_cols, wide), bf16),
            pltpu.VMEM((mask.shape[0] // LANES, LANES), jnp.int32),
            pltpu.VMEM((heads, wide), bf16),
            pltpu.VMEM(w_project.shape, bf16),
            pltpu.VMEM(w_out.shape, bf16),
            pltpu.VMEM(w_factors.shape, bf16),
            pltpu.VMEM((halves, rows_each, width), bf16),
            pltpu.VMEM((row_size // 2, halves, 2, tile_cols, group), bf16),
            pltpu.VMEM((col_size, 2, tile_cols, group), bf16),
            pltpu.VMEM((col_size, tile_rows, group), bf16),
            pltpu.VMEM((halves, depth, group), f32),
            pltpu.VMEM((col_size, halves, rows_each, group), f32),
            pltpu.VMEM((heads * stride, LANES), f32),
            pltpu.VMEM((parts, col_size, halves * rows_each, width // parts), bf16),
            pltpu.VMEM((parts, col_size, halves * rows_each, width // parts), bf16),
            pltpu.VMEM((depth, LANES), f32),
            pltpu.VMEM((col_size, rows_each, LANES), f32),
            pltpu.VMEM((rows_each, LANES), bf16),
            pltpu.VMEM((rows_each, LANES), bf16),
            pltpu.VMEM((col_size, rows_each, LANES), bf16),
            pltpu.VMEM((col_size, rows_each, LANES), bf16),
            pltpu.VMEM((tile_rows, wide), f32),
            pltpu.VMEM((tile_cols, wide), f32),
            pltpu.VMEM((halves, rows_each, width), bf16),
            pltpu.VMEM((halves * wide, halves * wide), bf16),
            pltpu.VMEM((halves, 2 * LANES, width), bf16),
            pltpu.VMEM(w_pairout.shape, bf16),
            pltpu.VMEM((2 * wide, 2 * wide), bf16),
            pltpu.VMEM(w_up.shape, bf16),
            pltpu.VMEM(w_down.shape, bf16),
            pltpu.SemaphoreType.DMA((12 + halves,)),
            pltpu.SemaphoreType.DMA((steps,)),
            pltpu.SemaphoreType.DMA((6, col_size - 1)),
            pltpu.SemaphoreType.DMA((6, col_size - 1)),
            pltpu.SemaphoreType.DMA((2, row_size * halves)),
            pltpu.SemaphoreType.DMA((2, col_size)),
            pltpu.SemaphoreType.DMA((row_size // 2 - 1,)),
            pltpu.SemaphoreType.DMA((row_size // 2 - 1,)),
            pltpu.SemaphoreType.DMA((row_size * halves,)),
            pltpu.SemaphoreType.DMA((2, col_size)),
            pltpu.SemaphoreType.DMA((col_size,)),
            pltpu.SemaphoreType.DMA((2 * col_size,)),
            pltpu.SemaphoreType.DMA((col_size,)),
            pltpu.SemaphoreType.DMA((parts, col_size - 1)),
            pltpu.SemaphoreType.DMA((parts, col_size - 1)),
        ],
        compiler_params=pltpu.CompilerParams(
            collective_id=3, has_side_effects=True, vmem_limit_bytes=40 * 1024 * 1024
        ),
        name="attend",
    )(
        *(
            pltpu.with_memory_space_constraint(array, pltpu.HBM)
            for array in (
                single,
                pair,
                mask.reshape(mask.shape[0] // LANES, LANES),
                w_bias.T,
                w_project,
                w_out,
                w_factors,
                w_pairout,
                w_up,
                w_down,
            )
        )
    )
    single_out, pair_out = finish(single_out, pair_out)
    return single_out.reshape(tile_rows, width), pair_out


def fits(row_size, col_size, single, pair, mask, w_bias, w_project, w_factors):
    tile_rows, tile_cols, wide = pair.shape
    heads = w_bias.shape[1]
    return (
        tile_rows == 2 * tile_cols
        and 2 * tile_cols == LANES
        and wide == LANES
        and w_factors.shape[1] == LANES
        and w_project.shape[2] == LANES
        and 4 * heads == LANES
        and heads % (2 * col_size) == 0
        and tile_cols % (8 * col_size) == 0
        and col_size == 2 * row_size
        and row_size % 2 == 0
        and tile_cols % (2 * update_block) == 0
        and mask.shape[0] % LANES == 0
    )


def per_device_keys(
    row_size, col_size,
    single, pair, residue_mask, w_bias, w_project, w_out, w_factors, w_pairout, w_up, w_down
):
    shape = pair.shape
    return attend(
        single, pair.reshape(2, shape[0] // 2, *shape[1:]), residue_mask,
        w_bias, w_project, w_out, w_factors, w_pairout, w_up, w_down, row_size, col_size,
    )


def dispatch(row_size, col_size, *arrays):
    single, pair, residue_mask, w_bias, w_project, w_out, w_factors = arrays[:7]
    if fits(row_size, col_size, single, pair, residue_mask, w_bias, w_project, w_factors):
        return per_device_keys(row_size, col_size, *arrays)
    return per_device(row_size, col_size, *arrays)


def solution(mesh):
    return jax.shard_map(
        functools.partial(dispatch, mesh.shape["rows"], mesh.shape["cols"]),
        mesh=mesh,
        in_specs=(
            P("rows", None),
            P("rows", "cols", None),
            P(),
            P(),
            P(None, None, "cols"),
            P(),
            P(),
            P(),
            P(),
            P(),
        ),
        out_specs=(P("rows", None), P("rows", "cols", None)),
        check_vma=False,
    )
```

```python
import functools
import math

import jax
import jax.numpy as jnp
from jax import lax
from jax.experimental import pallas as pl
from jax.experimental.pallas import tpu as pltpu
from jax.sharding import PartitionSpec as P

epsilon = 1e-05


def enter(axes):
    barrier = pltpu.get_barrier_semaphore()
    total = 0
    for axis, size in axes:
        me = lax.axis_index(axis)
        for step in range(1, size):
            pl.semaphore_signal(
                barrier,
                inc=1,
                device_id={axis: lax.rem(me + step, size)},
                device_id_type=pl.DeviceIdType.MESH,
            )
        total += size - 1
    pl.semaphore_wait(barrier, total)


def spread(axis, size, source, landing, send_sems, recv_sems):
    me = lax.axis_index(axis)
    copies = []
    for step in range(1, size):
        copy = pltpu.make_async_remote_copy(
            src_ref=source,
            dst_ref=landing.at[me],
            send_sem=send_sems.at[step - 1],
            recv_sem=recv_sems.at[step - 1],
            device_id={axis: lax.rem(me + step, size)},
            device_id_type=pl.DeviceIdType.MESH,
        )
        copy.start()
        copies.append(copy)
    return copies


def gather_kernel(axis, size, source, gathered, send_sems, recv_sems, own_sem):
    enter([(axis, size)])
    copies = spread(axis, size, source, gathered, send_sems, recv_sems)
    own = pltpu.make_async_copy(source, gathered.at[lax.axis_index(axis)], own_sem)
    own.start()
    own.wait()
    for copy in copies:
        copy.wait()


def gather(values, axis, size, collective_id):
    return pl.pallas_call(
        functools.partial(gather_kernel, axis, size),
        out_shape=jax.ShapeDtypeStruct((size, *values.shape), values.dtype),
        in_specs=[pl.BlockSpec(memory_space=pltpu.VMEM)],
        out_specs=pl.BlockSpec(memory_space=pltpu.VMEM),
        scratch_shapes=[
            pltpu.SemaphoreType.DMA((size - 1,)),
            pltpu.SemaphoreType.DMA((size - 1,)),
            pltpu.SemaphoreType.DMA,
        ],
        compiler_params=pltpu.CompilerParams(collective_id=collective_id, has_side_effects=True),
        name="gather_" + axis,
    )(values)


def single_kernel(
    row_size, col_size, tile_cols,
    mixed, single, w_out, w_factors, single_out, left_out, right_out,
    gathered, factor_right, send_sems, recv_sems, row_send, row_recv, own_sem,
):
    enter([("cols", col_size), ("rows", row_size)])
    tile_rows, width = mixed.shape
    me_col = lax.axis_index("cols")
    me_row = lax.axis_index("rows")
    copies = spread("cols", col_size, mixed, gathered, send_sems, recv_sems)
    own = pltpu.make_async_copy(mixed, gathered.at[me_col], own_sem)
    own.start()
    own.wait()
    for copy in copies:
        copy.wait()
    whole = jnp.concatenate([gathered[part] for part in range(col_size)], axis=1)
    total = jnp.dot(whole, w_out[...], preferred_element_type=jnp.float32)
    updated = (single[...].astype(jnp.float32) + total).astype(jnp.bfloat16)
    single_out[...] = updated
    normed = layer_norm(updated).astype(jnp.bfloat16)
    factors = jnp.dot(normed, w_factors[...], preferred_element_type=jnp.float32)
    factors = factors.astype(jnp.bfloat16).astype(jnp.float32)
    half = factors.shape[1] // 2
    swapped = jnp.concatenate([factors[:, half:], factors[:, :half]], axis=1)
    lower = lax.broadcasted_iota(jnp.int32, factors.shape, 1) < half
    left_out[...] = jnp.where(lower, factors, swapped)
    factor_right[...] = jnp.where(lower, swapped, factors).astype(jnp.bfloat16)
    first = me_col * tile_cols
    owner = first // tile_rows
    offset = pl.multiple_of(first - owner * tile_rows, tile_cols)
    piece = factor_right.at[pl.ds(offset, tile_cols)]

    @pl.when(me_row == owner)
    def _():
        local = pltpu.make_async_copy(piece, right_out, own_sem)
        local.start()
        sends = []
        for step in range(1, row_size):
            send = pltpu.make_async_remote_copy(
                src_ref=piece,
                dst_ref=right_out,
                send_sem=row_send.at[step - 1],
                recv_sem=row_recv,
                device_id={"rows": lax.rem(me_row + step, row_size)},
                device_id_type=pl.DeviceIdType.MESH,
            )
            send.start()
            sends.append(send)
        local.wait()
        for send in sends:
            send.wait_send()

    @pl.when(me_row != owner)
    def _():
        pltpu.make_async_remote_copy(
            src_ref=piece,
            dst_ref=right_out,
            send_sem=row_send.at[0],
            recv_sem=row_recv,
            device_id={"rows": lax.rem(me_row + 1, row_size)},
            device_id_type=pl.DeviceIdType.MESH,
        ).wait_recv()


def update_single(mixed, single, w_out, w_factors, row_size, col_size, tile_cols):
    tile_rows, width = single.shape
    wide = w_factors.shape[1]
    return pl.pallas_call(
        functools.partial(single_kernel, row_size, col_size, tile_cols),
        out_shape=(
            jax.ShapeDtypeStruct((tile_rows, width), jnp.bfloat16),
            jax.ShapeDtypeStruct((tile_rows, wide), jnp.float32),
            jax.ShapeDtypeStruct((tile_cols, wide), jnp.bfloat16),
        ),
        in_specs=[pl.BlockSpec(memory_space=pltpu.VMEM)] * 4,
        out_specs=[pl.BlockSpec(memory_space=pltpu.VMEM)] * 3,
        scratch_shapes=[
            pltpu.VMEM((col_size, *mixed.shape), jnp.bfloat16),
            pltpu.VMEM((tile_rows, wide), jnp.bfloat16),
            pltpu.SemaphoreType.DMA((col_size - 1,)),
            pltpu.SemaphoreType.DMA((col_size - 1,)),
            pltpu.SemaphoreType.DMA((row_size - 1,)),
            pltpu.SemaphoreType.DMA,
            pltpu.SemaphoreType.DMA,
        ],
        compiler_params=pltpu.CompilerParams(collective_id=2, has_side_effects=True),
        name="update_single",
    )(mixed, single, w_out, w_factors)


def matmul_norm(values):
    wide = values.shape[1]
    share = jnp.full((2 * wide, wide), 1.0 / wide, jnp.bfloat16)
    mean = jnp.dot(values, share[:wide], preferred_element_type=jnp.float32)
    centred = values.astype(jnp.float32) - mean
    square = centred * centred
    high = square.astype(jnp.bfloat16)
    low = (square - high.astype(jnp.float32)).astype(jnp.bfloat16)
    spread_out = jnp.dot(
        jnp.concatenate([high, low], 1), share, preferred_element_type=jnp.float32
    )
    return (centred * lax.rsqrt(spread_out + epsilon)).astype(jnp.bfloat16)


def norm_kernel(values, normed):
    normed[...] = matmul_norm(values[...])


def norm_rows(values, block):
    spec = pl.BlockSpec((block, values.shape[1]), lambda step: (step, 0))
    return pl.pallas_call(
        norm_kernel,
        out_shape=jax.ShapeDtypeStruct(values.shape, jnp.bfloat16),
        grid=(values.shape[0] // block,),
        in_specs=[spec],
        out_specs=spec,
        name="norm_pair",
    )(values)


def pair_kernel(pair, left, right, w_pairout, w_up, w_down, updated):
    block_rows, tile_cols, wide = pair.shape
    left_wide = left[...][:, None, :]
    right_wide = right[...].astype(jnp.float32)[None, :, :]
    lower = lax.broadcasted_iota(jnp.int32, pair.shape, 2) < wide // 2
    paired = jnp.where(lower, left_wide * right_wide, left_wide - right_wide)
    paired = paired.astype(jnp.bfloat16).reshape(block_rows * tile_cols, wide)
    flat = pair[...].reshape(block_rows * tile_cols, wide).astype(jnp.float32)
    mid = flat + jnp.dot(paired, w_pairout[...], preferred_element_type=jnp.float32)
    mid = mid.astype(jnp.bfloat16)
    normed = matmul_norm(mid)
    hidden = jnp.dot(normed, w_up[...], preferred_element_type=jnp.float32)
    hidden = jnp.maximum(hidden, 0.0).astype(jnp.bfloat16)
    out = mid.astype(jnp.float32) + jnp.dot(
        hidden, w_down[...], preferred_element_type=jnp.float32
    )
    updated[...] = out.astype(jnp.bfloat16).reshape(pair.shape)


def update_pair(pair, left, right, w_pairout, w_up, w_down):
    tile_rows, tile_cols, wide = pair.shape
    block = math.gcd(tile_rows, max(8, 1024 // tile_cols))
    tile = pl.BlockSpec((block, tile_cols, wide), lambda step: (step, 0, 0))

    def whole(array):
        return pl.BlockSpec(array.shape, lambda step: (0, 0))

    return pl.pallas_call(
        pair_kernel,
        out_shape=jax.ShapeDtypeStruct(pair.shape, jnp.bfloat16),
        grid=(tile_rows // block,),
        in_specs=[
            tile,
            pl.BlockSpec((block, wide), lambda step: (step, 0)),
            whole(right),
            whole(w_pairout),
            whole(w_up),
            whole(w_down),
        ],
        out_specs=tile,
        name="update_pair",
    )(pair, left, right, w_pairout, w_up, w_down)


def layer_norm(values):
    values = values.astype(jnp.float32)
    centred = values - jnp.mean(values, -1, keepdims=True)
    return centred * lax.rsqrt(jnp.mean(centred * centred, -1, keepdims=True) + epsilon)


def per_device(
    row_size, col_size,
    single, pair, residue_mask, w_bias, w_project, w_out, w_factors, w_pairout, w_up, w_down
):
    tile_rows = pair.shape[0]
    tile_cols = pair.shape[1]
    normed_pair = norm_rows(
        pair.reshape(tile_rows * tile_cols, pair.shape[2]), math.gcd(tile_rows * tile_cols, 1024)
    ).reshape(pair.shape)
    bias_local = jnp.einsum(
        "rcp,ph->hrc", normed_pair, w_bias, preferred_element_type=jnp.float32
    ).astype(jnp.bfloat16)
    normed_single = layer_norm(single).astype(jnp.bfloat16)
    projected = jnp.einsum(
        "rs,fsc->frc", normed_single, w_project, preferred_element_type=jnp.float32
    )
    query_rows = projected[0].astype(jnp.bfloat16)
    key_local = projected[1].astype(jnp.bfloat16)
    value_local = projected[2].astype(jnp.bfloat16)
    gate_values = jax.nn.sigmoid(projected[3])
    bias_heads = lax.all_to_all(bias_local, "cols", split_axis=0, concat_axis=2, tiled=True)
    both = gather(jnp.concatenate([key_local, value_local], 1), "rows", row_size, 1)
    both = both.reshape(row_size * tile_rows, both.shape[2])
    key_rows, value_rows = both[:, : key_local.shape[1]], both[:, key_local.shape[1] :]
    heads_here = bias_heads.shape[0]
    head_width = query_rows.shape[1] // heads_here
    residues = key_rows.shape[0]
    query_split = query_rows.reshape(tile_rows, heads_here, head_width)
    key_split = key_rows.reshape(residues, heads_here, head_width)
    value_split = value_rows.reshape(residues, heads_here, head_width)
    score_scale = 1.0 / math.sqrt(head_width)
    scores = jnp.einsum(
        "rhd,lhd->hrl", query_split, key_split, preferred_element_type=jnp.float32
    ) * score_scale + bias_heads.astype(jnp.float32)
    key_valid = (residue_mask > 0)[None, None, :]
    scores = jnp.where(key_valid, scores, -jnp.inf)
    weights = jax.nn.softmax(scores, axis=-1).astype(jnp.bfloat16)
    attended = jnp.einsum("hrl,lhd->rhd", weights, value_split, preferred_element_type=jnp.float32)
    attended = attended.reshape(tile_rows, heads_here * head_width)
    mixed = (attended * gate_values).astype(jnp.bfloat16)
    single_out, left, right = update_single(
        mixed, single, w_out, w_factors, row_size, col_size, tile_cols
    )
    return (single_out, update_pair(pair, left, right, w_pairout, w_up, w_down))


LANES = 128
excluded = -1e30
update_block = 16


def lane_iota(shape):
    return lax.broadcasted_iota(jnp.int32, shape, len(shape) - 1)


def centre_matrix(wide, copies):
    size = wide * copies
    row = lax.broadcasted_iota(jnp.int32, (size, size), 0)
    col = lax.broadcasted_iota(jnp.int32, (size, size), 1)
    share = jnp.where(row // wide == col // wide, 1.0 / wide, 0.0)
    return (jnp.where(row == col, 1.0, 0.0) - share).astype(jnp.bfloat16)


def norm_centred(values, centre, copies):
    centred = jnp.dot(values, centre, preferred_element_type=jnp.float32)
    wide = values.shape[1] // copies
    parts = []
    for index in range(copies):
        part = centred[:, index * wide : (index + 1) * wide]
        square = jnp.sum(part * part, axis=1, keepdims=True) * (1.0 / wide)
        parts.append((part * lax.rsqrt(square + epsilon)).astype(jnp.bfloat16))
    return parts


def exchange(index, turn, size):
    total, bit = 0, 1
    while bit < size:
        total = total + lax.rem(index // bit + turn // bit, 2) * bit
        bit *= 2
    return total


def twice(weights):
    zeros = jnp.zeros_like(weights)
    upper = jnp.concatenate([weights, zeros], axis=1)
    return jnp.concatenate([upper, jnp.concatenate([zeros, weights], axis=1)], axis=0)


def update_rows(pair_of, left_of, right, rows, centre, w_pairout, w_up, w_down):
    tile_cols, wide = right.shape
    lower = lane_iota((rows, tile_cols, wide)) < wide // 2

    def paired(index):
        left_wide = left_of(index)[:, None, :]
        right_wide = right[None, :, :]
        chosen = jnp.where(lower, left_wide * right_wide, left_wide - right_wide)
        return chosen.astype(jnp.bfloat16).reshape(rows * tile_cols, wide)

    flat = [pair_of(index).reshape(rows * tile_cols, wide) for index in range(2)]
    mid = jnp.concatenate(flat, axis=1).astype(jnp.float32) + jnp.dot(
        jnp.concatenate([paired(0), paired(1)], axis=1),
        w_pairout,
        preferred_element_type=jnp.float32,
    )
    mid = mid.astype(jnp.bfloat16)
    normed = jnp.concatenate(norm_centred(mid, centre, 2), axis=0)
    mid = jnp.concatenate([mid[:, :wide], mid[:, wide:]], axis=0)
    hidden = jnp.dot(normed, w_up, preferred_element_type=jnp.float32)
    hidden = jnp.maximum(hidden, 0.0).astype(jnp.bfloat16)
    out = mid.astype(jnp.float32) + jnp.dot(hidden, w_down, preferred_element_type=jnp.float32)
    return out.astype(jnp.bfloat16).reshape(2 * rows, tile_cols, wide)


def attend_kernel(
    row_size, col_size, heads, tile_cols, stride,
    single, pair, mask, w_bias, w_project, w_out, w_factors, w_pairout, w_up, w_down,
    single_out, pair_out,
    single_v, pair_v, mask_v, bias_w, project_v, out_v, factors_v, own_single,
    kv_send, kv_recv, q_recv, gate_send, gate_recv, bias_v, o_send, o_recv,
    st_send, st_recv, left_send, right_send, left_recv, right_recv, left_out, right_out, so_send, centre_v, spread_v,
    pairout_v, twice_v, up_v, down_v,
    load_sems, pair_sems, col_send, col_recv, fan_send, fan_recv,
    plane_sent, plane_came, kv_sent, kv_came, kv_relayed, q_sent, q_came, o_sent, o_came,
):
    me_row = lax.axis_index("rows")
    me_col = lax.axis_index("cols")
    total = row_size * col_size
    halves, depth, _, wide = pair.shape
    tile_rows, width = single.shape
    group = w_project.shape[2]
    rows_each = depth // col_size
    heads_here = heads // col_size
    head_width = group // heads_here
    chunk = depth // pair_sems.shape[0]
    loads = [
        pltpu.make_async_copy(source, target, load_sems.at[index])
        for index, (source, target) in enumerate(
            [(single, single_v)]
            + [(w_project.at[part], project_v.at[part]) for part in range(4)]
            + [(w_bias, bias_w), (mask, mask_v)]
            + [
                (single.at[pl.ds(half * depth + me_col * rows_each, rows_each)], own_single.at[half])
                for half in range(halves)
            ]
            + [(w_out, out_v), (w_factors, factors_v)]
            + [(w_pairout, pairout_v), (w_up, up_v), (w_down, down_v)]
        )
    ]
    for copy in loads[:7]:
        copy.start()
    barrier = pltpu.get_barrier_semaphore()
    me = me_row * col_size + me_col
    for step in range(1, total):
        to = lax.rem(me + step, total)
        pl.semaphore_signal(
            barrier,
            inc=1,
            device_id={"rows": to // col_size, "cols": lax.rem(to, col_size)},
            device_id_type=pl.DeviceIdType.MESH,
        )

    def pair_load(step):
        part = pl.ds(step * chunk, chunk)
        return pltpu.make_async_copy(pair.at[:, part], pair_v.at[:, part], pair_sems.at[step])

    for step in range(depth // chunk):
        pair_load(step).start()
    for copy in loads[7:]:
        copy.start()

    centre_v[...] = centre_matrix(wide, halves)

    def to_cols(kind, source_of, target):
        copies = []
        for step in range(1, col_size):
            to = lax.rem(me_col + step, col_size)
            copy = pltpu.make_async_remote_copy(
                src_ref=source_of(to),
                dst_ref=target,
                send_sem=col_send.at[kind, step - 1],
                recv_sem=col_recv.at[kind, step - 1],
                device_id={"cols": to},
                device_id_type=pl.DeviceIdType.MESH,
            )
            copy.start()
            copies.append(copy)
        return copies

    owner = me_col // halves
    mine = owner == me_row
    half_mine = lax.rem(me_col, halves)

    def fan_copies(kind, source_of, target):
        copies = []
        for step in range(row_size):
            for half in range(halves):
                to = halves * me_row + half
                copy = pltpu.make_async_remote_copy(
                    src_ref=source_of(half),
                    dst_ref=target.at[me_col],
                    send_sem=fan_send.at[kind, step * halves + half],
                    recv_sem=fan_recv.at[kind, me_col],
                    device_id={"rows": lax.rem(me_row + step, row_size), "cols": to},
                    device_id_type=pl.DeviceIdType.MESH,
                )
                copies.append((copy, step, to))
        return copies

    def on_some(copies, act):
        for copy, condition in copies:
            if condition is None:
                act(copy)
            else:
                pl.when(condition)(functools.partial(act, copy))

    kind_mine = lax.rem(me_row, 2)
    me_plane = me_row // 2
    row_mate = me_row + 1 - 2 * kind_mine
    col_mate = me_col + 1 - 2 * lax.rem(me_col, 2)

    def relay_keys(part, kind, slot):
        return pltpu.make_async_remote_copy(
            src_ref=kv_recv.at[part, kind],
            dst_ref=kv_recv.at[part, kind],
            send_sem=kv_relayed.at[slot],
            recv_sem=kv_came.at[kind, part],
            device_id={"rows": row_mate},
            device_id_type=pl.DeviceIdType.MESH,
        )

    def send_query(part, to, slot):
        return pltpu.make_async_remote_copy(
            src_ref=q_recv.at[part],
            dst_ref=q_recv.at[part],
            send_sem=q_sent.at[slot],
            recv_sem=q_came.at[part],
            device_id={"cols": to},
            device_id_type=pl.DeviceIdType.MESH,
        )

    def on_fan(copies, act):
        for copy, step, to in copies:
            if step:
                act(copy)
            else:
                pl.when(to != me_col)(functools.partial(act, copy))

    def fan_wait(kind, source_of, target):
        for part in range(col_size):
            copy = pltpu.make_async_remote_copy(
                src_ref=source_of(0),
                dst_ref=target.at[part],
                send_sem=fan_send.at[kind, 0],
                recv_sem=fan_recv.at[kind, part],
                device_id={"rows": lax.rem(me_row + 1, row_size)},
                device_id_type=pl.DeviceIdType.MESH,
            )
            pl.when(jnp.logical_not(jnp.logical_and(mine, part == me_col)))(copy.wait_recv)

    loads[0].wait()
    normed = layer_norm(single_v[...]).astype(jnp.bfloat16)
    def project(*kinds):
        weights = [project_v[kind] for kind in kinds]
        return jnp.dot(
            normed, jnp.concatenate(weights, axis=1), preferred_element_type=jnp.float32
        )

    loads[1].wait()
    q_recv[me_col] = project(0).astype(jnp.bfloat16)
    pl.semaphore_wait(barrier, total - 1)
    parts, _, _, part_width = o_send.shape
    each = part_width // group
    col_side = lax.rem(me_col, each)

    def turn_step(turn):
        return exchange(me_col // each, turn, parts)

    peers = [turn_step(turn) * each + col_side for turn in range(1, parts)]
    q_copies = [send_query(me_col, to, slot) for slot, to in enumerate(peers)]
    q_copies.append(send_query(me_col, col_mate, len(peers)))
    for copy in q_copies:
        copy.start()
    loads[2].wait()
    loads[3].wait()
    key_value = project(1, 2).astype(jnp.bfloat16)
    for half in range(halves):
        for kind in range(2):
            kv_send[me_plane, half, kind] = key_value[
                half * tile_cols : (half + 1) * tile_cols, kind * group : (kind + 1) * group
            ]
    planes = row_size // 2
    plane_copies = []
    for step in range(1, planes):
        plane = lax.rem(me_plane + step, planes)
        copy = pltpu.make_async_remote_copy(
            src_ref=kv_send.at[me_plane],
            dst_ref=kv_send.at[me_plane],
            send_sem=plane_sent.at[step - 1],
            recv_sem=plane_came.at[step - 1],
            device_id={"rows": 2 * plane + kind_mine},
            device_id_type=pl.DeviceIdType.MESH,
        )
        copy.start()
        plane_copies.append(copy)
    kv_copies = []

    def send_keys(step):
        plane = lax.rem(me_plane + planes - step, planes)
        for half in range(halves):
            for kind in range(2):
                to = halves * (2 * plane + kind_mine) + half
                row = 2 * me_plane + kind
                copy = pltpu.make_async_remote_copy(
                    src_ref=kv_send.at[plane, half, kind],
                    dst_ref=kv_recv.at[me_col, kind],
                    send_sem=kv_sent.at[(step * 2 + kind) * halves + half],
                    recv_sem=kv_came.at[kind, me_col],
                    device_id={"rows": row, "cols": to},
                    device_id_type=pl.DeviceIdType.MESH,
                )
                here = jnp.logical_and(row == me_row, to == me_col)
                kv_copies.append((copy, jnp.logical_not(here)))
        on_some(kv_copies[-2 * halves :], lambda copy: copy.start())

    send_keys(0)
    loads[4].wait()
    gate_send[...] = jax.nn.sigmoid(project(3)).reshape(halves, depth, group)

    def own_rows(to):
        return pl.ds(pl.multiple_of(to * rows_each, rows_each), rows_each)

    loads[5].wait()
    loads[6].wait()

    def relay_query(part):
        return send_query(part, col_mate, col_size // 2 + part // each)

    def bias_step(step, _):
        pair_load(step).wait()
        parts = [
            pair_v[half, pl.ds(step * chunk, chunk)].reshape(chunk * tile_cols, wide)
            for half in range(halves)
        ]
        parts = norm_centred(jnp.concatenate(parts, axis=1), centre_v[...], halves)
        parts = [part.reshape(chunk, 1, tile_cols, wide) for part in parts]
        normed_pair = jnp.concatenate(parts, axis=1).reshape(chunk * halves * tile_cols, wide)
        bias = lax.dot_general(
            bias_w[...], normed_pair, (((1,), (1,)), ((), ())), preferred_element_type=jnp.float32
        )
        bias = bias.astype(jnp.bfloat16).astype(jnp.float32)
        for part in range(chunk):
            bias_v[pl.ds(step * chunk + part, heads, stride=stride), :] = bias[
                :, part * LANES : (part + 1) * LANES
            ]
        return 0

    lax.fori_loop(0, depth // chunk, bias_step, 0)
    for step in range(1, planes):
        plane_copies[step - 1].wait_recv()
        send_keys(step)
    own_key = lax.rem(owner, 2) == kind_mine

    @pl.when(own_key)
    def _():
        kv_recv[me_col, kind_mine] = kv_send[owner // 2, half_mine, kind_mine]

    def relay_keys_turn(turn):
        for index in range(each):
            part = turn_step(turn) * each + index
            copy = relay_keys(part, kind_mine, part)
            own = jnp.logical_and(own_key, part == me_col)
            pl.when(jnp.logical_not(own))(copy.wait_recv)
            copy.start()

    same_plane = owner // 2 == me_plane
    pl.when(same_plane)(functools.partial(relay_keys_turn, 0))
    relays = [relay_query(peer) for peer in peers]
    for copy in relays:
        copy.wait_recv()
        copy.start()
    pl.when(jnp.logical_not(same_plane))(functools.partial(relay_keys_turn, 0))
    relay_keys_turn(1)
    relays += [relay_keys(part, kind_mine, part) for part in range(col_size)]

    def gate_copy(shift):
        to = lax.rem(me_col + shift, col_size)
        return pltpu.make_async_remote_copy(
            src_ref=gate_send.at[:, own_rows(to)],
            dst_ref=gate_recv.at[me_col],
            send_sem=col_send.at[1, shift - 1],
            recv_sem=col_recv.at[1, shift - 1],
            device_id={"cols": to},
            device_id_type=pl.DeviceIdType.MESH,
        )

    gate_copies = [gate_copy(shift) for shift in range(1, col_size)]
    for copy in gate_copies:
        copy.start()
    gate_recv[me_col] = gate_send[:, own_rows(me_col)]

    lane_row = lane_iota((2 * halves * heads, width))
    place = lax.broadcasted_iota(jnp.int32, (2 * halves * heads, width), 0)
    for half in range(halves):
        picked = jnp.where(place == half * heads + lane_row // head_width, 1.0, 0.0)
        spread_v[half, :LANES] = picked.astype(jnp.bfloat16)
        spread_v[half, LANES:] = picked.astype(jnp.bfloat16)

    length = jnp.sum(jnp.sum(mask_v[...], axis=1, keepdims=True), axis=0, keepdims=True)
    lane = lane_iota((depth, LANES))
    low = lane < tile_cols
    valid = me_col * tile_cols + lax.rem(lane, tile_cols) < length
    head_of = lane_iota((tile_cols, group)) // head_width
    head_masks = [
        jnp.where(head_of == head, 1.0, 0.0).astype(jnp.bfloat16) for head in range(heads_here)
    ]
    zeros = jnp.zeros((tile_cols, group), jnp.bfloat16)
    scale = 1.0 / math.sqrt(head_width)
    st_send[...] = jnp.zeros_like(st_send)
    block_place = lax.broadcasted_iota(jnp.int32, (heads_here * LANES, LANES), 0) // tile_cols
    block_target = (
        halves * heads + lax.rem(block_place, halves) * heads + block_place // halves
    )
    block_lane = lane_iota((heads_here * LANES, LANES))

    def attend_part(part):
        query = q_recv[part]
        query = jnp.concatenate([query[:depth], query[depth:]], axis=1)
        key, value = kv_recv[part, 0], kv_recv[part, 1]
        weights, value_rows = [], []
        stats = st_send[...]
        for first in range(0, heads_here, 2):
            key_rows = []
            for head in (first, first + 1):
                masked = key * head_masks[head]
                key_rows.append(jnp.concatenate([masked, zeros], axis=1))
                key_rows.append(jnp.concatenate([zeros, masked], axis=1))
            raw = lax.dot_general(
                query,
                jnp.concatenate(key_rows, axis=0),
                (((1,), (1,)), ((), ())),
                preferred_element_type=jnp.float32,
            )
            for head in (first, first + 1):
                index = part * heads_here + head
                bias = bias_v[pl.ds(pl.multiple_of(index * stride, 8), depth), :]
                scores = raw[:, (head - first) * LANES : (head - first + 1) * LANES] * scale + bias
                scores = jnp.where(valid, scores, excluded)
                top0 = jnp.max(jnp.where(low, scores, excluded), axis=1, keepdims=True)
                top1 = jnp.max(jnp.where(low, excluded, scores), axis=1, keepdims=True)
                weights.append(
                    jnp.exp(scores - jnp.where(low, top0, top1)).astype(jnp.bfloat16)
                )
                stats = jnp.where(lane == index, top0, stats)
                stats = jnp.where(lane == heads + index, top1, stats)
        for head in range(heads_here):
            masked = value * head_masks[head]
            value_rows.append(jnp.concatenate([masked, zeros], axis=1))
            value_rows.append(jnp.concatenate([zeros, masked], axis=1))
        weights = jnp.concatenate(weights, axis=1)
        mixed = jnp.dot(
            weights, jnp.concatenate(value_rows, axis=0), preferred_element_type=jnp.float32
        )
        ones = jnp.where(block_lane == block_target + part * heads_here, 1.0, 0.0)
        sums = jnp.dot(weights, ones.astype(jnp.bfloat16), preferred_element_type=jnp.float32)
        st_send[...] = stats + sums
        pieces = [
            mixed[:, half * group : (half + 1) * group].reshape(col_size, rows_each, group)
            for half in range(halves)
        ]
        return jnp.concatenate(pieces, axis=1).astype(jnp.bfloat16)

    def o_copy(step, shift):
        to = lax.rem(me_col + shift, col_size)
        return pltpu.make_async_remote_copy(
            src_ref=o_send.at[step, to],
            dst_ref=o_recv.at[step, me_col],
            send_sem=o_sent.at[step, shift - 1],
            recv_sem=o_came.at[step, shift - 1],
            device_id={"cols": to},
            device_id_type=pl.DeviceIdType.MESH,
        )

    def st_copy(shift):
        to = lax.rem(me_col + shift, col_size)
        return pltpu.make_async_remote_copy(
            src_ref=st_send.at[own_rows(to)],
            dst_ref=st_recv.at[me_col],
            send_sem=col_send.at[2, shift - 1],
            recv_sem=col_recv.at[2, shift - 1],
            device_id={"cols": to},
            device_id_type=pl.DeviceIdType.MESH,
        )

    def attend_step(turn, _):
        step = turn_step(turn)
        far = step * each + 1 - col_side
        relay_query(far).wait_recv()
        for index in range(each):
            part = step * each + index
            relay_keys(part, 1 - kind_mine, part).wait_recv()
        for index in range(each):
            o_send[step, :, :, index * group : (index + 1) * group] = attend_part(
                step * each + index
            )

        @pl.when(turn == parts - 1)
        def _():
            for shift in range(1, col_size):
                st_copy(shift).start()

        for shift in range(1, col_size):
            o_copy(step, shift).start()
        pl.when(turn + 2 < parts)(functools.partial(relay_keys_turn, turn + 2))
        return 0

    lax.fori_loop(0, parts, attend_step, 0)
    st_copies = [st_copy(shift) for shift in range(1, col_size)]
    st_recv[me_col] = st_send[own_rows(me_col)]
    for step in range(parts):
        o_recv[step, me_col] = o_send[step, me_col]
    o_copies = [o_copy(step, shift) for step in range(parts) for shift in range(1, col_size)]
    for copy in gate_copies + st_copies:
        copy.wait_recv()
    stats = st_recv[...]
    lane = lane_iota(stats.shape)
    top = jnp.max(stats, axis=0, keepdims=True)
    factor = jnp.exp(stats - top)
    sums = jnp.sum(factor * pltpu.roll(stats, halves * heads, axis=2), axis=0, keepdims=True)
    factor = jnp.where(lane < halves * heads, factor / sums, 0.0)
    factor = factor.reshape(col_size * rows_each, LANES)
    high = factor.astype(jnp.bfloat16)
    rest = (factor - high.astype(jnp.float32)).astype(jnp.bfloat16)
    factor = jnp.concatenate([high, rest], axis=1)
    scales = [
        jnp.dot(factor, spread_v[half], preferred_element_type=jnp.float32) for half in range(halves)
    ]
    gate = jnp.concatenate(
        [gate_recv[part].reshape(halves * rows_each, group) for part in range(col_size)], axis=1
    )
    for copy in o_copies:
        copy.wait_recv()
    attended = jnp.zeros((halves * rows_each, width), jnp.float32)
    for part in range(col_size):
        rows = slice(part * rows_each, (part + 1) * rows_each)
        part_scale = jnp.concatenate([scales[half][rows] for half in range(halves)], axis=0)
        whole = jnp.concatenate([o_recv[step, part] for step in range(parts)], axis=1)
        attended = attended + part_scale * whole.astype(jnp.float32)
    mixed = (attended * gate).astype(jnp.bfloat16)
    for copy in loads[7:]:
        copy.wait()
    added = jnp.dot(mixed, out_v[...], preferred_element_type=jnp.float32)
    own = own_single[...].astype(jnp.float32).reshape(halves * rows_each, width)
    updated = (own + added).astype(jnp.bfloat16)
    so_send[...] = updated.astype(jnp.float32).reshape(halves, rows_each, width).astype(jnp.bfloat16)
    factors = jnp.dot(
        layer_norm(updated).astype(jnp.bfloat16),
        factors_v[...],
        preferred_element_type=jnp.float32,
    )
    factors = factors.astype(jnp.bfloat16).astype(jnp.float32)
    first, second = factors[:rows_each], factors[rows_each:]
    shift = factors.shape[1] // 2
    low = lane_iota(first.shape) < shift
    left = jnp.where(low, first, pltpu.roll(second, shift, axis=1))
    right = jnp.where(low, pltpu.roll(first, shift, axis=1), second)
    left_send[...] = left.astype(jnp.bfloat16)
    right_send[...] = right.astype(jnp.bfloat16)
    right_copies = fan_copies(1, lambda half: right_send, right_recv)
    on_fan(right_copies, lambda copy: copy.start())
    left_copies = to_cols(4, lambda to: left_send, left_recv.at[me_col])
    left_recv[me_col] = left.astype(jnp.bfloat16)

    @pl.when(mine)
    def _():
        right_recv[me_col] = right_send[...]

    fan_wait(1, lambda half: right_send, right_recv)
    for copy in left_copies:
        copy.wait_recv()
    so_copies = to_cols(5, lambda to: so_send, single_out.at[:, me_col])
    single_out[:, me_col] = so_send[...]
    left = left_recv[...].astype(jnp.float32).reshape(depth, LANES)
    turned = pltpu.roll(left, shift, axis=1)
    low = lane_iota(left.shape) < shift
    left_out[:depth] = jnp.where(low, left, turned)
    left_out[depth:] = jnp.where(low, turned, left)
    right = right_recv[...].astype(jnp.float32).reshape(tile_cols, LANES)
    turned = pltpu.roll(right, shift, axis=1)
    right_out[...] = jnp.where(lane_iota(right.shape) // shift == half_mine, right, turned)

    twice_v[...] = twice(pairout_v[...])
    block = update_block
    def update_step(step, _):
        first = step * 2 * block
        half = first // depth
        pair_out[pl.ds(first, 2 * block)] = update_rows(
            lambda index: pair_v[half, pl.ds(first - half * depth + index * block, block)],
            lambda index: left_out[pl.ds(pl.multiple_of(first + index * block, 8), block)],
            right_out[...],
            block,
            centre_v[...],
            twice_v[...],
            up_v[...],
            down_v[...],
        )
        return 0

    lax.fori_loop(0, tile_rows // (2 * block), update_step, 0)

    for copies in (q_copies, relays, plane_copies, gate_copies, st_copies, o_copies, left_copies, so_copies):
        for copy in copies:
            copy.wait_send()
    on_some(kv_copies, lambda copy: copy.wait_send())
    on_fan(right_copies, lambda copy: copy.wait_send())
    for copy in so_copies:
        copy.wait_recv()


def finish_kernel(single, pair, single_out, pair_out, sems):
    copies = [pltpu.make_async_copy(single, single_out, sems.at[0])]
    steps = sems.shape[0] - 1
    rows = pair.shape[0] // steps
    for step in range(steps):
        part = pl.ds(step * rows, rows)
        copies.append(
            pltpu.make_async_copy(pair.at[part], pair_out.at[part], sems.at[1 + step])
        )
    for copy in copies:
        copy.start()
    for copy in copies:
        copy.wait()


def finish(single, pair):
    return pl.pallas_call(
        finish_kernel,
        out_shape=tuple(jax.ShapeDtypeStruct(array.shape, array.dtype) for array in (single, pair)),
        in_specs=[pl.BlockSpec(memory_space=pltpu.VMEM)] * 2,
        out_specs=[pl.BlockSpec(memory_space=pl.ANY)] * 2,
        scratch_shapes=[pltpu.SemaphoreType.DMA((9,))],
        compiler_params=pltpu.CompilerParams(vmem_limit_bytes=8 * 1024 * 1024),
        name="finish",
    )(single, pair)


def attend(
    single, pair, mask, w_bias, w_project, w_out, w_factors, w_pairout, w_up, w_down,
    row_size, col_size,
):
    halves, depth, tile_cols, wide = pair.shape
    tile_rows, width = single.shape
    heads = w_bias.shape[1]
    rows_each = depth // col_size
    group = w_project.shape[2]
    steps = depth // 16
    parts = col_size // 2
    stride = depth + 8
    any_spec = pl.BlockSpec(memory_space=pltpu.HBM)
    vmem_spec = pl.BlockSpec(memory_space=pltpu.VMEM)
    bf16, f32 = jnp.bfloat16, jnp.float32
    single_out, pair_out = pl.pallas_call(
        functools.partial(attend_kernel, row_size, col_size, heads, tile_cols, stride),
        out_shape=(
            pltpu.VMEM((halves, col_size, rows_each, width), bf16),
            pltpu.VMEM((tile_rows, tile_cols, wide), bf16),
        ),
        in_specs=[any_spec] * 10,
        out_specs=[vmem_spec] * 2,
        scratch_shapes=[
            pltpu.VMEM((tile_rows, width), bf16),
            pltpu.VMEM((halves, depth, tile_cols, wide), bf16),
            pltpu.VMEM((mask.shape[0] // LANES, LANES), jnp.int32),
            pltpu.VMEM((heads, wide), bf16),
            pltpu.VMEM(w_project.shape, bf16),
            pltpu.VMEM(w_out.shape, bf16),
            pltpu.VMEM(w_factors.shape, bf16),
            pltpu.VMEM((halves, rows_each, width), bf16),
            pltpu.VMEM((row_size // 2, halves, 2, tile_cols, group), bf16),
            pltpu.VMEM((col_size, 2, tile_cols, group), bf16),
            pltpu.VMEM((col_size, tile_rows, group), bf16),
            pltpu.VMEM((halves, depth, group), f32),
            pltpu.VMEM((col_size, halves, rows_each, group), f32),
            pltpu.VMEM((heads * stride, LANES), f32),
            pltpu.VMEM((parts, col_size, halves * rows_each, width // parts), bf16),
            pltpu.VMEM((parts, col_size, halves * rows_each, width // parts), bf16),
            pltpu.VMEM((depth, LANES), f32),
            pltpu.VMEM((col_size, rows_each, LANES), f32),
            pltpu.VMEM((rows_each, LANES), bf16),
            pltpu.VMEM((rows_each, LANES), bf16),
            pltpu.VMEM((col_size, rows_each, LANES), bf16),
            pltpu.VMEM((col_size, rows_each, LANES), bf16),
            pltpu.VMEM((tile_rows, wide), f32),
            pltpu.VMEM((tile_cols, wide), f32),
            pltpu.VMEM((halves, rows_each, width), bf16),
            pltpu.VMEM((halves * wide, halves * wide), bf16),
            pltpu.VMEM((halves, 2 * LANES, width), bf16),
            pltpu.VMEM(w_pairout.shape, bf16),
            pltpu.VMEM((2 * wide, 2 * wide), bf16),
            pltpu.VMEM(w_up.shape, bf16),
            pltpu.VMEM(w_down.shape, bf16),
            pltpu.SemaphoreType.DMA((12 + halves,)),
            pltpu.SemaphoreType.DMA((steps,)),
            pltpu.SemaphoreType.DMA((6, col_size - 1)),
            pltpu.SemaphoreType.DMA((6, col_size - 1)),
            pltpu.SemaphoreType.DMA((2, row_size * halves)),
            pltpu.SemaphoreType.DMA((2, col_size)),
            pltpu.SemaphoreType.DMA((row_size // 2 - 1,)),
            pltpu.SemaphoreType.DMA((row_size // 2 - 1,)),
            pltpu.SemaphoreType.DMA((row_size * halves,)),
            pltpu.SemaphoreType.DMA((2, col_size)),
            pltpu.SemaphoreType.DMA((col_size,)),
            pltpu.SemaphoreType.DMA((2 * col_size,)),
            pltpu.SemaphoreType.DMA((col_size,)),
            pltpu.SemaphoreType.DMA((parts, col_size - 1)),
            pltpu.SemaphoreType.DMA((parts, col_size - 1)),
        ],
        compiler_params=pltpu.CompilerParams(
            collective_id=3, has_side_effects=True, vmem_limit_bytes=40 * 1024 * 1024
        ),
        name="attend",
    )(
        *(
            pltpu.with_memory_space_constraint(array, pltpu.HBM)
            for array in (
                single,
                pair,
                mask.reshape(mask.shape[0] // LANES, LANES),
                w_bias.T,
                w_project,
                w_out,
                w_factors,
                w_pairout,
                w_up,
                w_down,
            )
        )
    )
    single_out, pair_out = finish(single_out, pair_out)
    return single_out.reshape(tile_rows, width), pair_out


def fits(row_size, col_size, single, pair, mask, w_bias, w_project, w_factors):
    tile_rows, tile_cols, wide = pair.shape
    heads = w_bias.shape[1]
    return (
        tile_rows == 2 * tile_cols
        and 2 * tile_cols == LANES
        and wide == LANES
        and w_factors.shape[1] == LANES
        and w_project.shape[2] == LANES
        and 4 * heads == LANES
        and heads % (2 * col_size) == 0
        and tile_cols % (8 * col_size) == 0
        and col_size == 2 * row_size
        and row_size % 2 == 0
        and col_size & (col_size - 1) == 0
        and tile_cols % (2 * update_block) == 0
        and mask.shape[0] % LANES == 0
    )


def per_device_keys(
    row_size, col_size,
    single, pair, residue_mask, w_bias, w_project, w_out, w_factors, w_pairout, w_up, w_down
):
    shape = pair.shape
    return attend(
        single, pair.reshape(2, shape[0] // 2, *shape[1:]), residue_mask,
        w_bias, w_project, w_out, w_factors, w_pairout, w_up, w_down, row_size, col_size,
    )


def dispatch(row_size, col_size, *arrays):
    single, pair, residue_mask, w_bias, w_project, w_out, w_factors = arrays[:7]
    if fits(row_size, col_size, single, pair, residue_mask, w_bias, w_project, w_factors):
        return per_device_keys(row_size, col_size, *arrays)
    return per_device(row_size, col_size, *arrays)


def solution(mesh):
    return jax.shard_map(
        functools.partial(dispatch, mesh.shape["rows"], mesh.shape["cols"]),
        mesh=mesh,
        in_specs=(
            P("rows", None),
            P("rows", "cols", None),
            P(),
            P(),
            P(None, None, "cols"),
            P(),
            P(),
            P(),
            P(),
            P(),
        ),
        out_specs=(P("rows", None), P("rows", "cols", None)),
        check_vma=False,
    )
```

```python
import functools
import math

import jax
import jax.numpy as jnp
from jax import lax
from jax.experimental import pallas as pl
from jax.experimental.pallas import tpu as pltpu
from jax.sharding import PartitionSpec as P

epsilon = 1e-05


def enter(axes):
    barrier = pltpu.get_barrier_semaphore()
    total = 0
    for axis, size in axes:
        me = lax.axis_index(axis)
        for step in range(1, size):
            pl.semaphore_signal(
                barrier,
                inc=1,
                device_id={axis: lax.rem(me + step, size)},
                device_id_type=pl.DeviceIdType.MESH,
            )
        total += size - 1
    pl.semaphore_wait(barrier, total)


def spread(axis, size, source, landing, send_sems, recv_sems):
    me = lax.axis_index(axis)
    copies = []
    for step in range(1, size):
        copy = pltpu.make_async_remote_copy(
            src_ref=source,
            dst_ref=landing.at[me],
            send_sem=send_sems.at[step - 1],
            recv_sem=recv_sems.at[step - 1],
            device_id={axis: lax.rem(me + step, size)},
            device_id_type=pl.DeviceIdType.MESH,
        )
        copy.start()
        copies.append(copy)
    return copies


def gather_kernel(axis, size, source, gathered, send_sems, recv_sems, own_sem):
    enter([(axis, size)])
    copies = spread(axis, size, source, gathered, send_sems, recv_sems)
    own = pltpu.make_async_copy(source, gathered.at[lax.axis_index(axis)], own_sem)
    own.start()
    own.wait()
    for copy in copies:
        copy.wait()


def gather(values, axis, size, collective_id):
    return pl.pallas_call(
        functools.partial(gather_kernel, axis, size),
        out_shape=jax.ShapeDtypeStruct((size, *values.shape), values.dtype),
        in_specs=[pl.BlockSpec(memory_space=pltpu.VMEM)],
        out_specs=pl.BlockSpec(memory_space=pltpu.VMEM),
        scratch_shapes=[
            pltpu.SemaphoreType.DMA((size - 1,)),
            pltpu.SemaphoreType.DMA((size - 1,)),
            pltpu.SemaphoreType.DMA,
        ],
        compiler_params=pltpu.CompilerParams(collective_id=collective_id, has_side_effects=True),
        name="gather_" + axis,
    )(values)


def single_kernel(
    row_size, col_size, tile_cols,
    mixed, single, w_out, w_factors, single_out, left_out, right_out,
    gathered, factor_right, send_sems, recv_sems, row_send, row_recv, own_sem,
):
    enter([("cols", col_size), ("rows", row_size)])
    tile_rows, width = mixed.shape
    me_col = lax.axis_index("cols")
    me_row = lax.axis_index("rows")
    copies = spread("cols", col_size, mixed, gathered, send_sems, recv_sems)
    own = pltpu.make_async_copy(mixed, gathered.at[me_col], own_sem)
    own.start()
    own.wait()
    for copy in copies:
        copy.wait()
    whole = jnp.concatenate([gathered[part] for part in range(col_size)], axis=1)
    total = jnp.dot(whole, w_out[...], preferred_element_type=jnp.float32)
    updated = (single[...].astype(jnp.float32) + total).astype(jnp.bfloat16)
    single_out[...] = updated
    normed = layer_norm(updated).astype(jnp.bfloat16)
    factors = jnp.dot(normed, w_factors[...], preferred_element_type=jnp.float32)
    factors = factors.astype(jnp.bfloat16).astype(jnp.float32)
    half = factors.shape[1] // 2
    swapped = jnp.concatenate([factors[:, half:], factors[:, :half]], axis=1)
    lower = lax.broadcasted_iota(jnp.int32, factors.shape, 1) < half
    left_out[...] = jnp.where(lower, factors, swapped)
    factor_right[...] = jnp.where(lower, swapped, factors).astype(jnp.bfloat16)
    first = me_col * tile_cols
    owner = first // tile_rows
    offset = pl.multiple_of(first - owner * tile_rows, tile_cols)
    piece = factor_right.at[pl.ds(offset, tile_cols)]

    @pl.when(me_row == owner)
    def _():
        local = pltpu.make_async_copy(piece, right_out, own_sem)
        local.start()
        sends = []
        for step in range(1, row_size):
            send = pltpu.make_async_remote_copy(
                src_ref=piece,
                dst_ref=right_out,
                send_sem=row_send.at[step - 1],
                recv_sem=row_recv,
                device_id={"rows": lax.rem(me_row + step, row_size)},
                device_id_type=pl.DeviceIdType.MESH,
            )
            send.start()
            sends.append(send)
        local.wait()
        for send in sends:
            send.wait_send()

    @pl.when(me_row != owner)
    def _():
        pltpu.make_async_remote_copy(
            src_ref=piece,
            dst_ref=right_out,
            send_sem=row_send.at[0],
            recv_sem=row_recv,
            device_id={"rows": lax.rem(me_row + 1, row_size)},
            device_id_type=pl.DeviceIdType.MESH,
        ).wait_recv()


def update_single(mixed, single, w_out, w_factors, row_size, col_size, tile_cols):
    tile_rows, width = single.shape
    wide = w_factors.shape[1]
    return pl.pallas_call(
        functools.partial(single_kernel, row_size, col_size, tile_cols),
        out_shape=(
            jax.ShapeDtypeStruct((tile_rows, width), jnp.bfloat16),
            jax.ShapeDtypeStruct((tile_rows, wide), jnp.float32),
            jax.ShapeDtypeStruct((tile_cols, wide), jnp.bfloat16),
        ),
        in_specs=[pl.BlockSpec(memory_space=pltpu.VMEM)] * 4,
        out_specs=[pl.BlockSpec(memory_space=pltpu.VMEM)] * 3,
        scratch_shapes=[
            pltpu.VMEM((col_size, *mixed.shape), jnp.bfloat16),
            pltpu.VMEM((tile_rows, wide), jnp.bfloat16),
            pltpu.SemaphoreType.DMA((col_size - 1,)),
            pltpu.SemaphoreType.DMA((col_size - 1,)),
            pltpu.SemaphoreType.DMA((row_size - 1,)),
            pltpu.SemaphoreType.DMA,
            pltpu.SemaphoreType.DMA,
        ],
        compiler_params=pltpu.CompilerParams(collective_id=2, has_side_effects=True),
        name="update_single",
    )(mixed, single, w_out, w_factors)


def matmul_norm(values):
    wide = values.shape[1]
    share = jnp.full((2 * wide, wide), 1.0 / wide, jnp.bfloat16)
    mean = jnp.dot(values, share[:wide], preferred_element_type=jnp.float32)
    centred = values.astype(jnp.float32) - mean
    square = centred * centred
    high = square.astype(jnp.bfloat16)
    low = (square - high.astype(jnp.float32)).astype(jnp.bfloat16)
    spread_out = jnp.dot(
        jnp.concatenate([high, low], 1), share, preferred_element_type=jnp.float32
    )
    return (centred * lax.rsqrt(spread_out + epsilon)).astype(jnp.bfloat16)


def norm_kernel(values, normed):
    normed[...] = matmul_norm(values[...])


def norm_rows(values, block):
    spec = pl.BlockSpec((block, values.shape[1]), lambda step: (step, 0))
    return pl.pallas_call(
        norm_kernel,
        out_shape=jax.ShapeDtypeStruct(values.shape, jnp.bfloat16),
        grid=(values.shape[0] // block,),
        in_specs=[spec],
        out_specs=spec,
        name="norm_pair",
    )(values)


def pair_kernel(pair, left, right, w_pairout, w_up, w_down, updated):
    block_rows, tile_cols, wide = pair.shape
    left_wide = left[...][:, None, :]
    right_wide = right[...].astype(jnp.float32)[None, :, :]
    lower = lax.broadcasted_iota(jnp.int32, pair.shape, 2) < wide // 2
    paired = jnp.where(lower, left_wide * right_wide, left_wide - right_wide)
    paired = paired.astype(jnp.bfloat16).reshape(block_rows * tile_cols, wide)
    flat = pair[...].reshape(block_rows * tile_cols, wide).astype(jnp.float32)
    mid = flat + jnp.dot(paired, w_pairout[...], preferred_element_type=jnp.float32)
    mid = mid.astype(jnp.bfloat16)
    normed = matmul_norm(mid)
    hidden = jnp.dot(normed, w_up[...], preferred_element_type=jnp.float32)
    hidden = jnp.maximum(hidden, 0.0).astype(jnp.bfloat16)
    out = mid.astype(jnp.float32) + jnp.dot(
        hidden, w_down[...], preferred_element_type=jnp.float32
    )
    updated[...] = out.astype(jnp.bfloat16).reshape(pair.shape)


def update_pair(pair, left, right, w_pairout, w_up, w_down):
    tile_rows, tile_cols, wide = pair.shape
    block = math.gcd(tile_rows, max(8, 1024 // tile_cols))
    tile = pl.BlockSpec((block, tile_cols, wide), lambda step: (step, 0, 0))

    def whole(array):
        return pl.BlockSpec(array.shape, lambda step: (0, 0))

    return pl.pallas_call(
        pair_kernel,
        out_shape=jax.ShapeDtypeStruct(pair.shape, jnp.bfloat16),
        grid=(tile_rows // block,),
        in_specs=[
            tile,
            pl.BlockSpec((block, wide), lambda step: (step, 0)),
            whole(right),
            whole(w_pairout),
            whole(w_up),
            whole(w_down),
        ],
        out_specs=tile,
        name="update_pair",
    )(pair, left, right, w_pairout, w_up, w_down)


def layer_norm(values):
    values = values.astype(jnp.float32)
    centred = values - jnp.mean(values, -1, keepdims=True)
    return centred * lax.rsqrt(jnp.mean(centred * centred, -1, keepdims=True) + epsilon)


def per_device(
    row_size, col_size,
    single, pair, residue_mask, w_bias, w_project, w_out, w_factors, w_pairout, w_up, w_down
):
    tile_rows = pair.shape[0]
    tile_cols = pair.shape[1]
    normed_pair = norm_rows(
        pair.reshape(tile_rows * tile_cols, pair.shape[2]), math.gcd(tile_rows * tile_cols, 1024)
    ).reshape(pair.shape)
    bias_local = jnp.einsum(
        "rcp,ph->hrc", normed_pair, w_bias, preferred_element_type=jnp.float32
    ).astype(jnp.bfloat16)
    normed_single = layer_norm(single).astype(jnp.bfloat16)
    projected = jnp.einsum(
        "rs,fsc->frc", normed_single, w_project, preferred_element_type=jnp.float32
    )
    query_rows = projected[0].astype(jnp.bfloat16)
    key_local = projected[1].astype(jnp.bfloat16)
    value_local = projected[2].astype(jnp.bfloat16)
    gate_values = jax.nn.sigmoid(projected[3])
    bias_heads = lax.all_to_all(bias_local, "cols", split_axis=0, concat_axis=2, tiled=True)
    both = gather(jnp.concatenate([key_local, value_local], 1), "rows", row_size, 1)
    both = both.reshape(row_size * tile_rows, both.shape[2])
    key_rows, value_rows = both[:, : key_local.shape[1]], both[:, key_local.shape[1] :]
    heads_here = bias_heads.shape[0]
    head_width = query_rows.shape[1] // heads_here
    residues = key_rows.shape[0]
    query_split = query_rows.reshape(tile_rows, heads_here, head_width)
    key_split = key_rows.reshape(residues, heads_here, head_width)
    value_split = value_rows.reshape(residues, heads_here, head_width)
    score_scale = 1.0 / math.sqrt(head_width)
    scores = jnp.einsum(
        "rhd,lhd->hrl", query_split, key_split, preferred_element_type=jnp.float32
    ) * score_scale + bias_heads.astype(jnp.float32)
    key_valid = (residue_mask > 0)[None, None, :]
    scores = jnp.where(key_valid, scores, -jnp.inf)
    weights = jax.nn.softmax(scores, axis=-1).astype(jnp.bfloat16)
    attended = jnp.einsum("hrl,lhd->rhd", weights, value_split, preferred_element_type=jnp.float32)
    attended = attended.reshape(tile_rows, heads_here * head_width)
    mixed = (attended * gate_values).astype(jnp.bfloat16)
    single_out, left, right = update_single(
        mixed, single, w_out, w_factors, row_size, col_size, tile_cols
    )
    return (single_out, update_pair(pair, left, right, w_pairout, w_up, w_down))


LANES = 128
excluded = -1e30
update_block = 32


def lane_iota(shape):
    return lax.broadcasted_iota(jnp.int32, shape, len(shape) - 1)


def centre_matrix(wide, copies):
    size = wide * copies
    row = lax.broadcasted_iota(jnp.int32, (size, size), 0)
    col = lax.broadcasted_iota(jnp.int32, (size, size), 1)
    share = jnp.where(row // wide == col // wide, 1.0 / wide, 0.0)
    return (jnp.where(row == col, 1.0, 0.0) - share).astype(jnp.bfloat16)


def norm_centred(values, centre, copies):
    centred = jnp.dot(values, centre, preferred_element_type=jnp.float32)
    wide = values.shape[1] // copies
    parts = []
    for index in range(copies):
        part = centred[:, index * wide : (index + 1) * wide]
        square = jnp.sum(part * part, axis=1, keepdims=True) * (1.0 / wide)
        parts.append((part * lax.rsqrt(square + epsilon)).astype(jnp.bfloat16))
    return parts


def exchange(index, turn, size):
    total, bit = 0, 1
    while bit < size:
        total = total + lax.rem(index // bit + turn // bit, 2) * bit
        bit *= 2
    return total


def twice(weights):
    zeros = jnp.zeros_like(weights)
    upper = jnp.concatenate([weights, zeros], axis=1)
    return jnp.concatenate([upper, jnp.concatenate([zeros, weights], axis=1)], axis=0)


def update_rows(pair_of, left_of, right, rows, centre, w_pairout, w_up, w_down):
    tile_cols, wide = right.shape
    lower = lane_iota((rows, tile_cols, wide)) < wide // 2

    def paired(index):
        left_wide = left_of(index)[:, None, :]
        right_wide = right[None, :, :]
        chosen = jnp.where(lower, left_wide * right_wide, left_wide - right_wide)
        return chosen.astype(jnp.bfloat16).reshape(rows * tile_cols, wide)

    flat = [pair_of(index).reshape(rows * tile_cols, wide) for index in range(2)]
    mid = jnp.concatenate(flat, axis=1).astype(jnp.float32) + jnp.dot(
        jnp.concatenate([paired(0), paired(1)], axis=1),
        w_pairout,
        preferred_element_type=jnp.float32,
    )
    mid = mid.astype(jnp.bfloat16)
    normed = jnp.concatenate(norm_centred(mid, centre, 2), axis=0)
    mid = jnp.concatenate([mid[:, :wide], mid[:, wide:]], axis=0)
    hidden = jnp.dot(normed, w_up, preferred_element_type=jnp.float32)
    hidden = jnp.maximum(hidden, 0.0).astype(jnp.bfloat16)
    out = mid.astype(jnp.float32) + jnp.dot(hidden, w_down, preferred_element_type=jnp.float32)
    return out.astype(jnp.bfloat16).reshape(2 * rows, tile_cols, wide)


def attend_kernel(
    row_size, col_size, heads, tile_cols, stride,
    single, pair, mask, w_bias, w_project, w_out, w_factors, w_pairout, w_up, w_down,
    single_out, pair_out,
    single_v, pair_v, mask_v, bias_w, project_v, out_v, factors_v, own_single,
    kv_send, kv_recv, q_recv, gate_send, gate_recv, bias_v, o_send, o_recv,
    st_send, st_recv, left_send, right_send, left_recv, right_recv, left_out, right_out, so_send, bias_t, st_rows, centre_v, spread_v,
    pairout_v, twice_v, up_v, down_v,
    load_sems, pair_sems, col_send, col_recv, fan_send, fan_recv,
    plane_sent, plane_came, kv_sent, kv_came, kv_relayed, q_sent, q_came, o_sent, o_came,
):
    me_row = lax.axis_index("rows")
    me_col = lax.axis_index("cols")
    total = row_size * col_size
    halves, depth, _, wide = pair.shape
    tile_rows, width = single.shape
    group = w_project.shape[2]
    rows_each = depth // col_size
    heads_here = heads // col_size
    head_width = group // heads_here
    chunk = depth // pair_sems.shape[0]
    loads = [
        pltpu.make_async_copy(source, target, load_sems.at[index])
        for index, (source, target) in enumerate(
            [(single, single_v)]
            + [(w_project.at[part], project_v.at[part]) for part in range(4)]
            + [(w_bias, bias_w), (mask, mask_v)]
            + [
                (single.at[pl.ds(half * depth + me_col * rows_each, rows_each)], own_single.at[half])
                for half in range(halves)
            ]
            + [(w_out, out_v), (w_factors, factors_v)]
            + [(w_pairout, pairout_v), (w_up, up_v), (w_down, down_v)]
        )
    ]
    for copy in loads[:7]:
        copy.start()
    barrier = pltpu.get_barrier_semaphore()
    me = me_row * col_size + me_col
    for step in range(1, total):
        to = lax.rem(me + step, total)
        pl.semaphore_signal(
            barrier,
            inc=1,
            device_id={"rows": to // col_size, "cols": lax.rem(to, col_size)},
            device_id_type=pl.DeviceIdType.MESH,
        )

    def pair_load(step):
        part = pl.ds(step * chunk, chunk)
        return pltpu.make_async_copy(pair.at[:, part], pair_v.at[:, part], pair_sems.at[step])

    for step in range(depth // chunk):
        pair_load(step).start()
    for copy in loads[7:]:
        copy.start()

    centre_v[...] = centre_matrix(wide, halves)

    def to_cols(kind, source_of, target):
        copies = []
        for step in range(1, col_size):
            to = lax.rem(me_col + step, col_size)
            copy = pltpu.make_async_remote_copy(
                src_ref=source_of(to),
                dst_ref=target,
                send_sem=col_send.at[kind, step - 1],
                recv_sem=col_recv.at[kind, step - 1],
                device_id={"cols": to},
                device_id_type=pl.DeviceIdType.MESH,
            )
            copy.start()
            copies.append(copy)
        return copies

    owner = me_col // halves
    mine = owner == me_row
    half_mine = lax.rem(me_col, halves)

    def fan_copies(kind, source_of, target):
        copies = []
        for step in range(row_size):
            for half in range(halves):
                to = halves * me_row + half
                copy = pltpu.make_async_remote_copy(
                    src_ref=source_of(half),
                    dst_ref=target.at[me_col],
                    send_sem=fan_send.at[kind, step * halves + half],
                    recv_sem=fan_recv.at[kind, me_col],
                    device_id={"rows": lax.rem(me_row + step, row_size), "cols": to},
                    device_id_type=pl.DeviceIdType.MESH,
                )
                copies.append((copy, step, to))
        return copies

    def on_some(copies, act):
        for copy, condition in copies:
            if condition is None:
                act(copy)
            else:
                pl.when(condition)(functools.partial(act, copy))

    kind_mine = lax.rem(me_row, 2)
    me_plane = me_row // 2
    row_mate = me_row + 1 - 2 * kind_mine
    col_mate = me_col + 1 - 2 * lax.rem(me_col, 2)

    def relay_keys(part, kind, slot):
        return pltpu.make_async_remote_copy(
            src_ref=kv_recv.at[part, kind],
            dst_ref=kv_recv.at[part, kind],
            send_sem=kv_relayed.at[slot],
            recv_sem=kv_came.at[kind, part],
            device_id={"rows": row_mate},
            device_id_type=pl.DeviceIdType.MESH,
        )

    def send_query(part, to, slot):
        return pltpu.make_async_remote_copy(
            src_ref=q_recv.at[part],
            dst_ref=q_recv.at[part],
            send_sem=q_sent.at[slot],
            recv_sem=q_came.at[part],
            device_id={"cols": to},
            device_id_type=pl.DeviceIdType.MESH,
        )

    def on_fan(copies, act):
        for copy, step, to in copies:
            if step:
                act(copy)
            else:
                pl.when(to != me_col)(functools.partial(act, copy))

    def fan_wait(kind, source_of, target):
        for part in range(col_size):
            copy = pltpu.make_async_remote_copy(
                src_ref=source_of(0),
                dst_ref=target.at[part],
                send_sem=fan_send.at[kind, 0],
                recv_sem=fan_recv.at[kind, part],
                device_id={"rows": lax.rem(me_row + 1, row_size)},
                device_id_type=pl.DeviceIdType.MESH,
            )
            pl.when(jnp.logical_not(jnp.logical_and(mine, part == me_col)))(copy.wait_recv)

    loads[0].wait()
    normed = layer_norm(single_v[...]).astype(jnp.bfloat16)
    def project(*kinds):
        weights = [project_v[kind] for kind in kinds]
        return jnp.dot(
            normed, jnp.concatenate(weights, axis=1), preferred_element_type=jnp.float32
        )

    loads[1].wait()
    q_recv[me_col] = project(0).astype(jnp.bfloat16)
    pl.semaphore_wait(barrier, total - 1)
    parts, _, _, part_width = o_send.shape
    each = part_width // group
    col_side = lax.rem(me_col, each)

    def turn_step(turn):
        return exchange(me_col // each, turn, parts)

    peers = [turn_step(turn) * each + col_side for turn in range(1, parts)]
    q_copies = [send_query(me_col, to, slot) for slot, to in enumerate(peers)]
    q_copies.append(send_query(me_col, col_mate, len(peers)))
    for copy in q_copies:
        copy.start()
    loads[2].wait()
    loads[3].wait()
    key_value = project(1, 2).astype(jnp.bfloat16)
    for half in range(halves):
        for kind in range(2):
            kv_send[me_plane, half, kind] = key_value[
                half * tile_cols : (half + 1) * tile_cols, kind * group : (kind + 1) * group
            ]
    planes = row_size // 2
    plane_copies = []
    for step in range(1, planes):
        plane = lax.rem(me_plane + step, planes)
        copy = pltpu.make_async_remote_copy(
            src_ref=kv_send.at[me_plane],
            dst_ref=kv_send.at[me_plane],
            send_sem=plane_sent.at[step - 1],
            recv_sem=plane_came.at[step - 1],
            device_id={"rows": 2 * plane + kind_mine},
            device_id_type=pl.DeviceIdType.MESH,
        )
        copy.start()
        plane_copies.append(copy)
    kv_copies = []

    def send_keys(step):
        plane = lax.rem(me_plane + planes - step, planes)
        for half in range(halves):
            for kind in range(2):
                to = halves * (2 * plane + kind_mine) + half
                row = 2 * me_plane + kind
                copy = pltpu.make_async_remote_copy(
                    src_ref=kv_send.at[plane, half, kind],
                    dst_ref=kv_recv.at[me_col, kind],
                    send_sem=kv_sent.at[(step * 2 + kind) * halves + half],
                    recv_sem=kv_came.at[kind, me_col],
                    device_id={"rows": row, "cols": to},
                    device_id_type=pl.DeviceIdType.MESH,
                )
                here = jnp.logical_and(row == me_row, to == me_col)
                kv_copies.append((copy, jnp.logical_not(here)))
        on_some(kv_copies[-2 * halves :], lambda copy: copy.start())

    send_keys(0)
    loads[4].wait()
    gate_send[...] = jax.nn.sigmoid(project(3)).astype(jnp.bfloat16).reshape(gate_send.shape)

    def own_rows(to):
        return pl.ds(pl.multiple_of(to * rows_each, rows_each), rows_each)

    loads[5].wait()
    loads[6].wait()

    def relay_query(part):
        return send_query(part, col_mate, col_size // 2 + part // each)

    def bias_step(step, _):
        pair_load(step).wait()
        parts = [
            pair_v[half, pl.ds(step * chunk, chunk)].reshape(chunk * tile_cols, wide)
            for half in range(halves)
        ]
        parts = norm_centred(jnp.concatenate(parts, axis=1), centre_v[...], halves)
        parts = [part.reshape(chunk, 1, tile_cols, wide) for part in parts]
        normed_pair = jnp.concatenate(parts, axis=1).reshape(chunk * halves * tile_cols, wide)
        bias = lax.dot_general(
            bias_w[...], normed_pair, (((1,), (1,)), ((), ())), preferred_element_type=jnp.float32
        )
        bias = bias.astype(jnp.bfloat16).astype(jnp.float32)
        for part in range(chunk):
            bias_v[pl.ds(step * chunk + part, heads, stride=stride), :] = bias[
                :, part * LANES : (part + 1) * LANES
            ]
        return 0

    lax.fori_loop(0, depth // chunk, bias_step, 0)
    lane_row = lane_iota((2 * halves * heads, width))
    place = lax.broadcasted_iota(jnp.int32, (2 * halves * heads, width), 0)
    for half in range(halves):
        picked = jnp.where(place == half * heads + lane_row // head_width, 1.0, 0.0)
        spread_v[half, :LANES] = picked.astype(jnp.bfloat16)
        spread_v[half, LANES:] = picked.astype(jnp.bfloat16)

    for step in range(1, planes):
        plane_copies[step - 1].wait_recv()
        send_keys(step)
    own_key = lax.rem(owner, 2) == kind_mine

    @pl.when(own_key)
    def _():
        kv_recv[me_col, kind_mine] = kv_send[owner // 2, half_mine, kind_mine]

    def relay_keys_turn(turn):
        for index in range(each):
            part = turn_step(turn) * each + index
            copy = relay_keys(part, kind_mine, part)
            own = jnp.logical_and(own_key, part == me_col)
            pl.when(jnp.logical_not(own))(copy.wait_recv)
            copy.start()

    st_rows[...] = jnp.zeros_like(st_rows)

    def turn_bias(turn, _):
        for index in range(each * heads_here):
            head = turn_step(turn) * each * heads_here + index
            rows = bias_v[pl.ds(pl.multiple_of(head * stride, 8), depth), :].T
            bias_t[head] = jnp.concatenate([rows[:tile_cols], rows[tile_cols:]], axis=1)
        return 0

    lax.fori_loop(0, parts, turn_bias, 0)
    same_plane = owner // 2 == me_plane
    pl.when(same_plane)(functools.partial(relay_keys_turn, 0))
    relays = [relay_query(peer) for peer in peers]
    for copy in relays:
        copy.wait_recv()
        copy.start()
    pl.when(jnp.logical_not(same_plane))(functools.partial(relay_keys_turn, 0))
    relay_keys_turn(1)
    relays += [relay_keys(part, kind_mine, part) for part in range(col_size)]

    def gate_copy(shift):
        to = lax.rem(me_col + shift, col_size)
        return pltpu.make_async_remote_copy(
            src_ref=gate_send.at[:, to],
            dst_ref=gate_recv.at[me_col],
            send_sem=col_send.at[1, shift - 1],
            recv_sem=col_recv.at[1, shift - 1],
            device_id={"cols": to},
            device_id_type=pl.DeviceIdType.MESH,
        )

    gate_copies = [gate_copy(shift) for shift in range(1, col_size)]
    for copy in gate_copies:
        copy.start()
    gate_recv[me_col] = gate_send[:, me_col]

    length = jnp.sum(jnp.sum(mask_v[...], axis=1, keepdims=True), axis=0, keepdims=True)
    key_place = lax.broadcasted_iota(jnp.int32, (tile_cols, tile_rows), 0)
    valid = me_col * tile_cols + key_place < length
    head_of = lane_iota((tile_cols, group)) // head_width
    head_masks = [
        jnp.where(head_of == head, 1.0, 0.0).astype(jnp.bfloat16) for head in range(heads_here)
    ]
    scale = 1.0 / math.sqrt(head_width)

    def attend_part(part):
        key, value = kv_recv[part, 0], kv_recv[part, 1]
        raw = lax.dot_general(
            jnp.concatenate([key * mask for mask in head_masks], axis=0),
            q_recv[part],
            (((1,), (1,)), ((), ())),
            preferred_element_type=jnp.float32,
        )
        weights = []
        for head in range(heads_here):
            index = part * heads_here + head
            scores = raw[head * tile_cols : (head + 1) * tile_cols] * scale + bias_t[index]
            scores = jnp.where(valid, scores, excluded)
            top = jnp.max(scores, axis=0, keepdims=True)
            weight = jnp.exp(scores - top)
            st_rows[pl.ds(index, 1), :] = top
            st_rows[pl.ds(halves * heads + index, 1), :] = jnp.sum(weight, axis=0, keepdims=True)
            weights.append(weight.astype(jnp.bfloat16))
        mixed = lax.dot_general(
            jnp.concatenate(weights, axis=0),
            jnp.concatenate([value * mask for mask in head_masks], axis=0),
            (((0,), (0,)), ((), ())),
            preferred_element_type=jnp.float32,
        )
        pieces = [
            mixed[half * depth : (half + 1) * depth].reshape(col_size, rows_each, group)
            for half in range(halves)
        ]
        return jnp.concatenate(pieces, axis=1).astype(jnp.bfloat16)

    def o_copy(step, shift):
        to = lax.rem(me_col + shift, col_size)
        return pltpu.make_async_remote_copy(
            src_ref=o_send.at[step, to],
            dst_ref=o_recv.at[step, me_col],
            send_sem=o_sent.at[step, shift - 1],
            recv_sem=o_came.at[step, shift - 1],
            device_id={"cols": to},
            device_id_type=pl.DeviceIdType.MESH,
        )

    def st_copy(shift):
        to = lax.rem(me_col + shift, col_size)
        return pltpu.make_async_remote_copy(
            src_ref=st_send.at[own_rows(to)],
            dst_ref=st_recv.at[me_col],
            send_sem=col_send.at[2, shift - 1],
            recv_sem=col_recv.at[2, shift - 1],
            device_id={"cols": to},
            device_id_type=pl.DeviceIdType.MESH,
        )

    def attend_step(turn, _):
        step = turn_step(turn)
        far = step * each + 1 - col_side
        relay_query(far).wait_recv()
        for index in range(each):
            part = step * each + index
            relay_keys(part, 1 - kind_mine, part).wait_recv()
        for index in range(each):
            o_send[step, :, :, index * group : (index + 1) * group] = attend_part(
                step * each + index
            )

        @pl.when(turn == parts - 1)
        def _():
            stats = st_rows[...].T
            st_send[...] = stats[:depth] + pltpu.roll(stats[depth:], heads, axis=1)
            for shift in range(1, col_size):
                st_copy(shift).start()

        for shift in range(1, col_size):
            o_copy(step, shift).start()
        pl.when(turn + 2 < parts)(functools.partial(relay_keys_turn, turn + 2))
        return 0

    lax.fori_loop(0, parts, attend_step, 0)
    st_copies = [st_copy(shift) for shift in range(1, col_size)]
    st_recv[me_col] = st_send[own_rows(me_col)]
    for step in range(parts):
        o_recv[step, me_col] = o_send[step, me_col]
    o_copies = [o_copy(step, shift) for step in range(parts) for shift in range(1, col_size)]
    for copy in gate_copies + st_copies:
        copy.wait_recv()
    stats = st_recv[...]
    lane = lane_iota(stats.shape)
    top = jnp.max(stats, axis=0, keepdims=True)
    factor = jnp.exp(stats - top)
    sums = jnp.sum(factor * pltpu.roll(stats, halves * heads, axis=2), axis=0, keepdims=True)
    factor = jnp.where(lane < halves * heads, factor / sums, 0.0)
    factor = factor.reshape(col_size * rows_each, LANES)
    high = factor.astype(jnp.bfloat16)
    rest = (factor - high.astype(jnp.float32)).astype(jnp.bfloat16)
    factor = jnp.concatenate([high, rest], axis=1)
    scales = [
        jnp.dot(factor, spread_v[half], preferred_element_type=jnp.float32) for half in range(halves)
    ]
    gate = jnp.concatenate(
        [
            gate_recv[part].astype(jnp.float32).reshape(halves * rows_each, group)
            for part in range(col_size)
        ],
        axis=1,
    )
    for copy in o_copies:
        copy.wait_recv()
    attended = jnp.zeros((halves * rows_each, width), jnp.float32)
    for part in range(col_size):
        rows = slice(part * rows_each, (part + 1) * rows_each)
        part_scale = jnp.concatenate([scales[half][rows] for half in range(halves)], axis=0)
        whole = jnp.concatenate([o_recv[step, part] for step in range(parts)], axis=1)
        attended = attended + part_scale * whole.astype(jnp.float32)
    mixed = (attended * gate).astype(jnp.bfloat16)
    for copy in loads[7:]:
        copy.wait()
    added = jnp.dot(mixed, out_v[...], preferred_element_type=jnp.float32)
    own = own_single[...].astype(jnp.float32).reshape(halves * rows_each, width)
    updated = (own + added).astype(jnp.bfloat16)
    so_send[...] = updated.astype(jnp.float32).reshape(halves, rows_each, width).astype(jnp.bfloat16)
    factors = jnp.dot(
        layer_norm(updated).astype(jnp.bfloat16),
        factors_v[...],
        preferred_element_type=jnp.float32,
    )
    factors = factors.astype(jnp.bfloat16).astype(jnp.float32)
    first, second = factors[:rows_each], factors[rows_each:]
    shift = factors.shape[1] // 2
    low = lane_iota(first.shape) < shift
    left = jnp.where(low, first, pltpu.roll(second, shift, axis=1))
    right = jnp.where(low, pltpu.roll(first, shift, axis=1), second)
    left_send[...] = left.astype(jnp.bfloat16)
    right_send[...] = right.astype(jnp.bfloat16)
    right_copies = fan_copies(1, lambda half: right_send, right_recv)
    on_fan(right_copies, lambda copy: copy.start())
    left_copies = to_cols(4, lambda to: left_send, left_recv.at[me_col])
    left_recv[me_col] = left.astype(jnp.bfloat16)

    @pl.when(mine)
    def _():
        right_recv[me_col] = right_send[...]

    fan_wait(1, lambda half: right_send, right_recv)
    for copy in left_copies:
        copy.wait_recv()
    so_copies = to_cols(5, lambda to: so_send, single_out.at[:, me_col])
    single_out[:, me_col] = so_send[...]
    left = left_recv[...].astype(jnp.float32).reshape(depth, LANES)
    turned = pltpu.roll(left, shift, axis=1)
    low = lane_iota(left.shape) < shift
    left_out[:depth] = jnp.where(low, left, turned)
    left_out[depth:] = jnp.where(low, turned, left)
    right = right_recv[...].astype(jnp.float32).reshape(tile_cols, LANES)
    turned = pltpu.roll(right, shift, axis=1)
    right_out[...] = jnp.where(lane_iota(right.shape) // shift == half_mine, right, turned)

    twice_v[...] = twice(pairout_v[...])
    block = update_block
    def update_step(step, _):
        first = step * 2 * block
        half = first // depth
        pair_out[pl.ds(first, 2 * block)] = update_rows(
            lambda index: pair_v[half, pl.ds(first - half * depth + index * block, block)],
            lambda index: left_out[pl.ds(pl.multiple_of(first + index * block, 8), block)],
            right_out[...],
            block,
            centre_v[...],
            twice_v[...],
            up_v[...],
            down_v[...],
        )
        return 0

    lax.fori_loop(0, tile_rows // (2 * block), update_step, 0)

    for copies in (q_copies, relays, plane_copies, gate_copies, st_copies, o_copies, left_copies, so_copies):
        for copy in copies:
            copy.wait_send()
    on_some(kv_copies, lambda copy: copy.wait_send())
    on_fan(right_copies, lambda copy: copy.wait_send())
    for copy in so_copies:
        copy.wait_recv()


def finish_kernel(single, pair, single_out, pair_out, sems):
    copies = [pltpu.make_async_copy(single, single_out, sems.at[0])]
    steps = sems.shape[0] - 1
    rows = pair.shape[0] // steps
    for step in range(steps):
        part = pl.ds(step * rows, rows)
        copies.append(
            pltpu.make_async_copy(pair.at[part], pair_out.at[part], sems.at[1 + step])
        )
    for copy in copies:
        copy.start()
    for copy in copies:
        copy.wait()


def finish(single, pair):
    return pl.pallas_call(
        finish_kernel,
        out_shape=tuple(jax.ShapeDtypeStruct(array.shape, array.dtype) for array in (single, pair)),
        in_specs=[pl.BlockSpec(memory_space=pltpu.VMEM)] * 2,
        out_specs=[pl.BlockSpec(memory_space=pl.ANY)] * 2,
        scratch_shapes=[pltpu.SemaphoreType.DMA((9,))],
        compiler_params=pltpu.CompilerParams(vmem_limit_bytes=8 * 1024 * 1024),
        name="finish",
    )(single, pair)


def attend(
    single, pair, mask, w_bias, w_project, w_out, w_factors, w_pairout, w_up, w_down,
    row_size, col_size,
):
    halves, depth, tile_cols, wide = pair.shape
    tile_rows, width = single.shape
    heads = w_bias.shape[1]
    rows_each = depth // col_size
    group = w_project.shape[2]
    steps = depth // 16
    parts = col_size // 2
    stride = depth + 8
    any_spec = pl.BlockSpec(memory_space=pltpu.HBM)
    vmem_spec = pl.BlockSpec(memory_space=pltpu.VMEM)
    bf16, f32 = jnp.bfloat16, jnp.float32
    single_out, pair_out = pl.pallas_call(
        functools.partial(attend_kernel, row_size, col_size, heads, tile_cols, stride),
        out_shape=(
            pltpu.VMEM((halves, col_size, rows_each, width), bf16),
            pltpu.VMEM((tile_rows, tile_cols, wide), bf16),
        ),
        in_specs=[any_spec] * 10,
        out_specs=[vmem_spec] * 2,
        scratch_shapes=[
            pltpu.VMEM((tile_rows, width), bf16),
            pltpu.VMEM((halves, depth, tile_cols, wide), bf16),
            pltpu.VMEM((mask.shape[0] // LANES, LANES), jnp.int32),
            pltpu.VMEM((heads, wide), bf16),
            pltpu.VMEM(w_project.shape, bf16),
            pltpu.VMEM(w_out.shape, bf16),
            pltpu.VMEM(w_factors.shape, bf16),
            pltpu.VMEM((halves, rows_each, width), bf16),
            pltpu.VMEM((row_size // 2, halves, 2, tile_cols, group), bf16),
            pltpu.VMEM((col_size, 2, tile_cols, group), bf16),
            pltpu.VMEM((col_size, tile_rows, group), bf16),
            pltpu.VMEM((halves, col_size, rows_each, group), bf16),
            pltpu.VMEM((col_size, halves, rows_each, group), bf16),
            pltpu.VMEM((heads * stride, LANES), f32),
            pltpu.VMEM((parts, col_size, halves * rows_each, width // parts), bf16),
            pltpu.VMEM((parts, col_size, halves * rows_each, width // parts), bf16),
            pltpu.VMEM((depth, LANES), f32),
            pltpu.VMEM((col_size, rows_each, LANES), f32),
            pltpu.VMEM((rows_each, LANES), bf16),
            pltpu.VMEM((rows_each, LANES), bf16),
            pltpu.VMEM((col_size, rows_each, LANES), bf16),
            pltpu.VMEM((col_size, rows_each, LANES), bf16),
            pltpu.VMEM((tile_rows, wide), f32),
            pltpu.VMEM((tile_cols, wide), f32),
            pltpu.VMEM((halves, rows_each, width), bf16),
            pltpu.VMEM((heads, tile_cols, tile_rows), f32),
            pltpu.VMEM((4 * heads, tile_rows), f32),
            pltpu.VMEM((halves * wide, halves * wide), bf16),
            pltpu.VMEM((halves, 2 * LANES, width), bf16),
            pltpu.VMEM(w_pairout.shape, bf16),
            pltpu.VMEM((2 * wide, 2 * wide), bf16),
            pltpu.VMEM(w_up.shape, bf16),
            pltpu.VMEM(w_down.shape, bf16),
            pltpu.SemaphoreType.DMA((12 + halves,)),
            pltpu.SemaphoreType.DMA((steps,)),
            pltpu.SemaphoreType.DMA((6, col_size - 1)),
            pltpu.SemaphoreType.DMA((6, col_size - 1)),
            pltpu.SemaphoreType.DMA((2, row_size * halves)),
            pltpu.SemaphoreType.DMA((2, col_size)),
            pltpu.SemaphoreType.DMA((row_size // 2 - 1,)),
            pltpu.SemaphoreType.DMA((row_size // 2 - 1,)),
            pltpu.SemaphoreType.DMA((row_size * halves,)),
            pltpu.SemaphoreType.DMA((2, col_size)),
            pltpu.SemaphoreType.DMA((col_size,)),
            pltpu.SemaphoreType.DMA((2 * col_size,)),
            pltpu.SemaphoreType.DMA((col_size,)),
            pltpu.SemaphoreType.DMA((parts, col_size - 1)),
            pltpu.SemaphoreType.DMA((parts, col_size - 1)),
        ],
        compiler_params=pltpu.CompilerParams(
            collective_id=3, has_side_effects=True, vmem_limit_bytes=40 * 1024 * 1024
        ),
        name="attend",
    )(
        *(
            pltpu.with_memory_space_constraint(array, pltpu.HBM)
            for array in (
                single,
                pair,
                mask.reshape(mask.shape[0] // LANES, LANES),
                w_bias.T,
                w_project,
                w_out,
                w_factors,
                w_pairout,
                w_up,
                w_down,
            )
        )
    )
    single_out, pair_out = finish(single_out, pair_out)
    return single_out.reshape(tile_rows, width), pair_out


def fits(row_size, col_size, single, pair, mask, w_bias, w_project, w_factors):
    tile_rows, tile_cols, wide = pair.shape
    heads = w_bias.shape[1]
    return (
        tile_rows == 2 * tile_cols
        and 2 * tile_cols == LANES
        and wide == LANES
        and w_factors.shape[1] == LANES
        and w_project.shape[2] == LANES
        and 4 * heads == LANES
        and heads % (2 * col_size) == 0
        and tile_cols % (8 * col_size) == 0
        and col_size == 2 * row_size
        and row_size % 2 == 0
        and col_size & (col_size - 1) == 0
        and tile_cols % (2 * update_block) == 0
        and mask.shape[0] % LANES == 0
    )


def per_device_keys(
    row_size, col_size,
    single, pair, residue_mask, w_bias, w_project, w_out, w_factors, w_pairout, w_up, w_down
):
    shape = pair.shape
    return attend(
        single, pair.reshape(2, shape[0] // 2, *shape[1:]), residue_mask,
        w_bias, w_project, w_out, w_factors, w_pairout, w_up, w_down, row_size, col_size,
    )


def dispatch(row_size, col_size, *arrays):
    single, pair, residue_mask, w_bias, w_project, w_out, w_factors = arrays[:7]
    if fits(row_size, col_size, single, pair, residue_mask, w_bias, w_project, w_factors):
        return per_device_keys(row_size, col_size, *arrays)
    return per_device(row_size, col_size, *arrays)


def solution(mesh):
    return jax.shard_map(
        functools.partial(dispatch, mesh.shape["rows"], mesh.shape["cols"]),
        mesh=mesh,
        in_specs=(
            P("rows", None),
            P("rows", "cols", None),
            P(),
            P(),
            P(None, None, "cols"),
            P(),
            P(),
            P(),
            P(),
            P(),
        ),
        out_specs=(P("rows", None), P("rows", "cols", None)),
        check_vma=False,
    )
```

```python
import functools
import math

import jax
import jax.numpy as jnp
from jax import lax
from jax.experimental import pallas as pl
from jax.experimental.pallas import tpu as pltpu
from jax.sharding import PartitionSpec as P

epsilon = 1e-05


def enter(axes):
    barrier = pltpu.get_barrier_semaphore()
    total = 0
    for axis, size in axes:
        me = lax.axis_index(axis)
        for step in range(1, size):
            pl.semaphore_signal(
                barrier,
                inc=1,
                device_id={axis: lax.rem(me + step, size)},
                device_id_type=pl.DeviceIdType.MESH,
            )
        total += size - 1
    pl.semaphore_wait(barrier, total)


def spread(axis, size, source, landing, send_sems, recv_sems):
    me = lax.axis_index(axis)
    copies = []
    for step in range(1, size):
        copy = pltpu.make_async_remote_copy(
            src_ref=source,
            dst_ref=landing.at[me],
            send_sem=send_sems.at[step - 1],
            recv_sem=recv_sems.at[step - 1],
            device_id={axis: lax.rem(me + step, size)},
            device_id_type=pl.DeviceIdType.MESH,
        )
        copy.start()
        copies.append(copy)
    return copies


def gather_kernel(axis, size, source, gathered, send_sems, recv_sems, own_sem):
    enter([(axis, size)])
    copies = spread(axis, size, source, gathered, send_sems, recv_sems)
    own = pltpu.make_async_copy(source, gathered.at[lax.axis_index(axis)], own_sem)
    own.start()
    own.wait()
    for copy in copies:
        copy.wait()


def gather(values, axis, size, collective_id):
    return pl.pallas_call(
        functools.partial(gather_kernel, axis, size),
        out_shape=jax.ShapeDtypeStruct((size, *values.shape), values.dtype),
        in_specs=[pl.BlockSpec(memory_space=pltpu.VMEM)],
        out_specs=pl.BlockSpec(memory_space=pltpu.VMEM),
        scratch_shapes=[
            pltpu.SemaphoreType.DMA((size - 1,)),
            pltpu.SemaphoreType.DMA((size - 1,)),
            pltpu.SemaphoreType.DMA,
        ],
        compiler_params=pltpu.CompilerParams(collective_id=collective_id, has_side_effects=True),
        name="gather_" + axis,
    )(values)


def single_kernel(
    row_size, col_size, tile_cols,
    mixed, single, w_out, w_factors, single_out, left_out, right_out,
    gathered, factor_right, send_sems, recv_sems, row_send, row_recv, own_sem,
):
    enter([("cols", col_size), ("rows", row_size)])
    tile_rows, width = mixed.shape
    me_col = lax.axis_index("cols")
    me_row = lax.axis_index("rows")
    copies = spread("cols", col_size, mixed, gathered, send_sems, recv_sems)
    own = pltpu.make_async_copy(mixed, gathered.at[me_col], own_sem)
    own.start()
    own.wait()
    for copy in copies:
        copy.wait()
    whole = jnp.concatenate([gathered[part] for part in range(col_size)], axis=1)
    total = jnp.dot(whole, w_out[...], preferred_element_type=jnp.float32)
    updated = (single[...].astype(jnp.float32) + total).astype(jnp.bfloat16)
    single_out[...] = updated
    normed = layer_norm(updated).astype(jnp.bfloat16)
    factors = jnp.dot(normed, w_factors[...], preferred_element_type=jnp.float32)
    factors = factors.astype(jnp.bfloat16).astype(jnp.float32)
    half = factors.shape[1] // 2
    swapped = jnp.concatenate([factors[:, half:], factors[:, :half]], axis=1)
    lower = lax.broadcasted_iota(jnp.int32, factors.shape, 1) < half
    left_out[...] = jnp.where(lower, factors, swapped)
    factor_right[...] = jnp.where(lower, swapped, factors).astype(jnp.bfloat16)
    first = me_col * tile_cols
    owner = first // tile_rows
    offset = pl.multiple_of(first - owner * tile_rows, tile_cols)
    piece = factor_right.at[pl.ds(offset, tile_cols)]

    @pl.when(me_row == owner)
    def _():
        local = pltpu.make_async_copy(piece, right_out, own_sem)
        local.start()
        sends = []
        for step in range(1, row_size):
            send = pltpu.make_async_remote_copy(
                src_ref=piece,
                dst_ref=right_out,
                send_sem=row_send.at[step - 1],
                recv_sem=row_recv,
                device_id={"rows": lax.rem(me_row + step, row_size)},
                device_id_type=pl.DeviceIdType.MESH,
            )
            send.start()
            sends.append(send)
        local.wait()
        for send in sends:
            send.wait_send()

    @pl.when(me_row != owner)
    def _():
        pltpu.make_async_remote_copy(
            src_ref=piece,
            dst_ref=right_out,
            send_sem=row_send.at[0],
            recv_sem=row_recv,
            device_id={"rows": lax.rem(me_row + 1, row_size)},
            device_id_type=pl.DeviceIdType.MESH,
        ).wait_recv()


def update_single(mixed, single, w_out, w_factors, row_size, col_size, tile_cols):
    tile_rows, width = single.shape
    wide = w_factors.shape[1]
    return pl.pallas_call(
        functools.partial(single_kernel, row_size, col_size, tile_cols),
        out_shape=(
            jax.ShapeDtypeStruct((tile_rows, width), jnp.bfloat16),
            jax.ShapeDtypeStruct((tile_rows, wide), jnp.float32),
            jax.ShapeDtypeStruct((tile_cols, wide), jnp.bfloat16),
        ),
        in_specs=[pl.BlockSpec(memory_space=pltpu.VMEM)] * 4,
        out_specs=[pl.BlockSpec(memory_space=pltpu.VMEM)] * 3,
        scratch_shapes=[
            pltpu.VMEM((col_size, *mixed.shape), jnp.bfloat16),
            pltpu.VMEM((tile_rows, wide), jnp.bfloat16),
            pltpu.SemaphoreType.DMA((col_size - 1,)),
            pltpu.SemaphoreType.DMA((col_size - 1,)),
            pltpu.SemaphoreType.DMA((row_size - 1,)),
            pltpu.SemaphoreType.DMA,
            pltpu.SemaphoreType.DMA,
        ],
        compiler_params=pltpu.CompilerParams(collective_id=2, has_side_effects=True),
        name="update_single",
    )(mixed, single, w_out, w_factors)


def matmul_norm(values):
    wide = values.shape[1]
    share = jnp.full((2 * wide, wide), 1.0 / wide, jnp.bfloat16)
    mean = jnp.dot(values, share[:wide], preferred_element_type=jnp.float32)
    centred = values.astype(jnp.float32) - mean
    square = centred * centred
    high = square.astype(jnp.bfloat16)
    low = (square - high.astype(jnp.float32)).astype(jnp.bfloat16)
    spread_out = jnp.dot(
        jnp.concatenate([high, low], 1), share, preferred_element_type=jnp.float32
    )
    return (centred * lax.rsqrt(spread_out + epsilon)).astype(jnp.bfloat16)


def norm_kernel(values, normed):
    normed[...] = matmul_norm(values[...])


def norm_rows(values, block):
    spec = pl.BlockSpec((block, values.shape[1]), lambda step: (step, 0))
    return pl.pallas_call(
        norm_kernel,
        out_shape=jax.ShapeDtypeStruct(values.shape, jnp.bfloat16),
        grid=(values.shape[0] // block,),
        in_specs=[spec],
        out_specs=spec,
        name="norm_pair",
    )(values)


def pair_kernel(pair, left, right, w_pairout, w_up, w_down, updated):
    block_rows, tile_cols, wide = pair.shape
    left_wide = left[...][:, None, :]
    right_wide = right[...].astype(jnp.float32)[None, :, :]
    lower = lax.broadcasted_iota(jnp.int32, pair.shape, 2) < wide // 2
    paired = jnp.where(lower, left_wide * right_wide, left_wide - right_wide)
    paired = paired.astype(jnp.bfloat16).reshape(block_rows * tile_cols, wide)
    flat = pair[...].reshape(block_rows * tile_cols, wide).astype(jnp.float32)
    mid = flat + jnp.dot(paired, w_pairout[...], preferred_element_type=jnp.float32)
    mid = mid.astype(jnp.bfloat16)
    normed = matmul_norm(mid)
    hidden = jnp.dot(normed, w_up[...], preferred_element_type=jnp.float32)
    hidden = jnp.maximum(hidden, 0.0).astype(jnp.bfloat16)
    out = mid.astype(jnp.float32) + jnp.dot(
        hidden, w_down[...], preferred_element_type=jnp.float32
    )
    updated[...] = out.astype(jnp.bfloat16).reshape(pair.shape)


def update_pair(pair, left, right, w_pairout, w_up, w_down):
    tile_rows, tile_cols, wide = pair.shape
    block = math.gcd(tile_rows, max(8, 1024 // tile_cols))
    tile = pl.BlockSpec((block, tile_cols, wide), lambda step: (step, 0, 0))

    def whole(array):
        return pl.BlockSpec(array.shape, lambda step: (0, 0))

    return pl.pallas_call(
        pair_kernel,
        out_shape=jax.ShapeDtypeStruct(pair.shape, jnp.bfloat16),
        grid=(tile_rows // block,),
        in_specs=[
            tile,
            pl.BlockSpec((block, wide), lambda step: (step, 0)),
            whole(right),
            whole(w_pairout),
            whole(w_up),
            whole(w_down),
        ],
        out_specs=tile,
        name="update_pair",
    )(pair, left, right, w_pairout, w_up, w_down)


def layer_norm(values):
    values = values.astype(jnp.float32)
    centred = values - jnp.mean(values, -1, keepdims=True)
    return centred * lax.rsqrt(jnp.mean(centred * centred, -1, keepdims=True) + epsilon)


def per_device(
    row_size, col_size,
    single, pair, residue_mask, w_bias, w_project, w_out, w_factors, w_pairout, w_up, w_down
):
    tile_rows = pair.shape[0]
    tile_cols = pair.shape[1]
    normed_pair = norm_rows(
        pair.reshape(tile_rows * tile_cols, pair.shape[2]), math.gcd(tile_rows * tile_cols, 1024)
    ).reshape(pair.shape)
    bias_local = jnp.einsum(
        "rcp,ph->hrc", normed_pair, w_bias, preferred_element_type=jnp.float32
    ).astype(jnp.bfloat16)
    normed_single = layer_norm(single).astype(jnp.bfloat16)
    projected = jnp.einsum(
        "rs,fsc->frc", normed_single, w_project, preferred_element_type=jnp.float32
    )
    query_rows = projected[0].astype(jnp.bfloat16)
    key_local = projected[1].astype(jnp.bfloat16)
    value_local = projected[2].astype(jnp.bfloat16)
    gate_values = jax.nn.sigmoid(projected[3])
    bias_heads = lax.all_to_all(bias_local, "cols", split_axis=0, concat_axis=2, tiled=True)
    both = gather(jnp.concatenate([key_local, value_local], 1), "rows", row_size, 1)
    both = both.reshape(row_size * tile_rows, both.shape[2])
    key_rows, value_rows = both[:, : key_local.shape[1]], both[:, key_local.shape[1] :]
    heads_here = bias_heads.shape[0]
    head_width = query_rows.shape[1] // heads_here
    residues = key_rows.shape[0]
    query_split = query_rows.reshape(tile_rows, heads_here, head_width)
    key_split = key_rows.reshape(residues, heads_here, head_width)
    value_split = value_rows.reshape(residues, heads_here, head_width)
    score_scale = 1.0 / math.sqrt(head_width)
    scores = jnp.einsum(
        "rhd,lhd->hrl", query_split, key_split, preferred_element_type=jnp.float32
    ) * score_scale + bias_heads.astype(jnp.float32)
    key_valid = (residue_mask > 0)[None, None, :]
    scores = jnp.where(key_valid, scores, -jnp.inf)
    weights = jax.nn.softmax(scores, axis=-1).astype(jnp.bfloat16)
    attended = jnp.einsum("hrl,lhd->rhd", weights, value_split, preferred_element_type=jnp.float32)
    attended = attended.reshape(tile_rows, heads_here * head_width)
    mixed = (attended * gate_values).astype(jnp.bfloat16)
    single_out, left, right = update_single(
        mixed, single, w_out, w_factors, row_size, col_size, tile_cols
    )
    return (single_out, update_pair(pair, left, right, w_pairout, w_up, w_down))


LANES = 128
excluded = -1e30
update_block = 32


def lane_iota(shape):
    return lax.broadcasted_iota(jnp.int32, shape, len(shape) - 1)


def centre_matrix(wide, copies):
    size = wide * copies
    row = lax.broadcasted_iota(jnp.int32, (size, size), 0)
    col = lax.broadcasted_iota(jnp.int32, (size, size), 1)
    share = jnp.where(row // wide == col // wide, 1.0 / wide, 0.0)
    return (jnp.where(row == col, 1.0, 0.0) - share).astype(jnp.bfloat16)


def norm_centred(values, centre, copies):
    centred = jnp.dot(values, centre, preferred_element_type=jnp.float32)
    wide = values.shape[1] // copies
    parts = []
    for index in range(copies):
        part = centred[:, index * wide : (index + 1) * wide]
        square = jnp.sum(part * part, axis=1, keepdims=True) * (1.0 / wide)
        parts.append((part * lax.rsqrt(square + epsilon)).astype(jnp.bfloat16))
    return parts


def exchange(index, turn, size):
    total, bit = 0, 1
    while bit < size:
        total = total + lax.rem(index // bit + turn // bit, 2) * bit
        bit *= 2
    return total


def twice(weights):
    zeros = jnp.zeros_like(weights)
    upper = jnp.concatenate([weights, zeros], axis=1)
    return jnp.concatenate([upper, jnp.concatenate([zeros, weights], axis=1)], axis=0)


def update_rows(pair_of, left_of, right, rows, centre, w_pairout, w_up, w_down):
    tile_cols, wide = right.shape
    lower = lane_iota((rows, tile_cols, wide)) < wide // 2

    def paired(index):
        left_wide = left_of(index)[:, None, :]
        right_wide = right[None, :, :]
        chosen = jnp.where(lower, left_wide * right_wide, left_wide - right_wide)
        return chosen.astype(jnp.bfloat16).reshape(rows * tile_cols, wide)

    flat = [pair_of(index).reshape(rows * tile_cols, wide) for index in range(2)]
    mid = jnp.concatenate(flat, axis=1).astype(jnp.float32) + jnp.dot(
        jnp.concatenate([paired(0), paired(1)], axis=1),
        w_pairout,
        preferred_element_type=jnp.float32,
    )
    mid = mid.astype(jnp.bfloat16)
    normed = jnp.concatenate(norm_centred(mid, centre, 2), axis=0)
    mid = jnp.concatenate([mid[:, :wide], mid[:, wide:]], axis=0)
    hidden = jnp.dot(normed, w_up, preferred_element_type=jnp.float32)
    hidden = jnp.maximum(hidden, 0.0).astype(jnp.bfloat16)
    out = mid.astype(jnp.float32) + jnp.dot(hidden, w_down, preferred_element_type=jnp.float32)
    return out.astype(jnp.bfloat16).reshape(2 * rows, tile_cols, wide)


def attend_kernel(
    row_size, col_size, heads, tile_cols, stride,
    single, pair, mask, w_bias, w_project, w_out, w_factors, w_pairout, w_up, w_down,
    single_out, pair_out,
    single_v, pair_v, mask_v, bias_w, project_v, out_v, factors_v, own_single,
    kv_send, kv_recv, q_recv, gate_send, gate_recv, bias_v, o_send, o_recv,
    st_send, st_recv, left_send, right_send, left_recv, right_recv, left_out, right_out, so_send, bias_t, st_rows, centre_v, spread_v,
    pairout_v, twice_v, up_v, down_v,
    load_sems, pair_sems, col_send, col_recv, fan_send, fan_recv,
    plane_sent, plane_came, kv_sent, kv_came, kv_relayed, q_sent, q_came, o_sent, o_came,
):
    me_row = lax.axis_index("rows")
    me_col = lax.axis_index("cols")
    total = row_size * col_size
    halves, depth, _, wide = pair.shape
    tile_rows, width = single.shape
    group = w_project.shape[2]
    rows_each = depth // col_size
    heads_here = heads // col_size
    head_width = group // heads_here
    chunk = depth // pair_sems.shape[0]
    loads = [
        pltpu.make_async_copy(source, target, load_sems.at[index])
        for index, (source, target) in enumerate(
            [(single, single_v)]
            + [(w_project.at[part], project_v.at[part]) for part in range(4)]
            + [(w_bias, bias_w), (mask, mask_v)]
            + [
                (single.at[pl.ds(half * depth + me_col * rows_each, rows_each)], own_single.at[half])
                for half in range(halves)
            ]
            + [(w_out, out_v), (w_factors, factors_v)]
            + [(w_pairout, pairout_v), (w_up, up_v), (w_down, down_v)]
        )
    ]
    for copy in loads[:7]:
        copy.start()
    barrier = pltpu.get_barrier_semaphore()
    me = me_row * col_size + me_col
    for step in range(1, total):
        to = lax.rem(me + step, total)
        pl.semaphore_signal(
            barrier,
            inc=1,
            device_id={"rows": to // col_size, "cols": lax.rem(to, col_size)},
            device_id_type=pl.DeviceIdType.MESH,
        )

    def pair_load(step):
        part = pl.ds(step * chunk, chunk)
        return pltpu.make_async_copy(pair.at[:, part], pair_v.at[:, part], pair_sems.at[step])

    for step in range(depth // chunk):
        pair_load(step).start()
    for copy in loads[7:]:
        copy.start()

    centre_v[...] = centre_matrix(wide, halves)

    def to_cols(kind, source_of, target):
        copies = []
        for step in range(1, col_size):
            to = lax.rem(me_col + step, col_size)
            copy = pltpu.make_async_remote_copy(
                src_ref=source_of(to),
                dst_ref=target,
                send_sem=col_send.at[kind, step - 1],
                recv_sem=col_recv.at[kind, step - 1],
                device_id={"cols": to},
                device_id_type=pl.DeviceIdType.MESH,
            )
            copy.start()
            copies.append(copy)
        return copies

    owner = me_col // halves
    mine = owner == me_row
    half_mine = lax.rem(me_col, halves)

    def fan_copies(kind, source_of, target):
        copies = []
        for step in range(row_size):
            for half in range(halves):
                to = halves * me_row + half
                copy = pltpu.make_async_remote_copy(
                    src_ref=source_of(half),
                    dst_ref=target.at[me_col],
                    send_sem=fan_send.at[kind, step * halves + half],
                    recv_sem=fan_recv.at[kind, me_col],
                    device_id={"rows": lax.rem(me_row + step, row_size), "cols": to},
                    device_id_type=pl.DeviceIdType.MESH,
                )
                copies.append((copy, step, to))
        return copies

    def on_some(copies, act):
        for copy, condition in copies:
            if condition is None:
                act(copy)
            else:
                pl.when(condition)(functools.partial(act, copy))

    kind_mine = lax.rem(me_row, 2)
    me_plane = me_row // 2
    row_mate = me_row + 1 - 2 * kind_mine
    col_mate = me_col + 1 - 2 * lax.rem(me_col, 2)

    def relay_keys(part, kind, slot):
        return pltpu.make_async_remote_copy(
            src_ref=kv_recv.at[part, kind],
            dst_ref=kv_recv.at[part, kind],
            send_sem=kv_relayed.at[slot],
            recv_sem=kv_came.at[kind, part],
            device_id={"rows": row_mate},
            device_id_type=pl.DeviceIdType.MESH,
        )

    def send_query(part, to, slot):
        return pltpu.make_async_remote_copy(
            src_ref=q_recv.at[part],
            dst_ref=q_recv.at[part],
            send_sem=q_sent.at[slot],
            recv_sem=q_came.at[part],
            device_id={"cols": to},
            device_id_type=pl.DeviceIdType.MESH,
        )

    def on_fan(copies, act):
        for copy, step, to in copies:
            if step:
                act(copy)
            else:
                pl.when(to != me_col)(functools.partial(act, copy))

    def fan_wait(kind, source_of, target):
        for part in range(col_size):
            copy = pltpu.make_async_remote_copy(
                src_ref=source_of(0),
                dst_ref=target.at[part],
                send_sem=fan_send.at[kind, 0],
                recv_sem=fan_recv.at[kind, part],
                device_id={"rows": lax.rem(me_row + 1, row_size)},
                device_id_type=pl.DeviceIdType.MESH,
            )
            pl.when(jnp.logical_not(jnp.logical_and(mine, part == me_col)))(copy.wait_recv)

    loads[0].wait()
    normed = layer_norm(single_v[...]).astype(jnp.bfloat16)
    def project(*kinds):
        weights = [project_v[kind] for kind in kinds]
        return jnp.dot(
            normed, jnp.concatenate(weights, axis=1), preferred_element_type=jnp.float32
        )

    loads[1].wait()
    q_recv[me_col] = project(0).astype(jnp.bfloat16)
    pl.semaphore_wait(barrier, total - 1)
    parts, _, _, part_width = o_send.shape
    each = part_width // group
    col_side = lax.rem(me_col, each)

    def turn_step(turn):
        return exchange(me_col // each, turn, parts)

    peers = [turn_step(turn) * each + col_side for turn in range(1, parts)]
    q_copies = [send_query(me_col, to, slot) for slot, to in enumerate(peers)]
    q_copies.append(send_query(me_col, col_mate, len(peers)))
    for copy in q_copies:
        copy.start()
    loads[2].wait()
    loads[3].wait()
    key_value = project(1, 2).astype(jnp.bfloat16)
    for half in range(halves):
        for kind in range(2):
            kv_send[me_plane, half, kind] = key_value[
                half * tile_cols : (half + 1) * tile_cols, kind * group : (kind + 1) * group
            ]
    planes = row_size // 2
    plane_copies = []
    for step in range(1, planes):
        plane = lax.rem(me_plane + step, planes)
        copy = pltpu.make_async_remote_copy(
            src_ref=kv_send.at[me_plane],
            dst_ref=kv_send.at[me_plane],
            send_sem=plane_sent.at[step - 1],
            recv_sem=plane_came.at[step - 1],
            device_id={"rows": 2 * plane + kind_mine},
            device_id_type=pl.DeviceIdType.MESH,
        )
        copy.start()
        plane_copies.append(copy)
    kv_copies = []

    def send_keys(step):
        plane = lax.rem(me_plane + planes - step, planes)
        for half in range(halves):
            for kind in range(2):
                to = halves * (2 * plane + kind_mine) + half
                row = 2 * me_plane + kind
                copy = pltpu.make_async_remote_copy(
                    src_ref=kv_send.at[plane, half, kind],
                    dst_ref=kv_recv.at[me_col, kind],
                    send_sem=kv_sent.at[(step * 2 + kind) * halves + half],
                    recv_sem=kv_came.at[kind, me_col],
                    device_id={"rows": row, "cols": to},
                    device_id_type=pl.DeviceIdType.MESH,
                )
                here = jnp.logical_and(row == me_row, to == me_col)
                kv_copies.append((copy, jnp.logical_not(here)))
        on_some(kv_copies[-2 * halves :], lambda copy: copy.start())

    send_keys(0)
    loads[4].wait()
    gate_send[...] = jax.nn.sigmoid(project(3)).astype(jnp.bfloat16).reshape(gate_send.shape)

    def own_rows(to):
        return pl.ds(pl.multiple_of(to * rows_each, rows_each), rows_each)

    loads[5].wait()
    loads[6].wait()

    def relay_query(part):
        return send_query(part, col_mate, col_size // 2 + part // each)

    def bias_step(step, _):
        pair_load(step).wait()
        parts = [
            pair_v[half, pl.ds(step * chunk, chunk)].reshape(chunk * tile_cols, wide)
            for half in range(halves)
        ]
        parts = norm_centred(jnp.concatenate(parts, axis=1), centre_v[...], halves)
        parts = [part.reshape(chunk, 1, tile_cols, wide) for part in parts]
        normed_pair = jnp.concatenate(parts, axis=1).reshape(chunk * halves * tile_cols, wide)
        bias = lax.dot_general(
            bias_w[...], normed_pair, (((1,), (1,)), ((), ())), preferred_element_type=jnp.float32
        )
        bias = bias.astype(jnp.bfloat16).astype(jnp.float32)
        for part in range(chunk):
            bias_v[pl.ds(step * chunk + part, heads, stride=stride), :] = bias[
                :, part * LANES : (part + 1) * LANES
            ]
        return 0

    lax.fori_loop(0, depth // chunk, bias_step, 0)
    lane_row = lane_iota((2 * halves * heads, width))
    place = lax.broadcasted_iota(jnp.int32, (2 * halves * heads, width), 0)
    for half in range(halves):
        picked = jnp.where(place == half * heads + lane_row // head_width, 1.0, 0.0)
        spread_v[half, :LANES] = picked.astype(jnp.bfloat16)
        spread_v[half, LANES:] = picked.astype(jnp.bfloat16)

    for step in range(1, planes):
        plane_copies[step - 1].wait_recv()
        send_keys(step)
    own_key = lax.rem(owner, 2) == kind_mine

    @pl.when(own_key)
    def _():
        kv_recv[me_col, kind_mine] = kv_send[owner // 2, half_mine, kind_mine]

    def relay_keys_turn(turn):
        for index in range(each):
            part = turn_step(turn) * each + index
            copy = relay_keys(part, kind_mine, part)
            own = jnp.logical_and(own_key, part == me_col)
            pl.when(jnp.logical_not(own))(copy.wait_recv)
            copy.start()

    st_rows[...] = jnp.zeros_like(st_rows)

    def turn_bias(turn, _):
        for index in range(each * heads_here):
            head = turn_step(turn) * each * heads_here + index
            rows = bias_v[pl.ds(pl.multiple_of(head * stride, 8), depth), :].T
            bias_t[head] = jnp.concatenate([rows[:tile_cols], rows[tile_cols:]], axis=1)
        return 0

    lax.fori_loop(0, parts, turn_bias, 0)
    same_plane = owner // 2 == me_plane
    pl.when(same_plane)(functools.partial(relay_keys_turn, 0))
    relays = [relay_query(peer) for peer in peers]
    for copy in relays:
        copy.wait_recv()
        copy.start()
    pl.when(jnp.logical_not(same_plane))(functools.partial(relay_keys_turn, 0))
    relay_keys_turn(1)
    relays += [relay_keys(part, kind_mine, part) for part in range(col_size)]

    def gate_copy(shift):
        to = lax.rem(me_col + shift, col_size)
        return pltpu.make_async_remote_copy(
            src_ref=gate_send.at[:, to],
            dst_ref=gate_recv.at[me_col],
            send_sem=col_send.at[1, shift - 1],
            recv_sem=col_recv.at[1, shift - 1],
            device_id={"cols": to},
            device_id_type=pl.DeviceIdType.MESH,
        )

    gate_copies = [gate_copy(shift) for shift in range(1, col_size)]
    for copy in gate_copies:
        copy.start()
    gate_recv[me_col] = gate_send[:, me_col]

    length = jnp.sum(jnp.sum(mask_v[...], axis=1, keepdims=True), axis=0, keepdims=True)
    key_place = lax.broadcasted_iota(jnp.int32, (tile_cols, tile_rows), 0)
    valid = me_col * tile_cols + key_place < length
    head_of = lane_iota((tile_cols, group)) // head_width
    head_masks = [
        jnp.where(head_of == head, 1.0, 0.0).astype(jnp.bfloat16) for head in range(heads_here)
    ]
    scale = 1.0 / math.sqrt(head_width)

    def attend_part(part):
        key, value = kv_recv[part, 0], kv_recv[part, 1]
        raw = lax.dot_general(
            jnp.concatenate([key * mask for mask in head_masks], axis=0),
            q_recv[part],
            (((1,), (1,)), ((), ())),
            preferred_element_type=jnp.float32,
        )
        weights = []
        for head in range(heads_here):
            index = part * heads_here + head
            scores = raw[head * tile_cols : (head + 1) * tile_cols] * scale + bias_t[index]
            scores = jnp.where(valid, scores, excluded)
            top = jnp.max(scores, axis=0, keepdims=True)
            weight = jnp.exp(scores - top)
            st_rows[pl.ds(index, 1), :] = top
            st_rows[pl.ds(halves * heads + index, 1), :] = jnp.sum(weight, axis=0, keepdims=True)
            weights.append(weight.astype(jnp.bfloat16))
        mixed = lax.dot_general(
            jnp.concatenate(weights, axis=0),
            jnp.concatenate([value * mask for mask in head_masks], axis=0),
            (((0,), (0,)), ((), ())),
            preferred_element_type=jnp.float32,
        )
        pieces = [
            mixed[half * depth : (half + 1) * depth].reshape(col_size, rows_each, group)
            for half in range(halves)
        ]
        return jnp.concatenate(pieces, axis=1).astype(jnp.bfloat16)

    def o_copy(step, shift):
        to = lax.rem(me_col + shift, col_size)
        return pltpu.make_async_remote_copy(
            src_ref=o_send.at[step, to],
            dst_ref=o_recv.at[step, me_col],
            send_sem=o_sent.at[step, shift - 1],
            recv_sem=o_came.at[step, shift - 1],
            device_id={"cols": to},
            device_id_type=pl.DeviceIdType.MESH,
        )

    def st_copy(shift):
        to = lax.rem(me_col + shift, col_size)
        return pltpu.make_async_remote_copy(
            src_ref=st_send.at[own_rows(to)],
            dst_ref=st_recv.at[me_col],
            send_sem=col_send.at[2, shift - 1],
            recv_sem=col_recv.at[2, shift - 1],
            device_id={"cols": to},
            device_id_type=pl.DeviceIdType.MESH,
        )

    def attend_step(turn, _):
        step = turn_step(turn)
        far = step * each + 1 - col_side
        relay_query(far).wait_recv()
        for index in range(each):
            part = step * each + index
            relay_keys(part, 1 - kind_mine, part).wait_recv()
        for index in range(each):
            o_send[step, :, :, index * group : (index + 1) * group] = attend_part(
                step * each + index
            )

        @pl.when(turn == parts - 1)
        def _():
            stats = st_rows[...].T
            st_send[...] = stats[:depth] + pltpu.roll(stats[depth:], heads, axis=1)
            for shift in range(1, col_size):
                st_copy(shift).start()

        for shift in range(1, col_size):
            o_copy(step, shift).start()
        pl.when(turn + 2 < parts)(functools.partial(relay_keys_turn, turn + 2))
        return 0

    lax.fori_loop(0, parts, attend_step, 0)
    st_copies = [st_copy(shift) for shift in range(1, col_size)]
    st_recv[me_col] = st_send[own_rows(me_col)]
    for step in range(parts):
        o_recv[step, me_col] = o_send[step, me_col]
    o_copies = [o_copy(step, shift) for step in range(parts) for shift in range(1, col_size)]
    for copy in gate_copies + st_copies:
        copy.wait_recv()
    stats = st_recv[...]
    lane = lane_iota(stats.shape)
    top = jnp.max(stats, axis=0, keepdims=True)
    factor = jnp.exp(stats - top)
    sums = jnp.sum(factor * pltpu.roll(stats, halves * heads, axis=2), axis=0, keepdims=True)
    factor = jnp.where(lane < halves * heads, factor / sums, 0.0)
    factor = factor.reshape(col_size * rows_each, LANES)
    high = factor.astype(jnp.bfloat16)
    rest = (factor - high.astype(jnp.float32)).astype(jnp.bfloat16)
    factor = jnp.concatenate([high, rest], axis=1)
    scales = [
        jnp.dot(factor, spread_v[half], preferred_element_type=jnp.float32) for half in range(halves)
    ]
    gate = jnp.concatenate(
        [
            gate_recv[part].astype(jnp.float32).reshape(halves * rows_each, group)
            for part in range(col_size)
        ],
        axis=1,
    )
    for copy in o_copies:
        copy.wait_recv()
    attended = jnp.zeros((halves * rows_each, width), jnp.float32)
    for part in range(col_size):
        rows = slice(part * rows_each, (part + 1) * rows_each)
        part_scale = jnp.concatenate([scales[half][rows] for half in range(halves)], axis=0)
        whole = jnp.concatenate([o_recv[step, part] for step in range(parts)], axis=1)
        attended = attended + part_scale * whole.astype(jnp.float32)
    mixed = (attended * gate).astype(jnp.bfloat16)
    for copy in loads[7:]:
        copy.wait()
    added = jnp.dot(mixed, out_v[...], preferred_element_type=jnp.float32)
    own = own_single[...].astype(jnp.float32).reshape(halves * rows_each, width)
    updated = (own + added).astype(jnp.bfloat16)
    so_send[...] = updated.astype(jnp.float32).reshape(halves, rows_each, width).astype(jnp.bfloat16)
    factors = jnp.dot(
        layer_norm(updated).astype(jnp.bfloat16),
        factors_v[...],
        preferred_element_type=jnp.float32,
    )
    factors = factors.astype(jnp.bfloat16).astype(jnp.float32)
    first, second = factors[:rows_each], factors[rows_each:]
    shift = factors.shape[1] // 2
    low = lane_iota(first.shape) < shift
    left = jnp.where(low, first, pltpu.roll(second, shift, axis=1))
    right = jnp.where(low, pltpu.roll(first, shift, axis=1), second)
    left_send[...] = left.astype(jnp.bfloat16)
    right_send[...] = right.astype(jnp.bfloat16)
    right_copies = fan_copies(1, lambda half: right_send, right_recv)
    on_fan(right_copies, lambda copy: copy.start())
    left_copies = to_cols(4, lambda to: left_send, left_recv.at[me_col])
    left_recv[me_col] = left.astype(jnp.bfloat16)

    @pl.when(mine)
    def _():
        right_recv[me_col] = right_send[...]

    fan_wait(1, lambda half: right_send, right_recv)
    for copy in left_copies:
        copy.wait_recv()
    so_copies = to_cols(5, lambda to: so_send, single_out.at[:, me_col])
    single_out[:, me_col] = so_send[...]
    left = left_recv[...].astype(jnp.float32).reshape(depth, LANES)
    turned = pltpu.roll(left, shift, axis=1)
    low = lane_iota(left.shape) < shift
    left_out[:depth] = jnp.where(low, left, turned)
    left_out[depth:] = jnp.where(low, turned, left)
    right = right_recv[...].astype(jnp.float32).reshape(tile_cols, LANES)
    turned = pltpu.roll(right, shift, axis=1)
    right_out[...] = jnp.where(lane_iota(right.shape) // shift == half_mine, right, turned)

    twice_v[...] = twice(pairout_v[...])
    block = update_block
    def update_step(step, _):
        first = step * 2 * block
        half = first // depth
        pair_out[pl.ds(first, 2 * block)] = update_rows(
            lambda index: pair_v[half, pl.ds(first - half * depth + index * block, block)],
            lambda index: left_out[pl.ds(pl.multiple_of(first + index * block, 8), block)],
            right_out[...],
            block,
            centre_v[...],
            twice_v[...],
            up_v[...],
            down_v[...],
        )
        return 0

    lax.fori_loop(0, tile_rows // (2 * block), update_step, 0)

    for copies in (q_copies, relays, plane_copies, gate_copies, st_copies, o_copies, left_copies, so_copies):
        for copy in copies:
            copy.wait_send()
    on_some(kv_copies, lambda copy: copy.wait_send())
    on_fan(right_copies, lambda copy: copy.wait_send())
    for copy in so_copies:
        copy.wait_recv()


def finish_kernel(single, pair, single_out, pair_out, sems):
    copies = [pltpu.make_async_copy(single, single_out, sems.at[0])]
    steps = sems.shape[0] - 1
    rows = pair.shape[0] // steps
    for step in range(steps):
        part = pl.ds(step * rows, rows)
        copies.append(
            pltpu.make_async_copy(pair.at[part], pair_out.at[part], sems.at[1 + step])
        )
    for copy in copies:
        copy.start()
    for copy in copies:
        copy.wait()


def finish(single, pair):
    return pl.pallas_call(
        finish_kernel,
        out_shape=tuple(jax.ShapeDtypeStruct(array.shape, array.dtype) for array in (single, pair)),
        in_specs=[pl.BlockSpec(memory_space=pltpu.VMEM)] * 2,
        out_specs=[pl.BlockSpec(memory_space=pl.ANY)] * 2,
        scratch_shapes=[pltpu.SemaphoreType.DMA((9,))],
        compiler_params=pltpu.CompilerParams(vmem_limit_bytes=8 * 1024 * 1024),
        name="finish",
    )(single, pair)


def attend(
    single, pair, mask, w_bias, w_project, w_out, w_factors, w_pairout, w_up, w_down,
    row_size, col_size,
):
    halves, depth, tile_cols, wide = pair.shape
    tile_rows, width = single.shape
    heads = w_bias.shape[1]
    rows_each = depth // col_size
    group = w_project.shape[2]
    steps = depth // 16
    parts = col_size // 2
    stride = depth + 8
    any_spec = pl.BlockSpec(memory_space=pltpu.HBM)
    vmem_spec = pl.BlockSpec(memory_space=pltpu.VMEM)
    bf16, f32 = jnp.bfloat16, jnp.float32
    single_out, pair_out = pl.pallas_call(
        functools.partial(attend_kernel, row_size, col_size, heads, tile_cols, stride),
        out_shape=(
            pltpu.VMEM((halves, col_size, rows_each, width), bf16),
            pltpu.VMEM((tile_rows, tile_cols, wide), bf16),
        ),
        in_specs=[any_spec] * 10,
        out_specs=[vmem_spec] * 2,
        scratch_shapes=[
            pltpu.VMEM((tile_rows, width), bf16),
            pltpu.VMEM((halves, depth, tile_cols, wide), bf16),
            pltpu.VMEM((mask.shape[0] // LANES, LANES), jnp.int32),
            pltpu.VMEM((heads, wide), bf16),
            pltpu.VMEM(w_project.shape, bf16),
            pltpu.VMEM(w_out.shape, bf16),
            pltpu.VMEM(w_factors.shape, bf16),
            pltpu.VMEM((halves, rows_each, width), bf16),
            pltpu.VMEM((row_size // 2, halves, 2, tile_cols, group), bf16),
            pltpu.VMEM((col_size, 2, tile_cols, group), bf16),
            pltpu.VMEM((col_size, tile_rows, group), bf16),
            pltpu.VMEM((halves, col_size, rows_each, group), bf16),
            pltpu.VMEM((col_size, halves, rows_each, group), bf16),
            pltpu.VMEM(((heads + 1) * stride, LANES), f32),
            pltpu.VMEM((parts, col_size, halves * rows_each, width // parts), bf16),
            pltpu.VMEM((parts, col_size, halves * rows_each, width // parts), bf16),
            pltpu.VMEM((depth, LANES), f32),
            pltpu.VMEM((col_size, rows_each, LANES), f32),
            pltpu.VMEM((rows_each, LANES), bf16),
            pltpu.VMEM((rows_each, LANES), bf16),
            pltpu.VMEM((col_size, rows_each, LANES), bf16),
            pltpu.VMEM((col_size, rows_each, LANES), bf16),
            pltpu.VMEM((tile_rows, wide), f32),
            pltpu.VMEM((tile_cols, wide), f32),
            pltpu.VMEM((halves, rows_each, width), bf16),
            pltpu.VMEM((heads, tile_cols, tile_rows), f32),
            pltpu.VMEM((4 * heads, tile_rows), f32),
            pltpu.VMEM((halves * wide, halves * wide), bf16),
            pltpu.VMEM((halves, 2 * LANES, width), bf16),
            pltpu.VMEM(w_pairout.shape, bf16),
            pltpu.VMEM((2 * wide, 2 * wide), bf16),
            pltpu.VMEM(w_up.shape, bf16),
            pltpu.VMEM(w_down.shape, bf16),
            pltpu.SemaphoreType.DMA((12 + halves,)),
            pltpu.SemaphoreType.DMA((steps,)),
            pltpu.SemaphoreType.DMA((6, col_size - 1)),
            pltpu.SemaphoreType.DMA((6, col_size - 1)),
            pltpu.SemaphoreType.DMA((2, row_size * halves)),
            pltpu.SemaphoreType.DMA((2, col_size)),
            pltpu.SemaphoreType.DMA((row_size // 2 - 1,)),
            pltpu.SemaphoreType.DMA((row_size // 2 - 1,)),
            pltpu.SemaphoreType.DMA((row_size * halves,)),
            pltpu.SemaphoreType.DMA((2, col_size)),
            pltpu.SemaphoreType.DMA((col_size,)),
            pltpu.SemaphoreType.DMA((2 * col_size,)),
            pltpu.SemaphoreType.DMA((col_size,)),
            pltpu.SemaphoreType.DMA((parts, col_size - 1)),
            pltpu.SemaphoreType.DMA((parts, col_size - 1)),
        ],
        compiler_params=pltpu.CompilerParams(
            collective_id=3, has_side_effects=True, vmem_limit_bytes=40 * 1024 * 1024
        ),
        name="attend",
    )(
        *(
            pltpu.with_memory_space_constraint(array, pltpu.HBM)
            for array in (
                single,
                pair,
                mask.reshape(mask.shape[0] // LANES, LANES),
                w_bias.T,
                w_project,
                w_out,
                w_factors,
                w_pairout,
                w_up,
                w_down,
            )
        )
    )
    single_out, pair_out = finish(single_out, pair_out)
    return single_out.reshape(tile_rows, width), pair_out


def fits(row_size, col_size, single, pair, mask, w_bias, w_project, w_factors):
    tile_rows, tile_cols, wide = pair.shape
    heads = w_bias.shape[1]
    return (
        tile_rows == 2 * tile_cols
        and 2 * tile_cols == LANES
        and wide == LANES
        and w_factors.shape[1] == LANES
        and w_project.shape[2] == LANES
        and 4 * heads == LANES
        and heads % (2 * col_size) == 0
        and tile_cols % (8 * col_size) == 0
        and col_size == 2 * row_size
        and row_size % 2 == 0
        and col_size & (col_size - 1) == 0
        and tile_cols % (2 * update_block) == 0
        and mask.shape[0] % LANES == 0
    )


def per_device_keys(
    row_size, col_size,
    single, pair, residue_mask, w_bias, w_project, w_out, w_factors, w_pairout, w_up, w_down
):
    shape = pair.shape
    return attend(
        single, pair.reshape(2, shape[0] // 2, *shape[1:]), residue_mask,
        w_bias, w_project, w_out, w_factors, w_pairout, w_up, w_down, row_size, col_size,
    )


def dispatch(row_size, col_size, *arrays):
    single, pair, residue_mask, w_bias, w_project, w_out, w_factors = arrays[:7]
    if fits(row_size, col_size, single, pair, residue_mask, w_bias, w_project, w_factors):
        return per_device_keys(row_size, col_size, *arrays)
    return per_device(row_size, col_size, *arrays)


def solution(mesh):
    return jax.shard_map(
        functools.partial(dispatch, mesh.shape["rows"], mesh.shape["cols"]),
        mesh=mesh,
        in_specs=(
            P("rows", None),
            P("rows", "cols", None),
            P(),
            P(),
            P(None, None, "cols"),
            P(),
            P(),
            P(),
            P(),
            P(),
        ),
        out_specs=(P("rows", None), P("rows", "cols", None)),
        check_vma=False,
    )
```
